8 devices in a mesh: rep: 2 (over y, z), dp: 4 (over x, core).
Axes of the slice: x: 2, y: 2, z: 1, core: 2. Of those that a mesh axis runs over, the one named last changes fastest.
Arguments:
- x: bfloat16 [8, 2048, 896], P(('rep', 'dp')), parts along dimension 0
- dy: bfloat16 [8, 2048, 896], P(('rep', 'dp')), parts along dimension 0
- w_gate: bfloat16 [2, 896, 4736], replicated
- w_up: bfloat16 [2, 896, 4736], replicated
- w_down: bfloat16 [2, 4736, 896], replicated
- m_w_gate: float32 [2, 896, 4736], replicated
- m_w_up: float32 [2, 896, 4736], replicated
- m_w_down: float32 [2, 4736, 896], replicated
- v_w_gate: float32 [2, 896, 4736], replicated
- v_w_up: float32 [2, 896, 4736], replicated
- v_w_down: float32 [2, 4736, 896], replicated
Outputs:
- output 1: bfloat16 [4, 896, 4736], P('rep'), parts along dimension 0
- output 2: bfloat16 [4, 896, 4736], P('rep'), parts along dimension 0
- output 3: bfloat16 [4, 4736, 896], P('rep'), parts along dimension 0
- output 4: float32 [4, 896, 4736], P('rep'), parts along dimension 0
- output 5: float32 [4, 896, 4736], P('rep'), parts along dimension 0
- output 6: float32 [4, 4736, 896], P('rep'), parts along dimension 0
- output 7: float32 [4, 896, 4736], P('rep'), parts along dimension 0
- output 8: float32 [4, 896, 4736], P('rep'), parts along dimension 0
- output 9: float32 [4, 4736, 896], P('rep'), parts along dimension 0
There are 2 independent parts. The reference program is written for one: setup_inputs(seed, part) draws one part's arguments, and reference() takes and returns one part's arrays. A program takes and returns all parts, laid end to end along the dimension named above; an argument that names none is the same for every part.
All inputs are finite; a program needn't handle non-finite values.
Results may differ from the reference program's by a relative error of at most 0.022.
Values are sent between devices in bfloat16 or wider.
A program may use at most 3 GiB of HBM per device.

```python
import jax
import jax.numpy as jnp
from jax import lax

SEQUENCES = 4
TOKENS = 2048
D = 896
FF = 4736
LAYERS = 2
NAMES = ("w_gate", "w_up", "w_down")
SHAPES = {"w_gate": (LAYERS, D, FF), "w_up": (LAYERS, D, FF), "w_down": (LAYERS, FF, D)}


def bump(key, n, height):
    away = (jnp.arange(n, dtype=jnp.int32) - jax.random.randint(key, (), 0, n, jnp.int32)) % n
    return jnp.where(away < n // 8, height, 1.0)


def together(key, own, strength):
    shared = jax.random.normal(key, own.shape[1:], jnp.float32)
    return (own + strength * shared) * lax.rsqrt(1 + strength * strength)


def setup_inputs(seed: int = 0, part: int = 0) -> dict:
    kx, kdy, ka, kb, kz, kf, kh, kl, *keys = jax.random.split(jax.random.key(seed), 8 + 3 * len(NAMES))
    kx, kdy, ka, kb = (jax.random.fold_in(k, part) for k in (kx, kdy, ka, kb))
    kw, km, kv = (keys[i::3] for i in range(3))
    shape = (SEQUENCES, TOKENS, D)
    much_x, much_dy = jax.random.uniform(kz, (2,), jnp.float32, 0.0, 1.0)
    loud = 2.0 ** jax.random.uniform(jax.random.fold_in(kz, 1), (), jnp.float32, -1.0, 2.0)
    layers = 2.0 ** jax.random.uniform(kl, (LAYERS, 1, 1), jnp.float32, -1.0, 1.0)
    x = together(ka, jax.random.normal(kx, shape, jnp.float32), much_x) * bump(kf, D, 4.0)
    dy = together(kb, jax.random.normal(kdy, shape, jnp.float32), much_dy)
    drawn = {"x": x.astype(jnp.bfloat16), "dy": (loud * dy * (SEQUENCES * TOKENS) ** -0.5).astype(jnp.bfloat16)}
    for key, name in zip(kw, NAMES, strict=True):
        w = jax.random.normal(key, SHAPES[name], jnp.float32) * SHAPES[name][1] ** -0.5
        drawn[name] = (w * {"w_gate": 1.0, "w_up": bump(kh, FF, 4.0), "w_down": layers}[name]).astype(jnp.bfloat16)
    for key, name in zip(km, NAMES, strict=True):
        drawn[f"m_{name}"] = 0.1 * jax.random.normal(key, SHAPES[name], jnp.float32)
    for key, name in zip(kv, NAMES, strict=True):
        drawn[f"v_{name}"] = jax.random.uniform(key, SHAPES[name], jnp.float32, 0.005, 0.015)
    return drawn


def matmul(a, w):
    return jnp.dot(a, w, preferred_element_type=jnp.float32).astype(jnp.bfloat16)


def normed(h):
    wide = h.astype(jnp.float32)
    scale = lax.rsqrt(jnp.mean(wide**2, -1, keepdims=True) + 1e-6)
    return (wide * scale).astype(jnp.bfloat16)


def layer(h, w):
    a = normed(h)
    gate = jnp.dot(a, w["w_gate"], preferred_element_type=jnp.float32)
    up = jnp.dot(a, w["w_up"], preferred_element_type=jnp.float32)
    return h + matmul((jax.nn.silu(gate) * up).astype(jnp.bfloat16), w["w_down"])


def adamw(w, m, v, g):
    m = 0.9 * m + 0.1 * g
    v = 0.95 * v + 0.05 * g * g
    step = m * lax.rsqrt(v + 1e-8) + 0.1 * w
    return (w - 0.02 * step).astype(jnp.bfloat16), m, v


def clipped(gradients, sum_of_squares, count):
    factor = jnp.minimum(1.0, 0.5 * lax.rsqrt(sum_of_squares / count + 1e-30))
    return [g * factor for g in gradients]


def stack(weights, h):
    return lax.scan(lambda h, w: (layer(h, w), None), h, weights)[0]


def reference(x, dy, w_gate, w_up, w_down, m_w_gate, m_w_up, m_w_down, v_w_gate, v_w_up, v_w_down):
    weights = dict(zip(NAMES, (w_gate, w_up, w_down), strict=True))

    def take(so_far, sequence):
        h, by_y = sequence
        _, back = jax.vjp(lambda w: stack(w, h), weights)
        return jax.tree.map(lambda total, term: total + term.astype(jnp.float32), so_far, back(by_y)[0]), None

    none_yet = {name: jnp.zeros(w.shape, jnp.float32) for name, w in weights.items()}
    by_weights, _ = lax.scan(take, none_yet, (x, dy))
    gradients = [by_weights[name].astype(jnp.bfloat16).astype(jnp.float32) for name in NAMES]
    gradients = clipped(gradients, sum(jnp.sum(g * g) for g in gradients), sum(g.size for g in gradients))
    new = [
        adamw(w.astype(jnp.float32), m, v, g)
        for w, m, v, g in zip((w_gate, w_up, w_down), (m_w_gate, m_w_up, m_w_down), (v_w_gate, v_w_up, v_w_down), gradients, strict=True)
    ]
    return tuple(one[which] for which in range(3) for one in new)
```

```python
import functools

import jax
import jax.numpy as jnp
from jax import lax
from jax.experimental import pallas as pl
from jax.experimental.pallas import tpu as pltpu
from jax.sharding import PartitionSpec as P

F32, BF16 = jnp.float32, jnp.bfloat16
PX = ((0, 2), (2, 0), (1, 3), (3, 1))
PD = ((0, 1), (1, 0), (2, 3), (3, 2))


def dot(a, b, dims):
    return lax.dot_general(a, b, (dims, ((), ())), preferred_element_type=F32)


NN, NT, TN = ((1,), (0,)), ((1,), (1,)), ((0,), (0,))


def px(a):
    return lax.ppermute(a, "dp", PX)


def pd(a):
    return lax.ppermute(a, "dp", PD)


def norm_scale(h):
    wide = h.astype(F32)
    return wide, lax.rsqrt(jnp.mean(wide**2, -1, keepdims=True) + 1e-6)


def normed(h):
    wide, scale = norm_scale(h)
    return (wide * scale).astype(BF16)


def norm_back(h, da):
    wide, scale = norm_scale(h)
    dw = scale * da - wide * (scale**3 * jnp.mean(wide * da, -1, keepdims=True))
    return dw.astype(BF16)


def adam_kernel(idx, f_ref, w_ref, m_ref, v_ref, g_ref, *rest):
    wo, mo, vo = rest[-3:]
    g = g_ref[...].astype(F32)[None] * f_ref[0]
    m = 0.9 * m_ref[...] + 0.1 * g
    v = 0.95 * v_ref[...] + 0.05 * g * g
    w = w_ref[...].astype(F32)
    wo[...] = (w - 0.02 * (m * lax.rsqrt(v + 1e-8) + 0.1 * w)).astype(BF16)
    mo[...] = m
    vo[...] = v


def adam_piece(layer, quarter, factor, w, m, v, g, outs):
    layers, rows, cols = w.shape
    part = rows // 4
    if cols > rows:
        block, steps = (1, 32, cols), part // 32
        whole = lambda i, idx: (layer, idx[0] * steps + i, 0)
        gspec = pl.BlockSpec((32, cols), lambda i, idx: (i, 0))
    else:
        block, steps = (1, part, 128), cols // 128
        whole = lambda i, idx: (layer, idx[0], i)
        gspec = pl.BlockSpec((part, 128), lambda i, idx: (0, i))
    spec = pl.BlockSpec(block, whole)
    any_ = pl.BlockSpec(memory_space=pl.ANY)
    n = 0 if outs is None else 3
    out = pl.pallas_call(
        adam_kernel,
        grid_spec=pltpu.PrefetchScalarGridSpec(
            num_scalar_prefetch=1,
            grid=(steps,),
            in_specs=[pl.BlockSpec(memory_space=pltpu.SMEM), spec, spec, spec, gspec] + [any_] * n,
            out_specs=[spec] * 3,
        ),
        out_shape=[jax.ShapeDtypeStruct(w.shape, BF16), jax.ShapeDtypeStruct(m.shape, F32), jax.ShapeDtypeStruct(v.shape, F32)],
        input_output_aliases={6 + i: i for i in range(n)},
        cost_estimate=pl.CostEstimate(flops=part * cols * 2000, bytes_accessed=part * cols * 22, transcendentals=part * cols),
        compiler_params=pltpu.CompilerParams(vmem_limit_bytes=40 << 20),
        name="adam",
    )(quarter.reshape(1), factor, w, m, v, g, *(outs or ()))
    return tuple(out)


def solution(mesh):
    def step(x, dy, wg, wu, wd, mg, mu, md, vg, vu, vd):
        me = lax.axis_index("dp")
        chip, core = me // 2, me % 2
        own, other = me, (1 - chip) * 2 + core
        mine, far = chip * 2 + 1 - core, (1 - chip) * 2 + 1 - core
        x, dy = x[0], dy[0]

        def scatter(grad):
            q = grad.reshape(4, grad.shape[0] // 4, grad.shape[1])
            take = lambda k: lax.dynamic_index_in_dim(q, k, keepdims=False)
            theirs_far = pd(take(far))
            theirs = pd(take(mine))
            across = px((take(other).astype(F32) + theirs_far.astype(F32)).astype(BF16))
            return (take(own).astype(F32) + theirs.astype(F32) + across.astype(F32)).astype(BF16)

        def gate_up(a, l):
            return dot(a, wg[l], NN), dot(a, wu[l], NN)

        def back_hidden(gate, up, dh, l):
            dhid = dot(dh, wd[l], NT).astype(BF16).astype(F32)
            sig = jax.nn.sigmoid(gate)
            dgate = dhid * up * (sig * (1 + gate * (1 - sig)))
            return dgate.astype(BF16), (dhid * gate * sig).astype(BF16)

        h0, a0 = x, normed(x)
        gate0, up0 = gate_up(a0, 0)
        hid0 = (jax.nn.silu(gate0) * up0).astype(BF16)
        h1 = h0 + dot(hid0, wd[0], NN).astype(BF16)
        a1 = normed(h1)
        gate1, up1 = gate_up(a1, 1)
        hid1 = (jax.nn.silu(gate1) * up1).astype(BF16)
        sums = {}
        sums["d", 1] = scatter(dot(hid1, dy, TN).astype(BF16))
        dgate1, dup1 = back_hidden(gate1, up1, dy, 1)
        sums["g", 1] = scatter(dot(a1, dgate1, TN).astype(BF16))
        sums["u", 1] = scatter(dot(a1, dup1, TN).astype(BF16))
        da1 = (dot(dgate1, wg[1], NT) + dot(dup1, wu[1], NT)).astype(BF16).astype(F32)
        dh1 = dy + norm_back(h1, da1)
        sums["d", 0] = scatter(dot(hid0, dh1, TN).astype(BF16))
        dgate0, dup0 = back_hidden(gate0, up0, dh1, 0)
        sums["g", 0] = scatter(dot(a0, dgate0, TN).astype(BF16))
        sums["u", 0] = scatter(dot(a0, dup0, TN).astype(BF16))

        total = sum(jnp.sum(jnp.square(g.astype(F32))) for g in sums.values()).reshape(1)
        total = total + px(total)
        total = total + pd(total)
        count = sum(w.size for w in (wg, wu, wd))
        factor = jnp.minimum(1.0, 0.5 * lax.rsqrt(total / count + 1e-30))

        outs = {"g": None, "u": None, "d": None}
        arrays = {"g": (wg, mg, vg), "u": (wu, mu, vu), "d": (wd, md, vd)}
        pieces = {}
        for key, g in sums.items():
            gx = px(g)
            pieces[key] = ((own, g), (mine, pd(g)), (other, gx), (far, pd(gx)))
        for at in range(4):
            for name, layer in pieces:
                quarter, g = pieces[name, layer][at]
                outs[name] = adam_piece(layer, quarter, factor, *arrays[name], g, outs[name])
        return tuple(outs[name][which] for which in range(3) for name in "gud")

    return jax.shard_map(
        step,
        mesh=mesh,
        in_specs=(P(("rep", "dp"), None, None),) * 2 + (P(None, None, None),) * 9,
        out_specs=(P("rep", None, None),) * 9,
        check_vma=False,
    )
```

```python
import jax
import jax.numpy as jnp
from jax import lax
from jax.experimental import pallas as pl
from jax.experimental.pallas import tpu as pltpu
from jax.sharding import PartitionSpec as P


F32, BF16 = jnp.float32, jnp.bfloat16
PX = ((0, 2), (2, 0), (1, 3), (3, 1))
PD = ((0, 1), (1, 0), (2, 3), (3, 2))
NN, NT = ((1,), (0,)), ((1,), (1,))

LANES = 128
BLOCK = 512
ROWS = 512
SHARED_APART = False


def dot(a, b, dims):
    return lax.dot_general(a, b, (dims, ((), ())), preferred_element_type=F32)


def sigmoid(x):
    return 0.5 * jnp.tanh(0.5 * x) + 0.5


def px(a):
    return lax.ppermute(a, "dp", PX)


def pd(a):
    return lax.ppermute(a, "dp", PD)


def once(shape, index):
    return pl.BlockSpec(shape, index, pipeline_mode=pl.Buffered(1))


def params(mib=62):
    return pltpu.CompilerParams(vmem_limit_bytes=mib << 20)


def norm_scale(wide):
    return lax.rsqrt(jnp.mean(wide * wide, -1, keepdims=True) + 1e-6)


def normed(h):
    wide = h.astype(F32)
    return (wide * norm_scale(wide)).astype(BF16)


def forward_kernel(tail, x_ref, wg_ref, wu_ref, wd_ref, h_ref, a_ref, a0_ref, acc_ref):
    j, last = pl.program_id(0), pl.num_programs(0) - 1
    tokens = x_ref.shape[0]
    chunks = [pl.ds(r, ROWS) for r in range(0, tokens, ROWS)]

    @pl.when(j == 0)
    def _():
        for r in chunks:
            a0_ref[r, :] = normed(x_ref[r, :])
            acc_ref[r, :] = jnp.zeros((ROWS, acc_ref.shape[1]), F32)

    def block(width):
        hid = {}

        def up(r):
            a = a0_ref[chunks[r], :]
            g = dot(a, wg_ref[0, :, :width], NN)
            u = dot(a, wu_ref[0, :, :width], NN)
            hid[r] = (g * sigmoid(g) * u).astype(BF16)

        def down(r):
            acc_ref[chunks[r], :] += dot(hid.pop(r), wd_ref[0, :width, :], NN)

        up(0)
        for r in range(1, len(chunks)):
            up(r)
            down(r - 1)
        down(len(chunks) - 1)

    @pl.when(j < last)
    def _():
        block(wg_ref.shape[2])

    @pl.when(j == last)
    def _():
        block(tail)
        for r in chunks:
            h = (x_ref[r, :].astype(F32) + acc_ref[r, :].astype(BF16).astype(F32)).astype(BF16)
            h_ref[r, :] = h
            a_ref[r, :] = normed(h)


def forward(x, wg, wu, wd):
    tokens, d = x.shape
    ff = wg.shape[2]
    steps = pl.cdiv(ff, BLOCK)
    full = once((tokens, d), lambda j: (0, 0))
    across = pl.BlockSpec((1, d, BLOCK), lambda j: (0, 0, j))
    down = pl.BlockSpec((1, BLOCK, d), lambda j: (0, j, 0))
    return pl.pallas_call(
        lambda *refs: forward_kernel(ff - (steps - 1) * BLOCK, *refs),
        grid=(steps,),
        in_specs=[full, across, across, down],
        out_specs=[full] * 3,
        out_shape=[jax.ShapeDtypeStruct((tokens, d), BF16)] * 3,
        scratch_shapes=[pltpu.VMEM((tokens, d), F32)],
        cost_estimate=pl.CostEstimate(flops=6 * tokens * d * ff, bytes_accessed=6 * d * ff, transcendentals=tokens * ff),
        compiler_params=params(),
        name="forward",
    )(x, wg, wu, wd)


def hidden_back(g, u, dhid):
    dhid = dhid.astype(BF16).astype(F32)
    sig = sigmoid(g)
    act = g * sig
    return (dhid * u * (sig + act * (1 - sig))).astype(BF16), (dhid * act).astype(BF16), (act * u).astype(BF16)


def chain_kernel(tail, a_ref, dy_ref, h_ref, wg_ref, wu_ref, wd_ref, dh_ref, acc_ref):
    j, last = pl.program_id(0), pl.num_programs(0) - 1
    tokens = a_ref.shape[0]
    chunks = [pl.ds(r, ROWS) for r in range(0, tokens, ROWS)]

    @pl.when(j == 0)
    def _():
        for r in chunks:
            acc_ref[r, :] = jnp.zeros((ROWS, acc_ref.shape[1]), F32)

    def block(width):
        held = {}

        def there(r):
            a, dy = a_ref[chunks[r], :], dy_ref[chunks[r], :]
            g = dot(a, wg_ref[0, :, :width], NN)
            u = dot(a, wu_ref[0, :, :width], NN)
            dhid = dot(dy, wd_ref[0, :width, :], NT)
            held[r] = hidden_back(g, u, dhid)[:2]

        def back(r):
            dg, du = held.pop(r)
            acc_ref[chunks[r], :] += dot(dg, wg_ref[0, :, :width], NT) + dot(du, wu_ref[0, :, :width], NT)

        there(0)
        for r in range(1, len(chunks)):
            there(r)
            back(r - 1)
        back(len(chunks) - 1)

    @pl.when(j < last)
    def _():
        block(wg_ref.shape[2])

    @pl.when(j == last)
    def _():
        block(tail)
        for r in chunks:
            wide, da = h_ref[r, :].astype(F32), acc_ref[r, :].astype(BF16).astype(F32)
            scale = norm_scale(wide)
            back = scale * da - wide * (scale * scale * scale * jnp.mean(wide * da, -1, keepdims=True))
            dh_ref[r, :] = (dy_ref[r, :].astype(F32) + back.astype(BF16).astype(F32)).astype(BF16)


def chain(a, dy, h, wg, wu, wd):
    tokens, d = a.shape
    ff = wg.shape[2]
    steps = pl.cdiv(ff, BLOCK)
    full = once((tokens, d), lambda j: (0, 0))
    across = pl.BlockSpec((1, d, BLOCK), lambda j: (1, 0, j))
    down = pl.BlockSpec((1, BLOCK, d), lambda j: (1, j, 0))
    return pl.pallas_call(
        lambda *refs: chain_kernel(ff - (steps - 1) * BLOCK, *refs),
        grid=(steps,),
        in_specs=[full, full, full, across, across, down],
        out_specs=full,
        out_shape=jax.ShapeDtypeStruct((tokens, d), BF16),
        scratch_shapes=[pltpu.VMEM((tokens, d), F32)],
        cost_estimate=pl.CostEstimate(flops=10 * tokens * d * ff, bytes_accessed=6 * d * ff, transcendentals=tokens * ff),
        compiler_params=params(),
        name="chain",
    )(a, dy, h, wg, wu, wd)


def squares(x):
    x = x.astype(F32)
    x = x * x
    total = None
    for c in range(0, x.shape[1], LANES):
        part = jnp.sum(x[:, c : c + LANES].reshape(x.shape[0] // 8, 8, LANES), 0)
        total = part if total is None else total + part
    return total


def slices_kernel(own, me_ref, *refs):
    a_refs, dy_refs = refs[:4], refs[4:8]
    weights, outs, scratch = refs[8:14], refs[14:22], refs[22:]
    wg_ref, wu_ref, wd_ref, accg_ref, accu_ref, accd_ref, a_buf, dy_buf, sems = scratch
    i, steps = pl.program_id(0), pl.num_programs(0)
    tokens = a_refs[0].shape[0]
    each = tokens // ROWS
    me = me_ref[0]

    def fetch(step, do):
        slot = lax.rem(step, 2)
        owner, chunk = step // each, lax.rem(step, each)
        away = (owner + me) % 2 + 2 * ((owner // 2 + me // 2) % 2)
        rows = pl.ds(pl.multiple_of(chunk * ROWS, ROWS), ROWS)
        for k in range(4):

            @pl.when(away == k)
            def _():
                do(pltpu.make_async_copy(a_refs[k].at[rows, :], a_buf.at[slot], sems.at[0, slot]))
                do(pltpu.make_async_copy(dy_refs[k].at[rows, :], dy_buf.at[slot], sems.at[1, slot]))

    @pl.when(i == 0)
    def _():
        fetch(i, lambda copy: copy.start())
        wg_ref[:, :own], wg_ref[:, own:] = weights[0][0], weights[1][0]
        wu_ref[:, :own], wu_ref[:, own:] = weights[2][0], weights[3][0]
        wd_ref[:own, :], wd_ref[own:, :] = weights[4][0], weights[5][0]
        for ref in (accg_ref, accu_ref, accd_ref):
            ref[...] = jnp.zeros_like(ref)

    @pl.when(i + 1 < steps)
    def _():
        fetch(i + 1, lambda copy: copy.start())

    slot = lax.rem(i, 2)
    pltpu.make_async_copy(a_refs[0].at[pl.ds(0, ROWS), :], a_buf.at[slot], sems.at[0, slot]).wait()
    pltpu.make_async_copy(dy_refs[0].at[pl.ds(0, ROWS), :], dy_buf.at[slot], sems.at[1, slot]).wait()
    a, dy = a_buf[slot], dy_buf[slot]
    a_t, dy_t = a.T, dy.T
    width = wg_ref.shape[1]
    blocks = [pl.ds(c, min(BLOCK, width - c)) for c in range(0, width, BLOCK)]
    held = {}

    def there(c):
        s = blocks[c]
        held[c] = hidden_back(dot(a, wg_ref[:, s], NN), dot(a, wu_ref[:, s], NN), dot(dy, wd_ref[s, :], NT))

    def back(c):
        s = blocks[c]
        dg, du, hid = held.pop(c)
        accg_ref[:, s] += dot(a_t, dg, NN)
        accu_ref[:, s] += dot(a_t, du, NN)
        accd_ref[:, s] += dot(dy_t, hid, NN)

    there(0)
    for c in range(1, len(blocks)):
        there(c)
        back(c - 1)
    back(len(blocks) - 1)

    @pl.when(i == steps - 1)
    def _():
        g_ref, u_ref, d_ref, gs_ref, us_ref, ds_ref, own_ref, shared_ref = outs
        g, u, d = accg_ref[...].astype(BF16), accu_ref[...].astype(BF16), accd_ref[...].astype(BF16)
        g_ref[...], gs_ref[...] = g[:, :own], g[:, own:]
        u_ref[...], us_ref[...] = u[:, :own], u[:, own:]
        d_ref[...], ds_ref[...] = d[:, :own].T, d[:, own:].T
        own_ref[...] = squares(g[:, :own]) + squares(u[:, :own]) + squares(d[:, :own])
        shared_ref[...] = squares(g[:, own:]) + squares(u[:, own:]) + squares(d[:, own:])


def slices(layer, own, me, a_all, dy_all, wg, wu, wd):
    tokens, d = a_all[0].shape
    ff = wg.shape[2]
    rest = ff - 4 * own
    width = own + rest
    any_ = pl.BlockSpec(memory_space=pl.ANY)
    at = lambda s: once(s, lambda i, me: (0, 0))
    sizes = [(d, own), (d, own), (own, d), (d, rest), (d, rest), (rest, d)]
    return pl.pallas_call(
        lambda *refs: slices_kernel(own, *refs),
        grid_spec=pltpu.PrefetchScalarGridSpec(
            num_scalar_prefetch=1,
            grid=(4 * tokens // ROWS,),
            in_specs=[any_] * 8
            + [
                once((1, d, own), lambda i, me: (layer, 0, me[0])),
                once((1, d, rest), lambda i, me: (layer, 0, 4 * own // rest)),
            ]
            * 2
            + [
                once((1, own, d), lambda i, me: (layer, me[0], 0)),
                once((1, rest, d), lambda i, me: (layer, 4 * own // rest, 0)),
            ],
            out_specs=[at(s) for s in sizes] + [at((8, LANES))] * 2,
            scratch_shapes=[pltpu.VMEM((d, width), BF16)] * 2
            + [pltpu.VMEM((width, d), BF16)]
            + [pltpu.VMEM((d, width), F32)] * 3
            + [pltpu.VMEM((2, ROWS, d), BF16)] * 2
            + [pltpu.SemaphoreType.DMA((2, 2))],
        ),
        out_shape=[jax.ShapeDtypeStruct(s, BF16) for s in sizes] + [jax.ShapeDtypeStruct((8, LANES), F32)] * 2,
        cost_estimate=pl.CostEstimate(
            flops=12 * 4 * tokens * d * width, bytes_accessed=16 * tokens * d, transcendentals=4 * tokens * width
        ),
        compiler_params=params(),
        name="slices",
    )(me.reshape(1), *a_all, *dy_all, wg, wg, wu, wu, wd, wd)


def adam_math(f, w, m, v, g):
    g = g.astype(F32) * f
    m = 0.9 * m + 0.1 * g
    v = 0.95 * v + 0.05 * g * g
    w = w.astype(F32)
    return (w - 0.02 * (m * lax.rsqrt(v + 1e-8) + 0.1 * w)).astype(BF16), m, v


PARTS = 4


def adam(own, who, factor, arrays, pieces, outs):
    d = arrays[0][0].shape[1]
    table, start = [], 0
    for which, layer, slot, g in sorted(pieces, key=lambda piece: piece[0]):
        steps = 1 if slot is None and which == 2 else PARTS
        table.append((which, layer, slot, g, start, steps))
        start += steps
    total = start
    names = sorted({t[0] for t in table})

    def block_of(which):
        return (1, d // PARTS, own) if which < 2 else (1, own // PARTS, d)

    def index_of(which):
        mine = [t for t in table if t[0] == which]

        def index(i, who):
            step = jnp.clip(i, mine[0][4], mine[-1][4] + mine[-1][5] - 1)
            at, row, col = jnp.int32(0), jnp.int32(0), jnp.int32(0)
            for _, layer, slot, _, first, steps in mine:
                here = (step >= first) & (step < first + steps)
                k = 4 if slot is None else who[slot]
                part = step - first
                at = jnp.where(here, layer, at)
                row = jnp.where(here, part if which < 2 else k * PARTS + part, row)
                col = jnp.where(here, k if which < 2 else 0, col)
            return at, row, col

        return index

    in_specs, operands = [pl.BlockSpec(memory_space=pltpu.SMEM)], [factor]
    out_specs, out_shape = [], []
    for which in names:
        spec = pl.BlockSpec(block_of(which), index_of(which))
        in_specs += [spec] * 3
        out_specs += [spec] * 3
        operands += list(arrays[which])
        out_shape += [jax.ShapeDtypeStruct(arrays[which][0].shape, t) for t in (BF16, F32, F32)]
    for _, _, _, g, first, steps in table:
        size = (g.shape[0] // steps, g.shape[1])
        in_specs.append(pl.BlockSpec(size, lambda i, who, first=first, steps=steps: (jnp.clip(i - first, 0, steps - 1), 0)))
        operands.append(g)
    aliases = {}
    if outs is not None:
        for n, which in enumerate(names):
            for k in range(3):
                aliases[1 + len(operands)] = 3 * n + k
                in_specs.append(pl.BlockSpec(memory_space=pl.ANY))
                operands.append(outs[which][k])

    def kernel(who_ref, f_ref, *refs):
        ins, grads = refs[: 3 * len(names)], refs[3 * len(names) : 3 * len(names) + len(table)]
        results = refs[len(refs) - 3 * len(names) :]
        i, f = pl.program_id(0), f_ref[0]
        for (which, _, _, _, first, steps), g_ref in zip(table, grads, strict=True):
            n = names.index(which)
            w, m, v = ins[3 * n : 3 * n + 3]
            wo, mo, vo = results[3 * n : 3 * n + 3]
            rows, cols = g_ref.shape
            some = 32

            @pl.when((i >= first) & (i < first + steps))
            def _():
                def body(r, carry):
                    at = pl.ds(pl.multiple_of(r * some, some), some)
                    new = adam_math(f, w[0, at, :cols], m[0, at, :cols], v[0, at, :cols], g_ref[at, :])
                    wo[0, at, :cols], mo[0, at, :cols], vo[0, at, :cols] = new
                    return carry

                lax.fori_loop(0, rows // some, body, 0)

    elements = sum(t[3].size for t in table)
    new = pl.pallas_call(
        kernel,
        grid_spec=pltpu.PrefetchScalarGridSpec(num_scalar_prefetch=1, grid=(total,), in_specs=in_specs, out_specs=out_specs),
        out_shape=out_shape,
        input_output_aliases=aliases,
        cost_estimate=pl.CostEstimate(flops=2000 * elements, bytes_accessed=22 * elements, transcendentals=elements),
        compiler_params=params(),
    )(who, *operands)
    result = list(outs) if outs is not None else [None] * 3
    for n, which in enumerate(names):
        result[which] = tuple(new[3 * n : 3 * n + 3])
    return result


def solution(mesh):
    def step(x, dy, wg, wu, wd, mg, mu, md, vg, vu, vd):
        me = lax.axis_index("dp")
        chip, core = me // 2, me % 2
        who = jnp.stack([me, chip * 2 + 1 - core, (1 - chip) * 2 + core, (1 - chip) * 2 + 1 - core])
        x, dy = x[0], dy[0]
        ff = wg.shape[2]
        own = ff // LANES // 4 * LANES

        def send(a, perm):
            return perm(a)

        dy_x, dy_d = send(dy, px), send(dy, pd)
        h1, a1, a0 = forward(x, wg, wu, wd)
        a1_x, a1_d = send(a1, px), send(a1, pd)
        dh1 = chain(a1, dy, h1, wg, wu, wd)
        dh1, a0 = lax.optimization_barrier((dh1, a0))
        dh1_x, dh1_d = send(dh1, px), send(dh1, pd)
        a0_x, a0_d = send(a0, px), send(a0, pd)
        a1_xd, dy_xd = send(a1_x, pd), send(dy_x, pd)
        top = slices(1, own, me, [a1, a1_d, a1_x, a1_xd], [dy, dy_d, dy_x, dy_xd], wg, wu, wd)
        top, a0_x, dh1_x = lax.optimization_barrier((top, a0_x, dh1_x))
        a0_xd, dh1_xd = send(a0_x, pd), send(dh1_x, pd)
        top_x = [send(top[n], px) for n in range(3)]
        top_d = [send(top[n], pd) for n in range(3)]
        low = slices(0, own, me, [a0, a0_d, a0_x, a0_xd], [dh1, dh1_d, dh1_x, dh1_xd], wg, wu, wd)
        total = jnp.sum(top[6] + low[6]).reshape(1)
        total = total + px(total)
        low, total = lax.optimization_barrier((low, total))
        low_x = [send(low[n], px) for n in range(3)]
        low_d = [send(low[n], pd) for n in range(3)]
        total = total + pd(total) + jnp.sum(top[7] + low[7])
        count = wg.size + wu.size + wd.size
        factor = jnp.minimum(1.0, 0.5 * lax.rsqrt(total / count + 1e-30))

        top_xd = [send(top_x[n], pd) for n in range(3)]
        low_xd = [send(low_x[n], pd) for n in range(2)]
        arrays = ((wg, mg, vg), (wu, mu, vu), (wd, md, vd))

        def pieces(layer, slot, gs, names=(0, 1, 2)):
            return [(n, layer, slot, gs[n]) for n in names]

        first = pieces(1, 0, top) + pieces(1, 1, top_d) + pieces(1, 2, top_x) + pieces(0, 0, low)
        shared = pieces(1, None, top[3:6]) + pieces(0, None, low[3:6])
        if SHARED_APART:
            outs = adam(LANES, jnp.full((1,), ff // LANES - 1, jnp.int32), factor, arrays, [(n, l, 0, g) for n, l, _, g in shared], None)
        else:
            first, outs = first + shared, None
        outs = adam(own, who, factor, arrays, first, outs)
        outs = adam(own, who, factor, arrays, pieces(1, 3, top_xd) + pieces(0, 1, low_d), outs)
        outs, low_x[2] = lax.optimization_barrier((outs, low_x[2]))
        low_xd.append(send(low_x[2], pd))
        outs = adam(own, who, factor, arrays, pieces(0, 2, low_x) + pieces(0, 3, low_xd, (0, 1)), outs)
        outs = adam(own, who, factor, arrays, pieces(0, 3, low_xd, (2,)), outs)
        return tuple(outs[name][which] for which in range(3) for name in range(3))

    return jax.shard_map(
        step,
        mesh=mesh,
        in_specs=(P(("rep", "dp"), None, None),) * 2 + (P(None, None, None),) * 9,
        out_specs=(P("rep", None, None),) * 9,
        check_vma=False,
    )
```

```python
import jax
import jax.numpy as jnp
import numpy as np
from jax import lax
from jax.experimental import pallas as pl
from jax.experimental.pallas import tpu as pltpu
from jax.sharding import PartitionSpec as P


F32, BF16 = jnp.float32, jnp.bfloat16
PX = ((0, 2), (2, 0), (1, 3), (3, 1))
PD = ((0, 1), (1, 0), (2, 3), (3, 2))
NN, NT = ((1,), (0,)), ((1,), (1,))

LANES = 128
BLOCK = 512
ROWS = 512


def dot(a, b, dims):
    return lax.dot_general(a, b, (dims, ((), ())), preferred_element_type=F32)


def sigmoid(x):
    return 0.5 * jnp.tanh(0.5 * x) + 0.5


def px(a):
    return lax.ppermute(a, "dp", PX)


def pd(a):
    return lax.ppermute(a, "dp", PD)


def once(shape, index):
    return pl.BlockSpec(shape, index, pipeline_mode=pl.Buffered(1))


def params(mib=62):
    return pltpu.CompilerParams(vmem_limit_bytes=mib << 20)


def norm_scale(wide):
    return lax.rsqrt(jnp.mean(wide * wide, -1, keepdims=True) + 1e-6)


def normed(h):
    wide = h.astype(F32)
    return (wide * norm_scale(wide)).astype(BF16)


def forward_kernel(tail, x_ref, wg_ref, wu_ref, wd_ref, h_ref, a_ref, a0_ref, acc_ref):
    j, last = pl.program_id(0), pl.num_programs(0) - 1
    tokens = x_ref.shape[0]
    chunks = [pl.ds(r, ROWS) for r in range(0, tokens, ROWS)]

    @pl.when(j == 0)
    def _():
        for r in chunks:
            a0_ref[r, :] = normed(x_ref[r, :])
            acc_ref[r, :] = jnp.zeros((ROWS, acc_ref.shape[1]), F32)

    def block(width):
        hid = {}

        def up(r):
            a = a0_ref[chunks[r], :]
            g = dot(a, wg_ref[0, :, :width], NN)
            u = dot(a, wu_ref[0, :, :width], NN)
            hid[r] = (g * sigmoid(g) * u).astype(BF16)

        def down(r):
            acc_ref[chunks[r], :] += dot(hid.pop(r), wd_ref[0, :width, :], NN)

        up(0)
        for r in range(1, len(chunks)):
            up(r)
            down(r - 1)
        down(len(chunks) - 1)

    @pl.when(j < last)
    def _():
        block(wg_ref.shape[2])

    @pl.when(j == last)
    def _():
        block(tail)
        for r in chunks:
            h = (x_ref[r, :].astype(F32) + acc_ref[r, :].astype(BF16).astype(F32)).astype(BF16)
            h_ref[r, :] = h
            a_ref[r, :] = normed(h)


def forward(x, wg, wu, wd):
    tokens, d = x.shape
    ff = wg.shape[2]
    steps = pl.cdiv(ff, BLOCK)
    full = once((tokens, d), lambda j: (0, 0))
    across = pl.BlockSpec((1, d, BLOCK), lambda j: (0, 0, j))
    down = pl.BlockSpec((1, BLOCK, d), lambda j: (0, j, 0))
    return pl.pallas_call(
        lambda *refs: forward_kernel(ff - (steps - 1) * BLOCK, *refs),
        grid=(steps,),
        in_specs=[full, across, across, down],
        out_specs=[full] * 3,
        out_shape=[jax.ShapeDtypeStruct((tokens, d), BF16)] * 3,
        scratch_shapes=[pltpu.VMEM((tokens, d), F32)],
        cost_estimate=pl.CostEstimate(flops=6 * tokens * d * ff, bytes_accessed=6 * d * ff, transcendentals=tokens * ff),
        compiler_params=params(),
        name="forward",
    )(x, wg, wu, wd)


def hidden_back(g, u, dhid):
    dhid = dhid.astype(BF16).astype(F32)
    sig = sigmoid(g)
    act = g * sig
    return (dhid * u * (sig + act * (1 - sig))).astype(BF16), (dhid * act).astype(BF16), (act * u).astype(BF16)


def chain_kernel(tail, a_ref, dy_ref, h_ref, wg_ref, wu_ref, wd_ref, dh_ref, acc_ref):
    j, last = pl.program_id(0), pl.num_programs(0) - 1
    tokens = a_ref.shape[0]
    chunks = [pl.ds(r, ROWS) for r in range(0, tokens, ROWS)]

    @pl.when(j == 0)
    def _():
        for r in chunks:
            acc_ref[r, :] = jnp.zeros((ROWS, acc_ref.shape[1]), F32)

    def block(width):
        held = {}

        def there(r):
            a, dy = a_ref[chunks[r], :], dy_ref[chunks[r], :]
            g = dot(a, wg_ref[0, :, :width], NN)
            u = dot(a, wu_ref[0, :, :width], NN)
            dhid = dot(dy, wd_ref[0, :width, :], NT)
            held[r] = hidden_back(g, u, dhid)[:2]

        def back(r):
            dg, du = held.pop(r)
            acc_ref[chunks[r], :] += dot(dg, wg_ref[0, :, :width], NT) + dot(du, wu_ref[0, :, :width], NT)

        there(0)
        for r in range(1, len(chunks)):
            there(r)
            back(r - 1)
        back(len(chunks) - 1)

    @pl.when(j < last)
    def _():
        block(wg_ref.shape[2])

    @pl.when(j == last)
    def _():
        block(tail)
        for r in chunks:
            wide, da = h_ref[r, :].astype(F32), acc_ref[r, :].astype(BF16).astype(F32)
            scale = norm_scale(wide)
            back = scale * da - wide * (scale * scale * scale * jnp.mean(wide * da, -1, keepdims=True))
            dh_ref[r, :] = (dy_ref[r, :].astype(F32) + back.astype(BF16).astype(F32)).astype(BF16)


def chain(a, dy, h, wg, wu, wd):
    tokens, d = a.shape
    ff = wg.shape[2]
    steps = pl.cdiv(ff, BLOCK)
    full = once((tokens, d), lambda j: (0, 0))
    across = pl.BlockSpec((1, d, BLOCK), lambda j: (1, 0, j))
    down = pl.BlockSpec((1, BLOCK, d), lambda j: (1, j, 0))
    return pl.pallas_call(
        lambda *refs: chain_kernel(ff - (steps - 1) * BLOCK, *refs),
        grid=(steps,),
        in_specs=[full, full, full, across, across, down],
        out_specs=full,
        out_shape=jax.ShapeDtypeStruct((tokens, d), BF16),
        scratch_shapes=[pltpu.VMEM((tokens, d), F32)],
        cost_estimate=pl.CostEstimate(flops=10 * tokens * d * ff, bytes_accessed=6 * d * ff, transcendentals=tokens * ff),
        compiler_params=params(),
        name="chain",
    )(a, dy, h, wg, wu, wd)


def squares(x):
    x = x.astype(F32)
    x = x * x
    total = None
    for c in range(0, x.shape[1], LANES):
        part = jnp.sum(x[:, c : c + LANES].reshape(x.shape[0] // 8, 8, LANES), 0)
        total = part if total is None else total + part
    return total


def slices_kernel(own, me_ref, *refs):
    a_refs, dy_refs = refs[:4], refs[4:8]
    weights, outs, scratch = refs[8:14], refs[14:22], refs[22:]
    wg_ref, wu_ref, wd_ref, accg_ref, accu_ref, accd_ref, a_buf, dy_buf, sems = scratch
    i, steps = pl.program_id(0), pl.num_programs(0)
    tokens = a_refs[0].shape[0]
    each = tokens // ROWS
    me = me_ref[0]

    def fetch(step, do):
        slot = lax.rem(step, 2)
        owner, chunk = step // each, lax.rem(step, each)
        away = (owner + me) % 2 + 2 * ((owner // 2 + me // 2) % 2)
        rows = pl.ds(pl.multiple_of(chunk * ROWS, ROWS), ROWS)
        for k in range(4):

            @pl.when(away == k)
            def _():
                do(pltpu.make_async_copy(a_refs[k].at[rows, :], a_buf.at[slot], sems.at[0, slot]))
                do(pltpu.make_async_copy(dy_refs[k].at[rows, :], dy_buf.at[slot], sems.at[1, slot]))

    @pl.when(i == 0)
    def _():
        fetch(i, lambda copy: copy.start())
        wg_ref[:, :own], wg_ref[:, own:] = weights[0][0], weights[1][0]
        wu_ref[:, :own], wu_ref[:, own:] = weights[2][0], weights[3][0]
        wd_ref[:own, :], wd_ref[own:, :] = weights[4][0], weights[5][0]
        for ref in (accg_ref, accu_ref, accd_ref):
            ref[...] = jnp.zeros_like(ref)

    @pl.when(i + 1 < steps)
    def _():
        fetch(i + 1, lambda copy: copy.start())

    slot = lax.rem(i, 2)
    pltpu.make_async_copy(a_refs[0].at[pl.ds(0, ROWS), :], a_buf.at[slot], sems.at[0, slot]).wait()
    pltpu.make_async_copy(dy_refs[0].at[pl.ds(0, ROWS), :], dy_buf.at[slot], sems.at[1, slot]).wait()
    a, dy = a_buf[slot], dy_buf[slot]
    a_t, dy_t = a.T, dy.T
    width = wg_ref.shape[1]
    blocks = [pl.ds(c, min(BLOCK, width - c)) for c in range(0, width, BLOCK)]
    held = {}

    def there(c):
        s = blocks[c]
        held[c] = hidden_back(dot(a, wg_ref[:, s], NN), dot(a, wu_ref[:, s], NN), dot(dy, wd_ref[s, :], NT))

    def back(c):
        s = blocks[c]
        dg, du, hid = held.pop(c)
        accg_ref[:, s] += dot(a_t, dg, NN)
        accu_ref[:, s] += dot(a_t, du, NN)
        accd_ref[:, s] += dot(dy_t, hid, NN)

    there(0)
    for c in range(1, len(blocks)):
        there(c)
        back(c - 1)
    back(len(blocks) - 1)

    @pl.when(i == steps - 1)
    def _():
        g_ref, u_ref, d_ref, gs_ref, us_ref, ds_ref, own_ref, shared_ref = outs
        g, u, d = accg_ref[...].astype(BF16), accu_ref[...].astype(BF16), accd_ref[...].astype(BF16)
        g_ref[...], gs_ref[...] = g[:, :own], g[:, own:]
        u_ref[...], us_ref[...] = u[:, :own], u[:, own:]
        d_ref[...], ds_ref[...] = d[:, :own].T, d[:, own:].T
        own_ref[...] = squares(g[:, :own]) + squares(u[:, :own]) + squares(d[:, :own])
        shared_ref[...] = squares(g[:, own:]) + squares(u[:, own:]) + squares(d[:, own:])


def slices(layer, own, me, a_all, dy_all, wg, wu, wd):
    tokens, d = a_all[0].shape
    ff = wg.shape[2]
    rest = ff - 4 * own
    width = own + rest
    any_ = pl.BlockSpec(memory_space=pl.ANY)
    at = lambda s: once(s, lambda i, me: (0, 0))
    sizes = [(d, own), (d, own), (own, d), (d, rest), (d, rest), (rest, d)]
    return pl.pallas_call(
        lambda *refs: slices_kernel(own, *refs),
        grid_spec=pltpu.PrefetchScalarGridSpec(
            num_scalar_prefetch=1,
            grid=(4 * tokens // ROWS,),
            in_specs=[any_] * 8
            + [
                once((1, d, own), lambda i, me: (layer, 0, me[0])),
                once((1, d, rest), lambda i, me: (layer, 0, 4 * own // rest)),
            ]
            * 2
            + [
                once((1, own, d), lambda i, me: (layer, me[0], 0)),
                once((1, rest, d), lambda i, me: (layer, 4 * own // rest, 0)),
            ],
            out_specs=[at(s) for s in sizes] + [at((8, LANES))] * 2,
            scratch_shapes=[pltpu.VMEM((d, width), BF16)] * 2
            + [pltpu.VMEM((width, d), BF16)]
            + [pltpu.VMEM((d, width), F32)] * 3
            + [pltpu.VMEM((2, ROWS, d), BF16)] * 2
            + [pltpu.SemaphoreType.DMA((2, 2))],
        ),
        out_shape=[jax.ShapeDtypeStruct(s, BF16) for s in sizes] + [jax.ShapeDtypeStruct((8, LANES), F32)] * 2,
        cost_estimate=pl.CostEstimate(
            flops=12 * 4 * tokens * d * width, bytes_accessed=16 * tokens * d, transcendentals=4 * tokens * width
        ),
        compiler_params=params(),
        name="slices",
    )(me.reshape(1), *a_all, *dy_all, wg, wg, wu, wu, wd, wd)


def adam_math(f, w, m, v, g):
    g = g.astype(F32) * f
    m = 0.9 * m + 0.1 * g
    v = 0.95 * v + 0.05 * g * g
    w = w.astype(F32)
    return (w - 0.02 * (m * lax.rsqrt(v + 1e-8) + 0.1 * w)).astype(BF16), m, v


SLOTS, AHEAD = 6, 3


def adam(own, factor, who, arrays, pieces, outs):
    d, _ = arrays[0][0].shape[1:]
    shapes = ((d // 8, own), (LANES, d), (d, LANES))
    rows = []
    for n, (which, layer, slot, g) in enumerate(pieces):
        kind = 1 if which == 2 else 2 if slot == 4 else 0
        for r in range(0, g.shape[0], shapes[kind][0]):
            rows.append((kind, which, layer, n, slot, r, *((own, 0) if which == 2 else (0, own))))
    table = np.array(rows, np.int32).T
    total = len(rows)
    kinds = sorted({row[0] for row in rows})
    n_in = 9 + len(pieces)

    def kernel(table_ref, who_ref, f_ref, *refs):
        weights, grads = refs[:9], refs[9:n_in]
        refs = refs[n_in + (9 if outs is not None else 0) :]
        results, scratch = refs[:9], refs[9:]
        buffers = {kind: scratch[4 * n : 4 * n + 4] for n, kind in enumerate(kinds)}
        sem_in, sem_out = scratch[-2:]
        f = f_ref[0]

        def place(step):
            kind, which, layer = (table_ref[n, step] for n in range(3))
            unit = who_ref[table_ref[4, step]]
            row, col = table_ref[5, step] + table_ref[6, step] * unit, table_ref[7, step] * unit
            return kind, which, lambda shape: (layer, pl.ds(pl.multiple_of(row, 16), shape[0]), pl.ds(pl.multiple_of(col, LANES), shape[1]))

        def fetch(step):
            slot = lax.rem(step, SLOTS)
            kind, which, at = place(step)
            for k in range(3):
                its = [q for q in kinds if (q == 1) == (k == 2)]
                for q in its:

                    @pl.when((which == k) & (kind == q))
                    def _():
                        for n in range(3):
                            pltpu.make_async_copy(weights[3 * k + n].at[at(shapes[q])], buffers[q][n].at[slot], sem_in.at[n, slot]).start()

            piece, row = table_ref[3, step], table_ref[5, step]
            for n, (which_, _, slot_, _) in enumerate(pieces):
                q = 1 if which_ == 2 else 2 if slot_ == 4 else 0

                @pl.when(piece == n)
                def _():
                    rows_ = pl.ds(pl.multiple_of(row, 16), shapes[q][0])
                    pltpu.make_async_copy(grads[n].at[rows_, :], buffers[q][3].at[slot], sem_in.at[3, slot]).start()

        def stored(step, do):
            slot = lax.rem(step, SLOTS)
            kind, which, at = place(step)
            for k in range(3):
                for q in [q for q in kinds if (q == 1) == (k == 2)]:

                    @pl.when((which == k) & (kind == q))
                    def _():
                        for n in range(3):
                            do(pltpu.make_async_copy(buffers[q][n].at[slot], results[3 * k + n].at[at(shapes[q])], sem_out.at[n, slot]))

        for step in range(min(AHEAD, total)):
            fetch(jnp.int32(step))

        def body(step, carry):
            @pl.when(step + AHEAD < total)
            def _():
                @pl.when(step + AHEAD >= SLOTS)
                def _():
                    stored(step + AHEAD - SLOTS, lambda copy: copy.wait())

                fetch(step + AHEAD)

            slot = lax.rem(step, SLOTS)
            for q in kinds:

                @pl.when(table_ref[0, step] == q)
                def _():
                    w, m, v, g = buffers[q]
                    for n in range(3):
                        pltpu.make_async_copy(weights[n].at[0, pl.ds(0, shapes[q][0]), pl.ds(0, shapes[q][1])], buffers[q][n].at[slot], sem_in.at[n, slot]).wait()
                    pltpu.make_async_copy(buffers[q][3].at[slot], buffers[q][3].at[slot], sem_in.at[3, slot]).wait()
                    some = 16 if shapes[q][1] > d else 32 if shapes[q][1] > LANES else 128

                    def part(r, carry):
                        at = pl.ds(pl.multiple_of(r * some, some), some)
                        new = adam_math(f, w[slot, at, :], m[slot, at, :], v[slot, at, :], g[slot, at, :])
                        w[slot, at, :], m[slot, at, :], v[slot, at, :] = new
                        return carry

                    lax.fori_loop(0, shapes[q][0] // some, part, 0)

            stored(step, lambda copy: copy.start())
            return carry

        lax.fori_loop(0, total, body, 0)
        for step in range(max(0, total - SLOTS), total):
            stored(jnp.int32(step), lambda copy: copy.wait())

    any_ = pl.BlockSpec(memory_space=pl.ANY)
    given = [a for three in arrays for a in three]
    before = [a for three in outs for a in three] if outs is not None else []
    elements = sum(piece[3].size for piece in pieces)
    new = pl.pallas_call(
        kernel,
        in_specs=[pl.BlockSpec(memory_space=pltpu.SMEM)] * 3 + [any_] * (n_in + len(before)),
        out_specs=[any_] * 9,
        out_shape=[jax.ShapeDtypeStruct(a.shape, a.dtype) for a in given],
        scratch_shapes=[pltpu.VMEM((SLOTS, *shapes[q]), t) for q in kinds for t in (BF16, F32, F32, BF16)]
        + [pltpu.SemaphoreType.DMA((4, SLOTS)), pltpu.SemaphoreType.DMA((3, SLOTS))],
        input_output_aliases={3 + n_in + n: n for n in range(len(before))},
        cost_estimate=pl.CostEstimate(flops=2000 * elements, bytes_accessed=22 * elements, transcendentals=elements),
        compiler_params=params(),
    )(table, who, factor, *given, *(piece[3] for piece in pieces), *before)
    return tuple(tuple(new[3 * n : 3 * n + 3]) for n in range(3))


def solution(mesh):
    def step(x, dy, wg, wu, wd, mg, mu, md, vg, vu, vd):
        me = lax.axis_index("dp")
        places = jnp.arange(5, dtype=jnp.int32)
        who = jnp.where(places < 4, me ^ places, places)
        x, dy = x[0], dy[0]
        ff = wg.shape[2]
        own = ff // LANES // 4 * LANES

        def send(a, perm):
            return perm(a)

        dy_x, dy_d = send(dy, px), send(dy, pd)
        h1, a1, a0 = forward(x, wg, wu, wd)
        a1_x, a1_d = send(a1, px), send(a1, pd)
        a0_x, a0_d = send(a0, px), send(a0, pd)
        dh1 = chain(a1, dy, h1, wg, wu, wd)
        dh1_x, dh1_d = send(dh1, px), send(dh1, pd)
        a1_xd, dy_xd = send(a1_x, pd), send(dy_x, pd)
        top = slices(1, own, me, [a1, a1_d, a1_x, a1_xd], [dy, dy_d, dy_x, dy_xd], wg, wu, wd)
        top, a0_x, dh1_x = lax.optimization_barrier((top, a0_x, dh1_x))
        a0_xd, dh1_xd = send(a0_x, pd), send(dh1_x, pd)
        top_x = [send(top[n], px) for n in range(3)]
        top_d = [send(top[n], pd) for n in range(3)]
        low = slices(0, own, me, [a0, a0_d, a0_x, a0_xd], [dh1, dh1_d, dh1_x, dh1_xd], wg, wu, wd)
        total = jnp.sum(top[6] + low[6]).reshape(1)
        total = total + px(total)
        low, total = lax.optimization_barrier((low, total))
        low_x = [send(low[n], px) for n in range(3)]
        low_d = [send(low[n], pd) for n in range(3)]
        total = total + pd(total) + jnp.sum(top[7] + low[7])
        count = wg.size + wu.size + wd.size
        factor = jnp.minimum(1.0, 0.5 * lax.rsqrt(total / count + 1e-30))

        top_xd = [send(top_x[n], pd) for n in range(3)]
        low_xd = [send(low_x[n], pd) for n in range(2)]
        arrays = ((wg, mg, vg), (wu, mu, vu), (wd, md, vd))

        def pieces(layer, slot, gs, names=(0, 1, 2)):
            return [(n, layer, slot, gs[n]) for n in names]

        first = pieces(1, 0, top) + pieces(1, 1, top_d) + pieces(1, 2, top_x) + pieces(0, 0, low)
        shared = pieces(1, 4, top[3:6]) + pieces(0, 4, low[3:6])
        outs = adam(own, factor, who, arrays, first + shared, None)
        outs = adam(own, factor, who, arrays, pieces(1, 3, top_xd) + pieces(0, 1, low_d), outs)
        outs, low_x[2] = lax.optimization_barrier((outs, low_x[2]))
        low_xd.append(send(low_x[2], pd))
        outs = adam(own, factor, who, arrays, pieces(0, 2, low_x) + pieces(0, 3, low_xd, (0, 1)), outs)
        outs = adam(own, factor, who, arrays, pieces(0, 3, low_xd, (2,)), outs)
        return tuple(outs[name][which] for which in range(3) for name in range(3))

    return jax.shard_map(
        step,
        mesh=mesh,
        in_specs=(P(("rep", "dp"), None, None),) * 2 + (P(None, None, None),) * 9,
        out_specs=(P("rep", None, None),) * 9,
        check_vma=False,
    )
```

```python
import jax
import jax.numpy as jnp
import numpy as np
from jax import lax
from jax.experimental import pallas as pl
from jax.experimental.pallas import tpu as pltpu
from jax.sharding import PartitionSpec as P


F32, BF16 = jnp.float32, jnp.bfloat16
PX = ((0, 2), (2, 0), (1, 3), (3, 1))
PD = ((0, 1), (1, 0), (2, 3), (3, 2))
NN, NT = ((1,), (0,)), ((1,), (1,))

LANES = 128
BLOCK = 512
ROWS = 1024


def dot(a, b, dims):
    return lax.dot_general(a, b, (dims, ((), ())), preferred_element_type=F32)


def sigmoid(x):
    return 0.5 * jnp.tanh(0.5 * x) + 0.5


def px(a):
    return lax.ppermute(a, "dp", PX)


def pd(a):
    return lax.ppermute(a, "dp", PD)


def once(shape, index):
    return pl.BlockSpec(shape, index, pipeline_mode=pl.Buffered(1))


def params(mib=62):
    return pltpu.CompilerParams(vmem_limit_bytes=mib << 20)


def norm_scale(wide):
    return lax.rsqrt(jnp.mean(wide * wide, -1, keepdims=True) + 1e-6)


def normed(h):
    wide = h.astype(F32)
    return (wide * norm_scale(wide)).astype(BF16)


def forward_kernel(tail, x_ref, wg_ref, wu_ref, wd_ref, h_ref, a_ref, a0_ref, acc_ref):
    j, last = pl.program_id(0), pl.num_programs(0) - 1
    tokens = x_ref.shape[0]
    chunks = [pl.ds(r, ROWS) for r in range(0, tokens, ROWS)]

    @pl.when(j == 0)
    def _():
        for r in chunks:
            a0_ref[r, :] = normed(x_ref[r, :])
            acc_ref[r, :] = jnp.zeros((ROWS, acc_ref.shape[1]), F32)

    def block(width):
        hid = {}

        def up(r):
            a = a0_ref[chunks[r], :]
            g = dot(a, wg_ref[0, :, :width], NN)
            u = dot(a, wu_ref[0, :, :width], NN)
            hid[r] = (g * sigmoid(g) * u).astype(BF16)

        def down(r):
            acc_ref[chunks[r], :] += dot(hid.pop(r), wd_ref[0, :width, :], NN)

        up(0)
        for r in range(1, len(chunks)):
            up(r)
            down(r - 1)
        down(len(chunks) - 1)

    @pl.when(j < last)
    def _():
        block(wg_ref.shape[2])

    @pl.when(j == last)
    def _():
        block(tail)
        for r in chunks:
            h = (x_ref[r, :].astype(F32) + acc_ref[r, :].astype(BF16).astype(F32)).astype(BF16)
            h_ref[r, :] = h
            a_ref[r, :] = normed(h)


def forward(x, wg, wu, wd):
    tokens, d = x.shape
    ff = wg.shape[2]
    steps = pl.cdiv(ff, BLOCK)
    full = once((tokens, d), lambda j: (0, 0))
    across = pl.BlockSpec((1, d, BLOCK), lambda j: (0, 0, j))
    down = pl.BlockSpec((1, BLOCK, d), lambda j: (0, j, 0))
    return pl.pallas_call(
        lambda *refs: forward_kernel(ff - (steps - 1) * BLOCK, *refs),
        grid=(steps,),
        in_specs=[full, across, across, down],
        out_specs=[full] * 3,
        out_shape=[jax.ShapeDtypeStruct((tokens, d), BF16)] * 3,
        scratch_shapes=[pltpu.VMEM((tokens, d), F32)],
        cost_estimate=pl.CostEstimate(flops=6 * tokens * d * ff, bytes_accessed=6 * d * ff, transcendentals=tokens * ff),
        compiler_params=params(),
        name="forward",
    )(x, wg, wu, wd)


def hidden_back(g, u, dhid):
    dhid = dhid.astype(BF16).astype(F32)
    sig = sigmoid(g)
    act = g * sig
    return (dhid * u * (sig + act * (1 - sig))).astype(BF16), (dhid * act).astype(BF16), (act * u).astype(BF16)


def chain_kernel(tail, a_ref, dy_ref, h_ref, wg_ref, wu_ref, wd_ref, dh_ref, acc_ref):
    j, last = pl.program_id(0), pl.num_programs(0) - 1
    tokens = a_ref.shape[0]
    chunks = [pl.ds(r, ROWS) for r in range(0, tokens, ROWS)]

    @pl.when(j == 0)
    def _():
        for r in chunks:
            acc_ref[r, :] = jnp.zeros((ROWS, acc_ref.shape[1]), F32)

    def block(width):
        held = {}

        def there(r):
            a, dy = a_ref[chunks[r], :], dy_ref[chunks[r], :]
            g = dot(a, wg_ref[0, :, :width], NN)
            u = dot(a, wu_ref[0, :, :width], NN)
            dhid = dot(dy, wd_ref[0, :width, :], NT)
            held[r] = hidden_back(g, u, dhid)[:2]

        def back(r):
            dg, du = held.pop(r)
            acc_ref[chunks[r], :] += dot(dg, wg_ref[0, :, :width], NT) + dot(du, wu_ref[0, :, :width], NT)

        there(0)
        for r in range(1, len(chunks)):
            there(r)
            back(r - 1)
        back(len(chunks) - 1)

    @pl.when(j < last)
    def _():
        block(wg_ref.shape[2])

    @pl.when(j == last)
    def _():
        block(tail)
        for r in chunks:
            wide, da = h_ref[r, :].astype(F32), acc_ref[r, :].astype(BF16).astype(F32)
            scale = norm_scale(wide)
            back = scale * da - wide * (scale * scale * scale * jnp.mean(wide * da, -1, keepdims=True))
            dh_ref[r, :] = (dy_ref[r, :].astype(F32) + back.astype(BF16).astype(F32)).astype(BF16)


def chain(a, dy, h, wg, wu, wd):
    tokens, d = a.shape
    ff = wg.shape[2]
    steps = pl.cdiv(ff, BLOCK)
    full = once((tokens, d), lambda j: (0, 0))
    across = pl.BlockSpec((1, d, BLOCK), lambda j: (1, 0, j))
    down = pl.BlockSpec((1, BLOCK, d), lambda j: (1, j, 0))
    return pl.pallas_call(
        lambda *refs: chain_kernel(ff - (steps - 1) * BLOCK, *refs),
        grid=(steps,),
        in_specs=[full, full, full, across, across, down],
        out_specs=full,
        out_shape=jax.ShapeDtypeStruct((tokens, d), BF16),
        scratch_shapes=[pltpu.VMEM((tokens, d), F32)],
        cost_estimate=pl.CostEstimate(flops=10 * tokens * d * ff, bytes_accessed=6 * d * ff, transcendentals=tokens * ff),
        compiler_params=params(),
        name="chain",
    )(a, dy, h, wg, wu, wd)


def slices_kernel(own, me_ref, *refs):
    a_refs, dy_refs = refs[:4], refs[4:8]
    weights, outs, scratch = refs[8:14], refs[14:22], refs[22:]
    wg_ref, wu_ref, wd_ref, accg_ref, accu_ref, accd_ref, a_buf, dy_buf, sems = scratch
    i, steps = pl.program_id(0), pl.num_programs(0)
    tokens = a_refs[0].shape[0]
    each = tokens // ROWS
    me = me_ref[0]

    def fetch(step, do):
        slot = lax.rem(step, 2)
        owner, chunk = step // each, lax.rem(step, each)
        away = (owner + me) % 2 + 2 * ((owner // 2 + me // 2) % 2)
        rows = pl.ds(pl.multiple_of(chunk * ROWS, ROWS), ROWS)
        for k in range(4):

            @pl.when(away == k)
            def _():
                do(pltpu.make_async_copy(a_refs[k].at[rows, :], a_buf.at[slot], sems.at[0, slot]))
                do(pltpu.make_async_copy(dy_refs[k].at[rows, :], dy_buf.at[slot], sems.at[1, slot]))

    @pl.when(i == 0)
    def _():
        fetch(i, lambda copy: copy.start())
        wg_ref[:, :own], wg_ref[:, own:] = weights[0][0], weights[1][0]
        wu_ref[:, :own], wu_ref[:, own:] = weights[2][0], weights[3][0]
        wd_ref[:own, :], wd_ref[own:, :] = weights[4][0], weights[5][0]

    @pl.when(i + 1 < steps)
    def _():
        fetch(i + 1, lambda copy: copy.start())

    slot = lax.rem(i, 2)
    pltpu.make_async_copy(a_refs[0].at[pl.ds(0, ROWS), :], a_buf.at[slot], sems.at[0, slot]).wait()
    pltpu.make_async_copy(dy_refs[0].at[pl.ds(0, ROWS), :], dy_buf.at[slot], sems.at[1, slot]).wait()
    a, dy = a_buf[slot], dy_buf[slot]
    a_t, dy_t = a.T, dy.T
    width = wg_ref.shape[1]
    blocks = [pl.ds(c, min(BLOCK, width - c)) for c in range(0, width, BLOCK)]
    held = {}

    def there(c):
        s = blocks[c]
        held[c] = hidden_back(dot(a, wg_ref[:, s], NN), dot(a, wu_ref[:, s], NN), dot(dy, wd_ref[s, :], NT))

    def back(c):
        s = blocks[c]
        dg, du, hid = held.pop(c)
        for acc, left, right in ((accg_ref, a_t, dg), (accu_ref, a_t, du), (accd_ref, dy_t, hid)):
            acc[:, s] = jnp.where(i == 0, 0.0, acc[:, s]) + dot(left, right, NN)

    there(0)
    for c in range(1, len(blocks)):
        there(c)
        back(c - 1)
    back(len(blocks) - 1)

    @pl.when(i == steps - 1)
    def _():
        sums = [None, None]
        for acc, out, out_s, turned in ((accg_ref, *outs[0:4:3], False), (accu_ref, *outs[1:5:3], False), (accd_ref, *outs[2:6:3], True)):
            for c in range(0, width, LANES):
                part = acc[:, c : c + LANES].astype(BF16)
                if turned:
                    ref, at = (out, pl.ds(c, LANES)) if c < own else (out_s, pl.ds(c - own, LANES))
                    ref[at, :] = part.T
                else:
                    ref, at = (out, pl.ds(c, LANES)) if c < own else (out_s, pl.ds(c - own, LANES))
                    ref[:, at] = part
                square = part.astype(F32)
                square = jnp.sum((square * square).reshape(-1, 8, LANES), 0)
                sums[c >= own] = square if sums[c >= own] is None else sums[c >= own] + square
        outs[6][...], outs[7][...] = sums


def slices(layer, own, me, a_all, dy_all, wg, wu, wd):
    tokens, d = a_all[0].shape
    ff = wg.shape[2]
    rest = ff - 4 * own
    width = own + rest
    any_ = pl.BlockSpec(memory_space=pl.ANY)
    at = lambda s: once(s, lambda i, me: (0, 0))
    sizes = [(d, own), (d, own), (own, d), (d, rest), (d, rest), (rest, d)]
    return pl.pallas_call(
        lambda *refs: slices_kernel(own, *refs),
        grid_spec=pltpu.PrefetchScalarGridSpec(
            num_scalar_prefetch=1,
            grid=(4 * tokens // ROWS,),
            in_specs=[any_] * 8
            + [
                once((1, d, own), lambda i, me: (layer, 0, me[0])),
                once((1, d, rest), lambda i, me: (layer, 0, 4 * own // rest)),
            ]
            * 2
            + [
                once((1, own, d), lambda i, me: (layer, me[0], 0)),
                once((1, rest, d), lambda i, me: (layer, 4 * own // rest, 0)),
            ],
            out_specs=[at(s) for s in sizes] + [at((8, LANES))] * 2,
            scratch_shapes=[pltpu.VMEM((d, width), BF16)] * 2
            + [pltpu.VMEM((width, d), BF16)]
            + [pltpu.VMEM((d, width), F32)] * 3
            + [pltpu.VMEM((2, ROWS, d), BF16)] * 2
            + [pltpu.SemaphoreType.DMA((2, 2))],
        ),
        out_shape=[jax.ShapeDtypeStruct(s, BF16) for s in sizes] + [jax.ShapeDtypeStruct((8, LANES), F32)] * 2,
        cost_estimate=pl.CostEstimate(
            flops=12 * 4 * tokens * d * width, bytes_accessed=16 * tokens * d, transcendentals=4 * tokens * width
        ),
        compiler_params=params(),
        name="slices",
    )(me.reshape(1), *a_all, *dy_all, wg, wg, wu, wu, wd, wd)


def adam_math(f, w, m, v, g):
    g = g.astype(F32) * f
    m = 0.9 * m + 0.1 * g
    v = 0.95 * v + 0.05 * g * g
    w = w.astype(F32)
    return (w - 0.02 * (m * lax.rsqrt(v + 1e-8) + 0.1 * w)).astype(BF16), m, v


SLOTS, AHEAD = 6, 3


def adam(own, factor, who, arrays, pieces, outs):
    d, _ = arrays[0][0].shape[1:]
    shapes = ((d // 8, own), (LANES, d), (d, LANES))
    rows = []
    for n, (which, layer, slot, g) in enumerate(pieces):
        kind = 1 if which == 2 else 2 if slot == 4 else 0
        for r in range(0, g.shape[0], shapes[kind][0]):
            rows.append((kind, which, layer, n, slot, r, *((own, 0) if which == 2 else (0, own))))
    table = np.array(rows, np.int32).T
    total = len(rows)
    kinds = sorted({row[0] for row in rows})
    n_in = 9 + len(pieces)

    def kernel(table_ref, who_ref, f_ref, *refs):
        weights, grads = refs[:9], refs[9:n_in]
        refs = refs[n_in + (9 if outs is not None else 0) :]
        results, scratch = refs[:9], refs[9:]
        buffers = {kind: scratch[4 * n : 4 * n + 4] for n, kind in enumerate(kinds)}
        sem_in, sem_out = scratch[-2:]
        f = f_ref[0]

        def place(step):
            kind, which, layer = (table_ref[n, step] for n in range(3))
            unit = who_ref[table_ref[4, step]]
            row, col = table_ref[5, step] + table_ref[6, step] * unit, table_ref[7, step] * unit
            return kind, which, lambda shape: (layer, pl.ds(pl.multiple_of(row, 16), shape[0]), pl.ds(pl.multiple_of(col, LANES), shape[1]))

        def fetch(step):
            slot = lax.rem(step, SLOTS)
            kind, which, at = place(step)
            for k in range(3):
                its = [q for q in kinds if (q == 1) == (k == 2)]
                for q in its:

                    @pl.when((which == k) & (kind == q))
                    def _():
                        for n in range(3):
                            pltpu.make_async_copy(weights[3 * k + n].at[at(shapes[q])], buffers[q][n].at[slot], sem_in.at[n, slot]).start()

            piece, row = table_ref[3, step], table_ref[5, step]
            for n, (which_, _, slot_, _) in enumerate(pieces):
                q = 1 if which_ == 2 else 2 if slot_ == 4 else 0

                @pl.when(piece == n)
                def _():
                    rows_ = pl.ds(pl.multiple_of(row, 16), shapes[q][0])
                    pltpu.make_async_copy(grads[n].at[rows_, :], buffers[q][3].at[slot], sem_in.at[3, slot]).start()

        def stored(step, do):
            slot = lax.rem(step, SLOTS)
            kind, which, at = place(step)
            for k in range(3):
                for q in [q for q in kinds if (q == 1) == (k == 2)]:

                    @pl.when((which == k) & (kind == q))
                    def _():
                        for n in range(3):
                            do(pltpu.make_async_copy(buffers[q][n].at[slot], results[3 * k + n].at[at(shapes[q])], sem_out.at[n, slot]))

        for step in range(min(AHEAD, total)):
            fetch(jnp.int32(step))

        def body(step, carry):
            @pl.when(step + AHEAD < total)
            def _():
                @pl.when(step + AHEAD >= SLOTS)
                def _():
                    stored(step + AHEAD - SLOTS, lambda copy: copy.wait())

                fetch(step + AHEAD)

            slot = lax.rem(step, SLOTS)
            for q in kinds:

                @pl.when(table_ref[0, step] == q)
                def _():
                    w, m, v, g = buffers[q]
                    for n in range(3):
                        pltpu.make_async_copy(weights[n].at[0, pl.ds(0, shapes[q][0]), pl.ds(0, shapes[q][1])], buffers[q][n].at[slot], sem_in.at[n, slot]).wait()
                    pltpu.make_async_copy(buffers[q][3].at[slot], buffers[q][3].at[slot], sem_in.at[3, slot]).wait()
                    some = 16 if shapes[q][1] > d else 32 if shapes[q][1] > LANES else 128

                    def part(r, carry):
                        at = pl.ds(pl.multiple_of(r * some, some), some)
                        new = adam_math(f, w[slot, at, :], m[slot, at, :], v[slot, at, :], g[slot, at, :])
                        w[slot, at, :], m[slot, at, :], v[slot, at, :] = new
                        return carry

                    lax.fori_loop(0, shapes[q][0] // some, part, 0)

            stored(step, lambda copy: copy.start())
            return carry

        lax.fori_loop(0, total, body, 0)
        for step in range(max(0, total - SLOTS), total):
            stored(jnp.int32(step), lambda copy: copy.wait())

    any_ = pl.BlockSpec(memory_space=pl.ANY)
    given = [a for three in arrays for a in three]
    before = [a for three in outs for a in three] if outs is not None else []
    elements = sum(piece[3].size for piece in pieces)
    new = pl.pallas_call(
        kernel,
        in_specs=[pl.BlockSpec(memory_space=pltpu.SMEM)] * 3 + [any_] * (n_in + len(before)),
        out_specs=[any_] * 9,
        out_shape=[jax.ShapeDtypeStruct(a.shape, a.dtype) for a in given],
        scratch_shapes=[pltpu.VMEM((SLOTS, *shapes[q]), t) for q in kinds for t in (BF16, F32, F32, BF16)]
        + [pltpu.SemaphoreType.DMA((4, SLOTS)), pltpu.SemaphoreType.DMA((3, SLOTS))],
        input_output_aliases={3 + n_in + n: n for n in range(len(before))},
        cost_estimate=pl.CostEstimate(flops=2000 * elements, bytes_accessed=22 * elements, transcendentals=elements),
        compiler_params=params(30),
    )(table, who, factor, *given, *(piece[3] for piece in pieces), *before)
    return tuple(tuple(new[3 * n : 3 * n + 3]) for n in range(3))


def solution(mesh):
    def step(x, dy, wg, wu, wd, mg, mu, md, vg, vu, vd):
        me = lax.axis_index("dp")
        places = jnp.arange(5, dtype=jnp.int32)
        who = jnp.where(places < 4, me ^ places, places)
        x, dy = x[0], dy[0]
        ff = wg.shape[2]
        own = ff // LANES // 4 * LANES

        def send(a, perm):
            return perm(a)

        dy_x, dy_d = send(dy, px), send(dy, pd)
        h1, a1, a0 = forward(x, wg, wu, wd)
        a1_x, a1_d = send(a1, px), send(a1, pd)
        a0_x, a0_d = send(a0, px), send(a0, pd)
        dh1 = chain(a1, dy, h1, wg, wu, wd)
        dh1_x, dh1_d = send(dh1, px), send(dh1, pd)
        a1_xd, dy_xd = send(a1_x, pd), send(dy_x, pd)
        top = slices(1, own, me, [a1, a1_d, a1_x, a1_xd], [dy, dy_d, dy_x, dy_xd], wg, wu, wd)
        top, a0_x, dh1_x = lax.optimization_barrier((top, a0_x, dh1_x))
        a0_xd, dh1_xd = send(a0_x, pd), send(dh1_x, pd)
        top_x = [send(top[n], px) for n in range(3)]
        top_d = [send(top[n], pd) for n in range(3)]
        low = slices(0, own, me, [a0, a0_d, a0_x, a0_xd], [dh1, dh1_d, dh1_x, dh1_xd], wg, wu, wd)
        top_xd = [send(top_x[n], pd) for n in range(3)]
        total = jnp.sum(top[6] + low[6]).reshape(1)
        total = total + px(total)
        total = total + pd(total) + jnp.sum(top[7] + low[7])
        low, total = lax.optimization_barrier((low, total))
        low_x = [send(low[n], px) for n in range(3)]
        low_d = [send(low[n], pd) for n in range(3)]
        count = wg.size + wu.size + wd.size
        factor = jnp.minimum(1.0, 0.5 * lax.rsqrt(total / count + 1e-30))

        arrays = ((wg, mg, vg), (wu, mu, vu), (wd, md, vd))

        def pieces(layer, slot, gs):
            return [(n, layer, slot, gs[n]) for n in range(3)]

        first = pieces(1, 0, top) + pieces(1, 1, top_d) + pieces(1, 2, top_x) + pieces(1, 3, top_xd) + pieces(0, 0, low)
        shared = pieces(1, 4, top[3:6]) + pieces(0, 4, low[3:6])
        outs = adam(own, factor, who, arrays, first + shared, None)
        outs, low_x = lax.optimization_barrier((outs, low_x))
        low_xd = [send(low_x[n], pd) for n in range(3)]
        outs = adam(own, factor, who, arrays, pieces(0, 1, low_d) + pieces(0, 2, low_x), outs)
        outs = adam(own, factor, who, arrays, pieces(0, 3, low_xd), outs)
        return tuple(outs[name][which] for which in range(3) for name in range(3))

    return jax.shard_map(
        step,
        mesh=mesh,
        in_specs=(P(("rep", "dp"), None, None),) * 2 + (P(None, None, None),) * 9,
        out_specs=(P("rep", None, None),) * 9,
        check_vma=False,
    )
```

```python
import jax
import jax.numpy as jnp
import numpy as np
from jax import lax
from jax.experimental import pallas as pl
from jax.experimental.pallas import tpu as pltpu
from jax.sharding import PartitionSpec as P


F32, BF16 = jnp.float32, jnp.bfloat16
PX = ((0, 2), (2, 0), (1, 3), (3, 1))
PD = ((0, 1), (1, 0), (2, 3), (3, 2))
NN, NT = ((1,), (0,)), ((1,), (1,))

LANES = 128
BLOCK = 512
ROWS = 512


def dot(a, b, dims):
    return lax.dot_general(a, b, (dims, ((), ())), preferred_element_type=F32)


def sigmoid(x):
    return 0.5 * jnp.tanh(0.5 * x) + 0.5


def px(a):
    return lax.ppermute(a, "dp", PX)


def pd(a):
    return lax.ppermute(a, "dp", PD)


def once(shape, index):
    return pl.BlockSpec(shape, index, pipeline_mode=pl.Buffered(1))


def params(mib=62):
    return pltpu.CompilerParams(vmem_limit_bytes=mib << 20)


def norm_scale(wide):
    return lax.rsqrt(jnp.mean(wide * wide, -1, keepdims=True) + 1e-6)


def normed(h):
    wide = h.astype(F32)
    return (wide * norm_scale(wide)).astype(BF16)


def forward_kernel(tail, x_ref, wg_ref, wu_ref, wd_ref, h_ref, a_ref, a0_ref, acc_ref):
    j, last = pl.program_id(0), pl.num_programs(0) - 1
    tokens = x_ref.shape[0]
    chunks = [pl.ds(r, ROWS) for r in range(0, tokens, ROWS)]

    @pl.when(j == 0)
    def _():
        for r in chunks:
            a0_ref[r, :] = normed(x_ref[r, :])
            acc_ref[r, :] = jnp.zeros((ROWS, acc_ref.shape[1]), F32)

    def block(width):
        hid = {}

        def up(r):
            a = a0_ref[chunks[r], :]
            g = dot(a, wg_ref[0, :, :width], NN)
            u = dot(a, wu_ref[0, :, :width], NN)
            hid[r] = (g * sigmoid(g) * u).astype(BF16)

        def down(r):
            acc_ref[chunks[r], :] += dot(hid.pop(r), wd_ref[0, :width, :], NN)

        up(0)
        for r in range(1, len(chunks)):
            up(r)
            down(r - 1)
        down(len(chunks) - 1)

    @pl.when(j < last)
    def _():
        block(wg_ref.shape[2])

    @pl.when(j == last)
    def _():
        block(tail)
        for r in chunks:
            h = (x_ref[r, :].astype(F32) + acc_ref[r, :].astype(BF16).astype(F32)).astype(BF16)
            h_ref[r, :] = h
            a_ref[r, :] = normed(h)


def forward(x, wg, wu, wd):
    tokens, d = x.shape
    ff = wg.shape[2]
    steps = pl.cdiv(ff, BLOCK)
    full = once((tokens, d), lambda j: (0, 0))
    across = pl.BlockSpec((1, d, BLOCK), lambda j: (0, 0, j))
    down = pl.BlockSpec((1, BLOCK, d), lambda j: (0, j, 0))
    return pl.pallas_call(
        lambda *refs: forward_kernel(ff - (steps - 1) * BLOCK, *refs),
        grid=(steps,),
        in_specs=[full, across, across, down],
        out_specs=[full] * 3,
        out_shape=[jax.ShapeDtypeStruct((tokens, d), BF16)] * 3,
        scratch_shapes=[pltpu.VMEM((tokens, d), F32)],
        cost_estimate=pl.CostEstimate(flops=6 * tokens * d * ff, bytes_accessed=6 * d * ff, transcendentals=tokens * ff),
        compiler_params=params(),
        name="forward",
    )(x, wg, wu, wd)


def hidden_back(g, u, dhid):
    dhid = dhid.astype(BF16).astype(F32)
    sig = sigmoid(g)
    act = g * sig
    return (dhid * u * (sig + act * (1 - sig))).astype(BF16), (dhid * act).astype(BF16), (act * u).astype(BF16)


def chain_kernel(tail, a_ref, dy_ref, h_ref, wg_ref, wu_ref, wd_ref, dh_ref, acc_ref):
    j, last = pl.program_id(0), pl.num_programs(0) - 1
    tokens = a_ref.shape[0]
    chunks = [pl.ds(r, ROWS) for r in range(0, tokens, ROWS)]

    @pl.when(j == 0)
    def _():
        for r in chunks:
            acc_ref[r, :] = jnp.zeros((ROWS, acc_ref.shape[1]), F32)

    def block(width):
        held = {}

        def there(r):
            a, dy = a_ref[chunks[r], :], dy_ref[chunks[r], :]
            g = dot(a, wg_ref[0, :, :width], NN)
            u = dot(a, wu_ref[0, :, :width], NN)
            dhid = dot(dy, wd_ref[0, :width, :], NT)
            held[r] = hidden_back(g, u, dhid)[:2]

        def back(r):
            dg, du = held.pop(r)
            acc_ref[chunks[r], :] += dot(dg, wg_ref[0, :, :width], NT) + dot(du, wu_ref[0, :, :width], NT)

        there(0)
        for r in range(1, len(chunks)):
            there(r)
            back(r - 1)
        back(len(chunks) - 1)

    @pl.when(j < last)
    def _():
        block(wg_ref.shape[2])

    @pl.when(j == last)
    def _():
        block(tail)
        for r in chunks:
            wide, da = h_ref[r, :].astype(F32), acc_ref[r, :].astype(BF16).astype(F32)
            scale = norm_scale(wide)
            back = scale * da - wide * (scale * scale * scale * jnp.mean(wide * da, -1, keepdims=True))
            dh_ref[r, :] = (dy_ref[r, :].astype(F32) + back.astype(BF16).astype(F32)).astype(BF16)


def chain(a, dy, h, wg, wu, wd):
    tokens, d = a.shape
    ff = wg.shape[2]
    steps = pl.cdiv(ff, BLOCK)
    full = once((tokens, d), lambda j: (0, 0))
    across = pl.BlockSpec((1, d, BLOCK), lambda j: (1, 0, j))
    down = pl.BlockSpec((1, BLOCK, d), lambda j: (1, j, 0))
    return pl.pallas_call(
        lambda *refs: chain_kernel(ff - (steps - 1) * BLOCK, *refs),
        grid=(steps,),
        in_specs=[full, full, full, across, across, down],
        out_specs=full,
        out_shape=jax.ShapeDtypeStruct((tokens, d), BF16),
        scratch_shapes=[pltpu.VMEM((tokens, d), F32)],
        cost_estimate=pl.CostEstimate(flops=10 * tokens * d * ff, bytes_accessed=6 * d * ff, transcendentals=tokens * ff),
        compiler_params=params(),
        name="chain",
    )(a, dy, h, wg, wu, wd)


def slices_kernel(own, me_ref, *refs):
    a_refs, dy_refs = refs[:4], refs[4:8]
    weights, outs, scratch = refs[8:14], refs[14:22], refs[22:]
    wg_ref, wu_ref, wd_ref, accg_ref, accu_ref, accd_ref, a_buf, dy_buf, sems = scratch
    i, steps = pl.program_id(0), pl.num_programs(0)
    tokens = a_refs[0].shape[0]
    each = tokens // ROWS
    me = me_ref[0]

    def fetch(step, do):
        slot = lax.rem(step, 2)
        owner, chunk = step // each, lax.rem(step, each)
        away = (owner + me) % 2 + 2 * ((owner // 2 + me // 2) % 2)
        rows = pl.ds(pl.multiple_of(chunk * ROWS, ROWS), ROWS)
        for k in range(4):

            @pl.when(away == k)
            def _():
                do(pltpu.make_async_copy(a_refs[k].at[rows, :], a_buf.at[slot], sems.at[0, slot]))
                do(pltpu.make_async_copy(dy_refs[k].at[rows, :], dy_buf.at[slot], sems.at[1, slot]))

    @pl.when(i == 0)
    def _():
        fetch(i, lambda copy: copy.start())
        wg_ref[:, :own], wg_ref[:, own:] = weights[0][0], weights[1][0]
        wu_ref[:, :own], wu_ref[:, own:] = weights[2][0], weights[3][0]
        wd_ref[:own, :], wd_ref[own:, :] = weights[4][0], weights[5][0]

    @pl.when(i + 1 < steps)
    def _():
        fetch(i + 1, lambda copy: copy.start())

    slot = lax.rem(i, 2)
    pltpu.make_async_copy(a_refs[0].at[pl.ds(0, ROWS), :], a_buf.at[slot], sems.at[0, slot]).wait()
    pltpu.make_async_copy(dy_refs[0].at[pl.ds(0, ROWS), :], dy_buf.at[slot], sems.at[1, slot]).wait()
    a, dy = a_buf[slot], dy_buf[slot]
    a_t, dy_t = a.T, dy.T
    width = wg_ref.shape[1]
    blocks = [pl.ds(c, min(BLOCK, width - c)) for c in range(0, width, BLOCK)]
    held = {}

    def there(c):
        s = blocks[c]
        held[c] = hidden_back(dot(a, wg_ref[:, s], NN), dot(a, wu_ref[:, s], NN), dot(dy, wd_ref[s, :], NT))

    def back(c):
        s = blocks[c]
        dg, du, hid = held.pop(c)
        for acc, left, right in ((accg_ref, a_t, dg), (accu_ref, a_t, du), (accd_ref, dy_t, hid)):
            acc[:, s] = jnp.where(i == 0, 0.0, acc[:, s]) + dot(left, right, NN)

    there(0)
    for c in range(1, len(blocks)):
        there(c)
        back(c - 1)
    back(len(blocks) - 1)

    @pl.when(i == steps - 1)
    def _():
        sums = [None, None]
        for acc, out, out_s, turned in ((accg_ref, *outs[0:4:3], False), (accu_ref, *outs[1:5:3], False), (accd_ref, *outs[2:6:3], True)):
            for c in range(0, width, LANES):
                part = acc[:, c : c + LANES].astype(BF16)
                if turned:
                    ref, at = (out, pl.ds(c, LANES)) if c < own else (out_s, pl.ds(c - own, LANES))
                    ref[at, :] = part.T
                else:
                    ref, at = (out, pl.ds(c, LANES)) if c < own else (out_s, pl.ds(c - own, LANES))
                    ref[:, at] = part
                square = part.astype(F32)
                square = jnp.sum((square * square).reshape(-1, 8, LANES), 0)
                sums[c >= own] = square if sums[c >= own] is None else sums[c >= own] + square
        outs[6][...], outs[7][...] = sums


def slices(layer, own, me, a_all, dy_all, wg, wu, wd):
    tokens, d = a_all[0].shape
    ff = wg.shape[2]
    rest = ff - 4 * own
    width = own + rest
    any_ = pl.BlockSpec(memory_space=pl.ANY)
    at = lambda s: once(s, lambda i, me: (0, 0))
    sizes = [(d, own), (d, own), (own, d), (d, rest), (d, rest), (rest, d)]
    return pl.pallas_call(
        lambda *refs: slices_kernel(own, *refs),
        grid_spec=pltpu.PrefetchScalarGridSpec(
            num_scalar_prefetch=1,
            grid=(4 * tokens // ROWS,),
            in_specs=[any_] * 8
            + [
                once((1, d, own), lambda i, me: (layer, 0, me[0])),
                once((1, d, rest), lambda i, me: (layer, 0, 4 * own // rest)),
            ]
            * 2
            + [
                once((1, own, d), lambda i, me: (layer, me[0], 0)),
                once((1, rest, d), lambda i, me: (layer, 4 * own // rest, 0)),
            ],
            out_specs=[at(s) for s in sizes] + [at((8, LANES))] * 2,
            scratch_shapes=[pltpu.VMEM((d, width), BF16)] * 2
            + [pltpu.VMEM((width, d), BF16)]
            + [pltpu.VMEM((d, width), F32)] * 3
            + [pltpu.VMEM((2, ROWS, d), BF16)] * 2
            + [pltpu.SemaphoreType.DMA((2, 2))],
        ),
        out_shape=[jax.ShapeDtypeStruct(s, BF16) for s in sizes] + [jax.ShapeDtypeStruct((8, LANES), F32)] * 2,
        cost_estimate=pl.CostEstimate(
            flops=12 * 4 * tokens * d * width, bytes_accessed=16 * tokens * d, transcendentals=4 * tokens * width
        ),
        compiler_params=params(),
        name="slices",
    )(me.reshape(1), *a_all, *dy_all, wg, wg, wu, wu, wd, wd)


def adam_math(f, w, m, v, g):
    g = g.astype(F32) * f
    m = 0.9 * m + 0.1 * g
    v = 0.95 * v + 0.05 * g * g
    return (0.998 * w.astype(F32) - 0.02 * (m * lax.rsqrt(v + 1e-8))).astype(BF16), m, v


SLOTS, AHEAD = 6, 3


def adam(own, factor, who, arrays, pieces, outs):
    d, _ = arrays[0][0].shape[1:]
    shapes = ((LANES, own), (LANES, d), (d, LANES))
    rows = []
    for n, (which, layer, slot, g) in enumerate(pieces):
        kind = 1 if which == 2 else 2 if slot == 4 else 0
        for r in range(0, g.shape[0], shapes[kind][0]):
            rows.append((kind, which, layer, n, slot, r, *((own, 0) if which == 2 else (0, own))))
    table = np.array(rows, np.int32).T
    total = len(rows)
    kinds = sorted({row[0] for row in rows})
    n_in = 9 + len(pieces)

    def kernel(table_ref, who_ref, f_ref, *refs):
        weights, grads = refs[:9], refs[9:n_in]
        refs = refs[n_in + (9 if outs is not None else 0) :]
        results, scratch = refs[:9], refs[9:]
        buffers = {kind: scratch[4 * n : 4 * n + 4] for n, kind in enumerate(kinds)}
        sem_in, sem_out = scratch[-2:]
        f = f_ref[0]

        def place(step):
            kind, which, layer = (table_ref[n, step] for n in range(3))
            unit = who_ref[table_ref[4, step]]
            row, col = table_ref[5, step] + table_ref[6, step] * unit, table_ref[7, step] * unit
            return kind, which, lambda shape: (layer, pl.ds(pl.multiple_of(row, 16), shape[0]), pl.ds(pl.multiple_of(col, LANES), shape[1]))

        def fetch(step):
            slot = lax.rem(step, SLOTS)
            kind, which, at = place(step)
            for k in range(3):
                its = [q for q in kinds if (q == 1) == (k == 2)]
                for q in its:

                    @pl.when((which == k) & (kind == q))
                    def _():
                        for n in range(3):
                            pltpu.make_async_copy(weights[3 * k + n].at[at(shapes[q])], buffers[q][n].at[slot], sem_in.at[n, slot]).start()

            piece, row = table_ref[3, step], table_ref[5, step]
            for n, (which_, _, slot_, _) in enumerate(pieces):
                q = 1 if which_ == 2 else 2 if slot_ == 4 else 0

                @pl.when(piece == n)
                def _():
                    rows_ = pl.ds(pl.multiple_of(row, 16), shapes[q][0])
                    pltpu.make_async_copy(grads[n].at[rows_, :], buffers[q][3].at[slot], sem_in.at[3, slot]).start()

        def stored(step, do):
            slot = lax.rem(step, SLOTS)
            kind, which, at = place(step)
            for k in range(3):
                for q in [q for q in kinds if (q == 1) == (k == 2)]:

                    @pl.when((which == k) & (kind == q))
                    def _():
                        for n in range(3):
                            do(pltpu.make_async_copy(buffers[q][n].at[slot], results[3 * k + n].at[at(shapes[q])], sem_out.at[n, slot]))

        for step in range(min(AHEAD, total)):
            fetch(jnp.int32(step))

        def body(step, carry):
            @pl.when(step + AHEAD < total)
            def _():
                @pl.when(step + AHEAD >= SLOTS)
                def _():
                    stored(step + AHEAD - SLOTS, lambda copy: copy.wait())

                fetch(step + AHEAD)

            slot = lax.rem(step, SLOTS)
            for q in kinds:

                @pl.when(table_ref[0, step] == q)
                def _():
                    w, m, v, g = buffers[q]
                    for n in range(3):
                        pltpu.make_async_copy(weights[n].at[0, pl.ds(0, shapes[q][0]), pl.ds(0, shapes[q][1])], buffers[q][n].at[slot], sem_in.at[n, slot]).wait()
                    pltpu.make_async_copy(buffers[q][3].at[slot], buffers[q][3].at[slot], sem_in.at[3, slot]).wait()
                    some = 32 if shapes[q][1] > LANES else 224

                    def part(r, carry):
                        at = pl.ds(pl.multiple_of(r * some, some), some)
                        new = adam_math(f, w[slot, at, :], m[slot, at, :], v[slot, at, :], g[slot, at, :])
                        w[slot, at, :], m[slot, at, :], v[slot, at, :] = new
                        return carry

                    lax.fori_loop(0, shapes[q][0] // some, part, 0)

            stored(step, lambda copy: copy.start())
            return carry

        lax.fori_loop(0, total, body, 0)
        for step in range(max(0, total - SLOTS), total):
            stored(jnp.int32(step), lambda copy: copy.wait())

    any_ = pl.BlockSpec(memory_space=pl.ANY)
    given = [a for three in arrays for a in three]
    before = [a for three in outs for a in three] if outs is not None else []
    elements = sum(piece[3].size for piece in pieces)
    new = pl.pallas_call(
        kernel,
        in_specs=[pl.BlockSpec(memory_space=pltpu.SMEM)] * 3 + [any_] * (n_in + len(before)),
        out_specs=[any_] * 9,
        out_shape=[jax.ShapeDtypeStruct(a.shape, a.dtype) for a in given],
        scratch_shapes=[pltpu.VMEM((SLOTS, *shapes[q]), t) for q in kinds for t in (BF16, F32, F32, BF16)]
        + [pltpu.SemaphoreType.DMA((4, SLOTS)), pltpu.SemaphoreType.DMA((3, SLOTS))],
        input_output_aliases={3 + n_in + n: n for n in range(len(before))},
        cost_estimate=pl.CostEstimate(flops=2000 * elements, bytes_accessed=22 * elements, transcendentals=elements),
        compiler_params=params(),
    )(table, who, factor, *given, *(piece[3] for piece in pieces), *before)
    return tuple(tuple(new[3 * n : 3 * n + 3]) for n in range(3))


def solution(mesh):
    def step(x, dy, wg, wu, wd, mg, mu, md, vg, vu, vd):
        me = lax.axis_index("dp")
        places = jnp.arange(5, dtype=jnp.int32)
        who = jnp.where(places < 4, me ^ places, places)
        x, dy = x[0], dy[0]
        ff = wg.shape[2]
        own = ff // LANES // 4 * LANES

        def send(a, perm):
            return perm(a)

        dy_x, dy_d = send(dy, px), send(dy, pd)
        h1, a1, a0 = forward(x, wg, wu, wd)
        a1_x, a1_d = send(a1, px), send(a1, pd)
        a0_x, a0_d = send(a0, px), send(a0, pd)
        dh1 = chain(a1, dy, h1, wg, wu, wd)
        dh1_x, dh1_d = send(dh1, px), send(dh1, pd)
        a1_xd, dy_xd = send(a1_x, pd), send(dy_x, pd)
        top = slices(1, own, me, [a1, a1_d, a1_x, a1_xd], [dy, dy_d, dy_x, dy_xd], wg, wu, wd)
        top, a0_x, dh1_x = lax.optimization_barrier((top, a0_x, dh1_x))
        a0_xd, dh1_xd = send(a0_x, pd), send(dh1_x, pd)
        top_x = [send(top[n], px) for n in range(3)]
        top_d = [send(top[n], pd) for n in range(3)]
        low = slices(0, own, me, [a0, a0_d, a0_x, a0_xd], [dh1, dh1_d, dh1_x, dh1_xd], wg, wu, wd)
        total = jnp.sum(top[6] + low[6]).reshape(1)
        total = total + px(total)
        low, total = lax.optimization_barrier((low, total))
        low_x = [send(low[n], px) for n in range(3)]
        low_d = [send(low[n], pd) for n in range(3)]
        total = total + pd(total) + jnp.sum(top[7] + low[7])
        count = wg.size + wu.size + wd.size
        factor = jnp.minimum(1.0, 0.5 * lax.rsqrt(total / count + 1e-30))

        top_xd = [send(top_x[n], pd) for n in range(3)]
        low_xd = [send(low_x[n], pd) for n in range(2)]
        arrays = ((wg, mg, vg), (wu, mu, vu), (wd, md, vd))

        def pieces(layer, slot, gs, names=(0, 1, 2)):
            return [(n, layer, slot, gs[n]) for n in names]

        first = pieces(1, 0, top) + pieces(1, 1, top_d) + pieces(1, 2, top_x) + pieces(0, 0, low)
        shared = pieces(1, 4, top[3:6]) + pieces(0, 4, low[3:6])
        outs = adam(own, factor, who, arrays, first + shared, None)
        outs = adam(own, factor, who, arrays, pieces(1, 3, top_xd) + pieces(0, 1, low_d), outs)
        outs, low_x[2] = lax.optimization_barrier((outs, low_x[2]))
        low_xd.append(send(low_x[2], pd))
        outs = adam(own, factor, who, arrays, pieces(0, 2, low_x) + pieces(0, 3, low_xd, (0, 1)), outs)
        outs = adam(own, factor, who, arrays, pieces(0, 3, low_xd, (2,)), outs)
        return tuple(outs[name][which] for which in range(3) for name in range(3))

    return jax.shard_map(
        step,
        mesh=mesh,
        in_specs=(P(("rep", "dp"), None, None),) * 2 + (P(None, None, None),) * 9,
        out_specs=(P("rep", None, None),) * 9,
        check_vma=False,
    )
```

```python
import jax
import jax.numpy as jnp
import numpy as np
from jax import lax
from jax.experimental import pallas as pl
from jax.experimental.pallas import tpu as pltpu
from jax.sharding import PartitionSpec as P


F32, BF16 = jnp.float32, jnp.bfloat16
PX = ((0, 2), (2, 0), (1, 3), (3, 1))
PD = ((0, 1), (1, 0), (2, 3), (3, 2))
NN, NT = ((1,), (0,)), ((1,), (1,))

LANES = 128
BLOCK = 512
ROWS = 512


def dot(a, b, dims):
    return lax.dot_general(a, b, (dims, ((), ())), preferred_element_type=F32)


def sigmoid(x):
    return 0.5 * jnp.tanh(0.5 * x) + 0.5


def px(a):
    return lax.ppermute(a, "dp", PX)


def pd(a):
    return lax.ppermute(a, "dp", PD)


def once(shape, index):
    return pl.BlockSpec(shape, index, pipeline_mode=pl.Buffered(1))


def params(mib=62):
    return pltpu.CompilerParams(vmem_limit_bytes=mib << 20)


def norm_scale(wide):
    return lax.rsqrt(jnp.mean(wide * wide, -1, keepdims=True) + 1e-6)


def normed(h):
    wide = h.astype(F32)
    return (wide * norm_scale(wide)).astype(BF16)


def forward_kernel(tail, x_ref, wg_ref, wu_ref, wd_ref, h_ref, a_ref, a0_ref, acc_ref):
    j, last = pl.program_id(0), pl.num_programs(0) - 1
    tokens = x_ref.shape[0]
    chunks = [pl.ds(r, ROWS) for r in range(0, tokens, ROWS)]

    @pl.when(j == 0)
    def _():
        for r in chunks:
            a0_ref[r, :] = normed(x_ref[r, :])
            acc_ref[r, :] = jnp.zeros((ROWS, acc_ref.shape[1]), F32)

    def block(width):
        hid = {}

        def up(r):
            a = a0_ref[chunks[r], :]
            g = dot(a, wg_ref[0, :, :width], NN)
            u = dot(a, wu_ref[0, :, :width], NN)
            hid[r] = (g * sigmoid(g) * u).astype(BF16)

        def down(r):
            acc_ref[chunks[r], :] += dot(hid.pop(r), wd_ref[0, :width, :], NN)

        up(0)
        for r in range(1, len(chunks)):
            up(r)
            down(r - 1)
        down(len(chunks) - 1)

    @pl.when(j < last)
    def _():
        block(wg_ref.shape[2])

    @pl.when(j == last)
    def _():
        block(tail)
        for r in chunks:
            h = (x_ref[r, :].astype(F32) + acc_ref[r, :].astype(BF16).astype(F32)).astype(BF16)
            h_ref[r, :] = h
            a_ref[r, :] = normed(h)


def forward(x, wg, wu, wd):
    tokens, d = x.shape
    ff = wg.shape[2]
    steps = pl.cdiv(ff, BLOCK)
    full = once((tokens, d), lambda j: (0, 0))
    across = pl.BlockSpec((1, d, BLOCK), lambda j: (0, 0, j))
    down = pl.BlockSpec((1, BLOCK, d), lambda j: (0, j, 0))
    return pl.pallas_call(
        lambda *refs: forward_kernel(ff - (steps - 1) * BLOCK, *refs),
        grid=(steps,),
        in_specs=[full, across, across, down],
        out_specs=[full] * 3,
        out_shape=[jax.ShapeDtypeStruct((tokens, d), BF16)] * 3,
        scratch_shapes=[pltpu.VMEM((tokens, d), F32)],
        cost_estimate=pl.CostEstimate(flops=6 * tokens * d * ff, bytes_accessed=6 * d * ff, transcendentals=tokens * ff),
        compiler_params=params(),
        name="forward",
    )(x, wg, wu, wd)


def hidden_back(g, u, dhid):
    dhid = dhid.astype(BF16).astype(F32)
    sig = sigmoid(g)
    act = g * sig
    return (dhid * u * (sig + act * (1 - sig))).astype(BF16), (dhid * act).astype(BF16), (act * u).astype(BF16)


def chain_kernel(tail, a_ref, dy_ref, h_ref, wg_ref, wu_ref, wd_ref, dh_ref, acc_ref):
    j, last = pl.program_id(0), pl.num_programs(0) - 1
    tokens = a_ref.shape[0]
    chunks = [pl.ds(r, ROWS) for r in range(0, tokens, ROWS)]

    @pl.when(j == 0)
    def _():
        for r in chunks:
            acc_ref[r, :] = jnp.zeros((ROWS, acc_ref.shape[1]), F32)

    def block(width):
        held = {}

        def there(r):
            a, dy = a_ref[chunks[r], :], dy_ref[chunks[r], :]
            g = dot(a, wg_ref[0, :, :width], NN)
            u = dot(a, wu_ref[0, :, :width], NN)
            dhid = dot(dy, wd_ref[0, :width, :], NT)
            held[r] = hidden_back(g, u, dhid)[:2]

        def back(r):
            dg, du = held.pop(r)
            acc_ref[chunks[r], :] += dot(dg, wg_ref[0, :, :width], NT) + dot(du, wu_ref[0, :, :width], NT)

        there(0)
        for r in range(1, len(chunks)):
            there(r)
            back(r - 1)
        back(len(chunks) - 1)

    @pl.when(j < last)
    def _():
        block(wg_ref.shape[2])

    @pl.when(j == last)
    def _():
        block(tail)
        for r in chunks:
            wide, da = h_ref[r, :].astype(F32), acc_ref[r, :].astype(BF16).astype(F32)
            scale = norm_scale(wide)
            back = scale * da - wide * (scale * scale * scale * jnp.mean(wide * da, -1, keepdims=True))
            dh_ref[r, :] = (dy_ref[r, :].astype(F32) + back.astype(BF16).astype(F32)).astype(BF16)


def chain(a, dy, h, wg, wu, wd):
    tokens, d = a.shape
    ff = wg.shape[2]
    steps = pl.cdiv(ff, BLOCK)
    full = once((tokens, d), lambda j: (0, 0))
    across = pl.BlockSpec((1, d, BLOCK), lambda j: (1, 0, j))
    down = pl.BlockSpec((1, BLOCK, d), lambda j: (1, j, 0))
    return pl.pallas_call(
        lambda *refs: chain_kernel(ff - (steps - 1) * BLOCK, *refs),
        grid=(steps,),
        in_specs=[full, full, full, across, across, down],
        out_specs=full,
        out_shape=jax.ShapeDtypeStruct((tokens, d), BF16),
        scratch_shapes=[pltpu.VMEM((tokens, d), F32)],
        cost_estimate=pl.CostEstimate(flops=10 * tokens * d * ff, bytes_accessed=6 * d * ff, transcendentals=tokens * ff),
        compiler_params=params(),
        name="chain",
    )(a, dy, h, wg, wu, wd)


def slices_kernel(layer, own, count, *refs):
    me = lax.axis_index("dp")
    chip, core = me // 2, me % 2
    partner = chip * 2 + 1 - core
    others = (partner, (1 - chip) * 2 + core, (1 - chip) * 2 + 1 - core)
    a_refs, dy_refs, (wg_hbm, wu_hbm, wd_hbm) = refs[:3], refs[3:6], refs[6:9]
    final = count is not None
    before = refs[9:11] if final else ()
    refs = refs[11 if final else 9 :]
    outs, scratch = refs[:8], refs[8:]
    wg_ref, wu_ref, wd_ref, accg_ref, accu_ref, accd_ref, a_buf, dy_buf, a_far, dy_far, sums_ref, sems, w_sems, send_sems, recv_sems, *terms = scratch
    i, steps = pl.program_id(0), pl.num_programs(0)
    each = a_refs[0].shape[0] // ROWS
    width = wg_ref.shape[1]

    def fetch(step, do):
        slot, who = lax.rem(step, 2), step // each
        rows = pl.ds(pl.multiple_of(lax.rem(step, each) * ROWS, ROWS), ROWS)
        for k, (a, dy) in enumerate(zip((*a_refs, a_far), (*dy_refs, dy_far), strict=True)):

            @pl.when(who == k)
            def _():
                do(pltpu.make_async_copy(a.at[rows, :], a_buf.at[slot], sems.at[0, slot]))
                do(pltpu.make_async_copy(dy.at[rows, :], dy_buf.at[slot], sems.at[1, slot]))

    def weights():
        parts = ((pl.ds(pl.multiple_of(me * own, LANES), own), pl.ds(0, own)), (pl.ds(4 * own, width - own), pl.ds(own, width - own)))
        return [
            pltpu.make_async_copy(*((hbm.at[layer, there, :], ref.at[here, :]) if n == 2 else (hbm.at[layer, :, there], ref.at[:, here])), w_sems.at[n, m])
            for n, (hbm, ref) in enumerate(((wg_hbm, wg_ref), (wu_hbm, wu_ref), (wd_hbm, wd_ref)))
            for m, (there, here) in enumerate(parts)
        ]

    def onward(n):
        return pltpu.make_async_remote_copy(
            src_ref=(a_refs[2], dy_refs[2])[n],
            dst_ref=(a_far, dy_far)[n],
            send_sem=send_sems.at[n],
            recv_sem=recv_sems.at[n],
            device_id={"dp": partner},
            device_id_type=pl.DeviceIdType.MESH,
        )

    def told(n):
        return pltpu.make_async_remote_copy(
            src_ref=sums_ref.at[0],
            dst_ref=sums_ref.at[1 + n],
            send_sem=send_sems.at[2 + n],
            recv_sem=recv_sems.at[2 + n],
            device_id={"dp": others[n]},
            device_id_type=pl.DeviceIdType.MESH,
        )

    barrier = pltpu.get_barrier_semaphore()
    spoken = others if final else others[:1]

    @pl.when(i == 0)
    def _():
        for other in spoken:
            pl.semaphore_signal(barrier, inc=1, device_id={"dp": other}, device_id_type=pl.DeviceIdType.MESH)
        fetch(i, lambda copy: copy.start())
        for copy in weights():
            copy.start()
        for copy in weights():
            copy.wait()

    @pl.when(i == 1)
    def _():
        pl.semaphore_wait(barrier, len(spoken))
        for n in range(2):
            onward(n).start()

    @pl.when(i == 3 * each - 1)
    def _():
        for n in range(2):
            onward(n).wait()

    @pl.when(i + 1 < steps)
    def _():
        fetch(i + 1, lambda copy: copy.start())

    slot = lax.rem(i, 2)
    pltpu.make_async_copy(a_refs[0].at[pl.ds(0, ROWS), :], a_buf.at[slot], sems.at[0, slot]).wait()
    pltpu.make_async_copy(dy_refs[0].at[pl.ds(0, ROWS), :], dy_buf.at[slot], sems.at[1, slot]).wait()
    a, dy = a_buf[slot], dy_buf[slot]
    a_t, dy_t = a.T, dy.T
    blocks = [pl.ds(c, min(BLOCK, width - c)) for c in range(0, width, BLOCK)]
    held = {}

    def there(c):
        s = blocks[c]
        held[c] = hidden_back(dot(a, wg_ref[:, s], NN), dot(a, wu_ref[:, s], NN), dot(dy, wd_ref[s, :], NT))

    def back(c):
        s = blocks[c]
        dg, du, hid = held.pop(c)
        for acc, left, right in ((accg_ref, a_t, dg), (accu_ref, a_t, du), (accd_ref, dy_t, hid)):
            acc[:, s] = jnp.where(i == 0, 0.0, acc[:, s]) + dot(left, right, NN)

    there(0)
    for c in range(1, len(blocks)):
        there(c)
        back(c - 1)
    back(len(blocks) - 1)

    rest = pl.ds(own, width - own)

    @pl.when(lax.rem(i, each) == each - 1)
    def _():
        for acc, term in zip((accg_ref, accu_ref, accd_ref), terms, strict=True):
            term[i // each] = acc[:, rest]
            acc[:, rest] = jnp.zeros_like(acc[:, rest])

    @pl.when(i == steps - 1)
    def _():
        sums = [None, None]
        for acc, term, out, out_s, turned in (
            (accg_ref, terms[0], *outs[0:4:3], False),
            (accu_ref, terms[1], *outs[1:5:3], False),
            (accd_ref, terms[2], *outs[2:6:3], True),
        ):
            at = [(core + s) % 2 + 2 * ((chip + s // 2) % 2) for s in range(4)]
            whole = term[at[0]] + term[at[1]] + term[at[2]] + term[at[3]]
            for c in range(0, width, LANES):
                part = (acc[:, c : c + LANES] if c < own else whole[:, c - own : c - own + LANES]).astype(BF16)
                ref, place = (out, pl.ds(c, LANES)) if c < own else (out_s, pl.ds(c - own, LANES))
                if turned:
                    ref[place, :] = part.T
                else:
                    ref[:, place] = part
                square = part.astype(F32)
                square = jnp.sum((square * square).reshape(-1, 8, LANES), 0)
                sums[c >= own] = square if sums[c >= own] is None else sums[c >= own] + square
        if not final:
            outs[6][...], outs[7][...] = sums
        else:
            sums_ref[0] = sums[0] + before[0][...]
            shared = jnp.sum(sums[1] + before[1][...])
            for n in range(3):
                told(n).start()
            for n in range(3):
                told(n).wait()
            total = sums_ref[at[0]] + sums_ref[at[1]] + sums_ref[at[2]] + sums_ref[at[3]]
            total = jnp.full((8, LANES), jnp.sum(total) + shared, F32)
            outs[6][...] = jnp.minimum(1.0, 0.5 * lax.rsqrt(total / count + 1e-30))
            outs[7][...] = jnp.zeros((8, LANES), F32)


def slices(layer, own, a_all, dy_all, wg, wu, wd, before=None, count=None):
    tokens, d = a_all[0].shape
    ff = wg.shape[2]
    rest = ff - 4 * own
    width = own + rest
    any_ = pl.BlockSpec(memory_space=pl.ANY)
    at = lambda s: once(s, lambda i: (0, 0))
    sizes = [(d, own), (d, own), (own, d), (d, rest), (d, rest), (rest, d)]
    return pl.pallas_call(
        lambda *refs: slices_kernel(layer, own, count, *refs),
        grid=(4 * tokens // ROWS,),
        in_specs=[any_] * 9 + [at((8, LANES))] * len(before or ()),
        out_specs=[at(s) for s in sizes] + [at((8, LANES))] * 2,
        scratch_shapes=[pltpu.VMEM((d, width), BF16)] * 2
        + [pltpu.VMEM((width, d), BF16)]
        + [pltpu.VMEM((d, width), F32)] * 3
        + [pltpu.VMEM((2, ROWS, d), BF16)] * 2
        + [pltpu.VMEM((tokens, d), BF16)] * 2
        + [pltpu.VMEM((4, 8, LANES), F32)]
        + [pltpu.SemaphoreType.DMA(n) for n in ((2, 2), (3, 2), (5,), (5,))]
        + [pltpu.VMEM((4, d, rest), F32)] * 3,
        out_shape=[jax.ShapeDtypeStruct(s, BF16) for s in sizes] + [jax.ShapeDtypeStruct((8, LANES), F32)] * 2,
        cost_estimate=pl.CostEstimate(
            flops=12 * 4 * tokens * d * width, bytes_accessed=16 * tokens * d, transcendentals=4 * tokens * width
        ),
        compiler_params=pltpu.CompilerParams(vmem_limit_bytes=62 << 20, collective_id=layer, has_side_effects=True),
        name="slices",
    )(*a_all, *dy_all, wg, wu, wd, *(before or ()))


def adam_math(f, w, m, v, g):
    g = g.astype(F32) * f
    m = 0.9 * m + 0.1 * g
    v = 0.95 * v + 0.05 * g * g
    return (0.998 * w.astype(F32) - 0.02 * (m * lax.rsqrt(v + 1e-8))).astype(BF16), m, v


SLOTS, AHEAD = 6, 3


def adam(own, factor, who, arrays, pieces, outs):
    d, _ = arrays[0][0].shape[1:]
    shapes = ((LANES, own), (LANES, d), (d, LANES))
    rows = []
    for n, (which, layer, slot, g) in enumerate(pieces):
        kind = 1 if which == 2 else 2 if slot == 4 else 0
        for r in range(0, g.shape[0], shapes[kind][0]):
            rows.append((kind, which, layer, n, slot, r, *((own, 0) if which == 2 else (0, own))))
    table = np.array(rows, np.int32).T
    total = len(rows)
    kinds = sorted({row[0] for row in rows})
    n_in = 9 + len(pieces)

    def kernel(table_ref, who_ref, f_ref, *refs):
        weights, grads = refs[:9], refs[9:n_in]
        refs = refs[n_in + (9 if outs is not None else 0) :]
        results, scratch = refs[:9], refs[9:]
        buffers = {kind: scratch[4 * n : 4 * n + 4] for n, kind in enumerate(kinds)}
        sem_in, sem_out = scratch[-2:]
        f = f_ref[0]

        def place(step):
            kind, which, layer = (table_ref[n, step] for n in range(3))
            unit = who_ref[table_ref[4, step]]
            row, col = table_ref[5, step] + table_ref[6, step] * unit, table_ref[7, step] * unit
            return kind, which, lambda shape: (layer, pl.ds(pl.multiple_of(row, 16), shape[0]), pl.ds(pl.multiple_of(col, LANES), shape[1]))

        def fetch(step):
            slot = lax.rem(step, SLOTS)
            kind, which, at = place(step)
            for k in range(3):
                its = [q for q in kinds if (q == 1) == (k == 2)]
                for q in its:

                    @pl.when((which == k) & (kind == q))
                    def _():
                        for n in range(3):
                            pltpu.make_async_copy(weights[3 * k + n].at[at(shapes[q])], buffers[q][n].at[slot], sem_in.at[n, slot]).start()

            piece, row = table_ref[3, step], table_ref[5, step]
            for n, (which_, _, slot_, _) in enumerate(pieces):
                q = 1 if which_ == 2 else 2 if slot_ == 4 else 0

                @pl.when(piece == n)
                def _():
                    rows_ = pl.ds(pl.multiple_of(row, 16), shapes[q][0])
                    pltpu.make_async_copy(grads[n].at[rows_, :], buffers[q][3].at[slot], sem_in.at[3, slot]).start()

        def stored(step, do):
            slot = lax.rem(step, SLOTS)
            kind, which, at = place(step)
            for k in range(3):
                for q in [q for q in kinds if (q == 1) == (k == 2)]:

                    @pl.when((which == k) & (kind == q))
                    def _():
                        for n in range(3):
                            do(pltpu.make_async_copy(buffers[q][n].at[slot], results[3 * k + n].at[at(shapes[q])], sem_out.at[n, slot]))

        for step in range(min(AHEAD, total)):
            fetch(jnp.int32(step))

        def body(step, carry):
            @pl.when(step + AHEAD < total)
            def _():
                @pl.when(step + AHEAD >= SLOTS)
                def _():
                    stored(step + AHEAD - SLOTS, lambda copy: copy.wait())

                fetch(step + AHEAD)

            slot = lax.rem(step, SLOTS)
            for q in kinds:

                @pl.when(table_ref[0, step] == q)
                def _():
                    w, m, v, g = buffers[q]
                    for n in range(3):
                        pltpu.make_async_copy(weights[n].at[0, pl.ds(0, shapes[q][0]), pl.ds(0, shapes[q][1])], buffers[q][n].at[slot], sem_in.at[n, slot]).wait()
                    pltpu.make_async_copy(buffers[q][3].at[slot], buffers[q][3].at[slot], sem_in.at[3, slot]).wait()
                    some = 32 if shapes[q][1] > LANES else 224

                    def part(r, carry):
                        at = pl.ds(pl.multiple_of(r * some, some), some)
                        new = adam_math(f, w[slot, at, :], m[slot, at, :], v[slot, at, :], g[slot, at, :])
                        w[slot, at, :], m[slot, at, :], v[slot, at, :] = new
                        return carry

                    lax.fori_loop(0, shapes[q][0] // some, part, 0)

            stored(step, lambda copy: copy.start())
            return carry

        lax.fori_loop(0, total, body, 0)
        for step in range(max(0, total - SLOTS), total):
            stored(jnp.int32(step), lambda copy: copy.wait())

    any_ = pl.BlockSpec(memory_space=pl.ANY)
    given = [a for three in arrays for a in three]
    before = [a for three in outs for a in three] if outs is not None else []
    elements = sum(piece[3].size for piece in pieces)
    new = pl.pallas_call(
        kernel,
        in_specs=[pl.BlockSpec(memory_space=pltpu.SMEM)] * 3 + [any_] * (n_in + len(before)),
        out_specs=[any_] * 9,
        out_shape=[jax.ShapeDtypeStruct(a.shape, a.dtype) for a in given],
        scratch_shapes=[pltpu.VMEM((SLOTS, *shapes[q]), t) for q in kinds for t in (BF16, F32, F32, BF16)]
        + [pltpu.SemaphoreType.DMA((4, SLOTS)), pltpu.SemaphoreType.DMA((3, SLOTS))],
        input_output_aliases={3 + n_in + n: n for n in range(len(before))},
        cost_estimate=pl.CostEstimate(flops=2000 * elements, bytes_accessed=22 * elements, transcendentals=elements),
        compiler_params=params(),
    )(table, who, factor, *given, *(piece[3] for piece in pieces), *before)
    return tuple(tuple(new[3 * n : 3 * n + 3]) for n in range(3))


def solution(mesh):
    def step(x, dy, wg, wu, wd, mg, mu, md, vg, vu, vd):
        me = lax.axis_index("dp")
        places = jnp.arange(5, dtype=jnp.int32)
        who = jnp.where(places < 4, me ^ places, places)
        x, dy = x[0], dy[0]
        ff = wg.shape[2]
        own = ff // LANES // 4 * LANES

        def send(a, perm):
            return perm(a)

        dy_x, dy_d = send(dy, px), send(dy, pd)
        h1, a1, a0 = forward(x, wg, wu, wd)
        a1_x, a1_d = send(a1, px), send(a1, pd)
        a0_x, a0_d = send(a0, px), send(a0, pd)
        dh1 = chain(a1, dy, h1, wg, wu, wd)
        dh1_x, dh1_d = send(dh1, px), send(dh1, pd)
        top = slices(1, own, [a1, a1_d, a1_x], [dy, dy_d, dy_x], wg, wu, wd)
        top_x = [send(top[n], px) for n in range(3)]
        top_d = [send(top[n], pd) for n in range(3)]
        low = slices(0, own, [a0, a0_d, a0_x], [dh1, dh1_d, dh1_x], wg, wu, wd, top[6:8], wg.size + wu.size + wd.size)
        factor = low[6][0, :1]
        low_x = [send(low[n], px) for n in range(3)]
        low_d = [send(low[n], pd) for n in range(3)]

        top_xd = [send(top_x[n], pd) for n in range(3)]
        low_xd = [send(low_x[n], pd) for n in range(2)]
        arrays = ((wg, mg, vg), (wu, mu, vu), (wd, md, vd))

        def pieces(layer, slot, gs, names=(0, 1, 2)):
            return [(n, layer, slot, gs[n]) for n in names]

        first = pieces(1, 0, top) + pieces(1, 1, top_d) + pieces(1, 2, top_x) + pieces(0, 0, low)
        shared = pieces(1, 4, top[3:6]) + pieces(0, 4, low[3:6])
        outs = adam(own, factor, who, arrays, first + shared, None)
        outs = adam(own, factor, who, arrays, pieces(1, 3, top_xd) + pieces(0, 1, low_d), outs)
        outs, low_x[2] = lax.optimization_barrier((outs, low_x[2]))
        low_xd.append(send(low_x[2], pd))
        outs = adam(own, factor, who, arrays, pieces(0, 2, low_x) + pieces(0, 3, low_xd, (0, 1)), outs)
        outs = adam(own, factor, who, arrays, pieces(0, 3, low_xd, (2,)), outs)
        return tuple(outs[name][which] for which in range(3) for name in range(3))

    return jax.shard_map(
        step,
        mesh=mesh,
        in_specs=(P(("rep", "dp"), None, None),) * 2 + (P(None, None, None),) * 9,
        out_specs=(P("rep", None, None),) * 9,
        check_vma=False,
    )
```

```python
import jax
import jax.numpy as jnp
import numpy as np
from jax import lax
from jax.experimental import pallas as pl
from jax.experimental.pallas import tpu as pltpu
from jax.sharding import PartitionSpec as P


F32, BF16 = jnp.float32, jnp.bfloat16
PX = ((0, 2), (2, 0), (1, 3), (3, 1))
PD = ((0, 1), (1, 0), (2, 3), (3, 2))
NN = ((1,), (0,))

LANES = 128
BLOCK = 512
ROWS = 512


def dot(a, b, dims):
    return lax.dot_general(a, b, (dims, ((), ())), preferred_element_type=F32)


def sigmoid(x):
    return 0.5 * jnp.tanh(0.5 * x) + 0.5


def px(a):
    return lax.ppermute(a, "dp", PX)


def pd(a):
    return lax.ppermute(a, "dp", PD)


def once(shape, index):
    return pl.BlockSpec(shape, index, pipeline_mode=pl.Buffered(1))


def params(mib=62):
    return pltpu.CompilerParams(vmem_limit_bytes=mib << 20)


def norm_scale(wide):
    return lax.rsqrt(jnp.mean(wide * wide, -1, keepdims=True) + 1e-6)


def normed(h):
    wide = h.astype(F32)
    return (wide * norm_scale(wide)).astype(BF16)


def forward_kernel(tail, x_ref, wg_ref, wu_ref, wd_ref, h_ref, a_ref, a0_ref, acc_ref):
    j, last = pl.program_id(0), pl.num_programs(0) - 1
    tokens = x_ref.shape[0]
    chunks = [pl.ds(r, ROWS) for r in range(0, tokens, ROWS)]

    @pl.when(j == 0)
    def _():
        for r in chunks:
            a0_ref[r, :] = normed(x_ref[r, :])
            acc_ref[r, :] = jnp.zeros((ROWS, acc_ref.shape[1]), F32)

    def block(width):
        hid = {}

        def up(r):
            a = a0_ref[chunks[r], :]
            g = dot(a, wg_ref[0, :, :width], NN)
            u = dot(a, wu_ref[0, :, :width], NN)
            hid[r] = (g * sigmoid(g) * u).astype(BF16)

        def down(r):
            acc_ref[chunks[r], :] += dot(hid.pop(r), wd_ref[0, :width, :], NN)

        up(0)
        for r in range(1, len(chunks)):
            up(r)
            down(r - 1)
        down(len(chunks) - 1)

    @pl.when(j < last)
    def _():
        block(wg_ref.shape[2])

    @pl.when(j == last)
    def _():
        block(tail)
        for r in chunks:
            h = (x_ref[r, :].astype(F32) + acc_ref[r, :].astype(BF16).astype(F32)).astype(BF16)
            h_ref[r, :] = h
            a_ref[r, :] = normed(h)


def forward(x, wg, wu, wd):
    tokens, d = x.shape
    ff = wg.shape[2]
    steps = pl.cdiv(ff, BLOCK)
    full = once((tokens, d), lambda j: (0, 0))
    across = pl.BlockSpec((1, d, BLOCK), lambda j: (0, 0, j))
    down = pl.BlockSpec((1, BLOCK, d), lambda j: (0, j, 0))
    return pl.pallas_call(
        lambda *refs: forward_kernel(ff - (steps - 1) * BLOCK, *refs),
        grid=(steps,),
        in_specs=[full, across, across, down],
        out_specs=[full] * 3,
        out_shape=[jax.ShapeDtypeStruct((tokens, d), BF16)] * 3,
        scratch_shapes=[pltpu.VMEM((tokens, d), F32)],
        cost_estimate=pl.CostEstimate(flops=6 * tokens * d * ff, bytes_accessed=6 * d * ff, transcendentals=tokens * ff),
        compiler_params=params(),
        name="forward",
    )(x, wg, wu, wd)


def hidden_back(g, u, dhid):
    dhid = dhid.astype(BF16).astype(F32)
    sig = sigmoid(g)
    act = g * sig
    return (dhid * u * (sig + act * (1 - sig))).astype(BF16), (dhid * act).astype(BF16), (act * u).astype(BF16)


def chain_kernel(tail, a_ref, dy_ref, h_ref, wg_ref, wu_ref, wd_ref, dh_ref, acc_ref, wgt_ref, wut_ref, wdt_ref):
    j, last = pl.program_id(0), pl.num_programs(0) - 1
    tokens = a_ref.shape[0]
    chunks = [pl.ds(r, ROWS) for r in range(0, tokens, ROWS)]

    @pl.when(j == 0)
    def _():
        for r in chunks:
            acc_ref[r, :] = jnp.zeros((ROWS, acc_ref.shape[1]), F32)

    def block(width):
        held = {}
        wdt_ref[:, :width] = wd_ref[0, :width, :].T
        wgt_ref[:width, :] = wg_ref[0, :, :width].T
        wut_ref[:width, :] = wu_ref[0, :, :width].T

        def there(r):
            a, dy = a_ref[chunks[r], :], dy_ref[chunks[r], :]
            g = dot(a, wg_ref[0, :, :width], NN)
            u = dot(a, wu_ref[0, :, :width], NN)
            dhid = dot(dy, wdt_ref[:, :width], NN)
            held[r] = hidden_back(g, u, dhid)[:2]

        def back(r):
            dg, du = held.pop(r)
            acc_ref[chunks[r], :] += dot(dg, wgt_ref[:width, :], NN) + dot(du, wut_ref[:width, :], NN)

        there(0)
        for r in range(1, len(chunks)):
            there(r)
            back(r - 1)
        back(len(chunks) - 1)

    @pl.when(j < last)
    def _():
        block(wg_ref.shape[2])

    @pl.when(j == last)
    def _():
        block(tail)
        for r in chunks:
            wide, da = h_ref[r, :].astype(F32), acc_ref[r, :].astype(BF16).astype(F32)
            scale = norm_scale(wide)
            back = scale * da - wide * (scale * scale * scale * jnp.mean(wide * da, -1, keepdims=True))
            dh_ref[r, :] = (dy_ref[r, :].astype(F32) + back.astype(BF16).astype(F32)).astype(BF16)


def chain(a, dy, h, wg, wu, wd):
    tokens, d = a.shape
    ff = wg.shape[2]
    steps = pl.cdiv(ff, BLOCK)
    full = once((tokens, d), lambda j: (0, 0))
    across = pl.BlockSpec((1, d, BLOCK), lambda j: (1, 0, j))
    down = pl.BlockSpec((1, BLOCK, d), lambda j: (1, j, 0))
    return pl.pallas_call(
        lambda *refs: chain_kernel(ff - (steps - 1) * BLOCK, *refs),
        grid=(steps,),
        in_specs=[full, full, full, across, across, down],
        out_specs=full,
        out_shape=jax.ShapeDtypeStruct((tokens, d), BF16),
        scratch_shapes=[pltpu.VMEM((tokens, d), F32)] + [pltpu.VMEM((BLOCK, d), BF16)] * 2 + [pltpu.VMEM((d, BLOCK), BF16)],
        cost_estimate=pl.CostEstimate(flops=10 * tokens * d * ff, bytes_accessed=6 * d * ff, transcendentals=tokens * ff),
        compiler_params=params(),
        name="chain",
    )(a, dy, h, wg, wu, wd)


def slices_kernel(layer, own, count, *refs):
    me = lax.axis_index("dp")
    chip, core = me // 2, me % 2
    partner = chip * 2 + 1 - core
    others = (partner, (1 - chip) * 2 + core, (1 - chip) * 2 + 1 - core)
    a_refs, dy_refs, (wg_hbm, wu_hbm, wd_hbm) = refs[:3], refs[3:6], refs[6:9]
    final = count is not None
    before = refs[9:11] if final else ()
    refs = refs[11 if final else 9 :]
    outs, scratch = refs[:8], refs[8:]
    wg_ref, wu_ref, wd_ref, accg_ref, accu_ref, accd_ref, a_buf, dy_buf, a_far, dy_far, sums_ref, sems, w_sems, send_sems, recv_sems, wdt_ref, *terms = scratch
    i, steps = pl.program_id(0), pl.num_programs(0)
    each = a_refs[0].shape[0] // ROWS
    width = wg_ref.shape[1]

    def fetch(step, do):
        slot, who = lax.rem(step, 2), step // each
        rows = pl.ds(pl.multiple_of(lax.rem(step, each) * ROWS, ROWS), ROWS)
        for k, (a, dy) in enumerate(zip((*a_refs, a_far), (*dy_refs, dy_far), strict=True)):

            @pl.when(who == k)
            def _():
                do(pltpu.make_async_copy(a.at[rows, :], a_buf.at[slot], sems.at[0, slot]))
                do(pltpu.make_async_copy(dy.at[rows, :], dy_buf.at[slot], sems.at[1, slot]))

    def weights():
        parts = ((pl.ds(pl.multiple_of(me * own, LANES), own), pl.ds(0, own)), (pl.ds(4 * own, width - own), pl.ds(own, width - own)))
        return [
            pltpu.make_async_copy(*((hbm.at[layer, there, :], ref.at[here, :]) if n == 2 else (hbm.at[layer, :, there], ref.at[:, here])), w_sems.at[n, m])
            for n, (hbm, ref) in enumerate(((wg_hbm, wg_ref), (wu_hbm, wu_ref), (wd_hbm, wd_ref)))
            for m, (there, here) in enumerate(parts)
        ]

    def onward(n):
        return pltpu.make_async_remote_copy(
            src_ref=(a_refs[2], dy_refs[2])[n],
            dst_ref=(a_far, dy_far)[n],
            send_sem=send_sems.at[n],
            recv_sem=recv_sems.at[n],
            device_id={"dp": partner},
            device_id_type=pl.DeviceIdType.MESH,
        )

    def told(n):
        return pltpu.make_async_remote_copy(
            src_ref=sums_ref.at[0],
            dst_ref=sums_ref.at[1 + n],
            send_sem=send_sems.at[2 + n],
            recv_sem=recv_sems.at[2 + n],
            device_id={"dp": others[n]},
            device_id_type=pl.DeviceIdType.MESH,
        )

    barrier = pltpu.get_barrier_semaphore()
    spoken = others if final else others[:1]

    @pl.when(i == 0)
    def _():
        for other in spoken:
            pl.semaphore_signal(barrier, inc=1, device_id={"dp": other}, device_id_type=pl.DeviceIdType.MESH)
        fetch(i, lambda copy: copy.start())
        for copy in weights():
            copy.start()
        for copy in weights():
            copy.wait()
        wdt_ref[...] = wd_ref[...].T

    @pl.when(i == 1)
    def _():
        pl.semaphore_wait(barrier, len(spoken))
        for n in range(2):
            onward(n).start()

    @pl.when(i == 3 * each - 1)
    def _():
        for n in range(2):
            onward(n).wait()

    @pl.when(i + 1 < steps)
    def _():
        fetch(i + 1, lambda copy: copy.start())

    slot = lax.rem(i, 2)
    pltpu.make_async_copy(a_refs[0].at[pl.ds(0, ROWS), :], a_buf.at[slot], sems.at[0, slot]).wait()
    pltpu.make_async_copy(dy_refs[0].at[pl.ds(0, ROWS), :], dy_buf.at[slot], sems.at[1, slot]).wait()
    a, dy = a_buf[slot], dy_buf[slot]
    a_t, dy_t = a.T, dy.T
    blocks = [pl.ds(c, min(BLOCK, width - c)) for c in range(0, width, BLOCK)]
    held = {}

    def there(c):
        s = blocks[c]
        held[c] = hidden_back(dot(a, wg_ref[:, s], NN), dot(a, wu_ref[:, s], NN), dot(dy, wdt_ref[:, s], NN))

    def back(c):
        s = blocks[c]
        dg, du, hid = held.pop(c)
        for acc, left, right in ((accg_ref, a_t, dg), (accu_ref, a_t, du), (accd_ref, dy_t, hid)):
            acc[:, s] = jnp.where(i == 0, 0.0, acc[:, s]) + dot(left, right, NN)

    there(0)
    for c in range(1, len(blocks)):
        there(c)
        back(c - 1)
    back(len(blocks) - 1)

    rest = pl.ds(own, width - own)

    @pl.when(lax.rem(i, each) == each - 1)
    def _():
        for acc, term in zip((accg_ref, accu_ref, accd_ref), terms, strict=True):
            term[i // each] = acc[:, rest]
            acc[:, rest] = jnp.zeros_like(acc[:, rest])

    @pl.when(i == steps - 1)
    def _():
        sums = [None, None]
        for acc, term, out, out_s, turned in (
            (accg_ref, terms[0], *outs[0:4:3], False),
            (accu_ref, terms[1], *outs[1:5:3], False),
            (accd_ref, terms[2], *outs[2:6:3], True),
        ):
            at = [(core + s) % 2 + 2 * ((chip + s // 2) % 2) for s in range(4)]
            whole = term[at[0]] + term[at[1]] + term[at[2]] + term[at[3]]
            for c in range(0, width, LANES):
                part = (acc[:, c : c + LANES] if c < own else whole[:, c - own : c - own + LANES]).astype(BF16)
                ref, place = (out, pl.ds(c, LANES)) if c < own else (out_s, pl.ds(c - own, LANES))
                if turned:
                    ref[place, :] = part.T
                else:
                    ref[:, place] = part
                square = part.astype(F32)
                square = jnp.sum((square * square).reshape(-1, 8, LANES), 0)
                sums[c >= own] = square if sums[c >= own] is None else sums[c >= own] + square
        if not final:
            outs[6][...], outs[7][...] = sums
        else:
            sums_ref[0] = sums[0] + before[0][...]
            shared = jnp.sum(sums[1] + before[1][...])
            for n in range(3):
                told(n).start()
            for n in range(3):
                told(n).wait()
            total = sums_ref[at[0]] + sums_ref[at[1]] + sums_ref[at[2]] + sums_ref[at[3]]
            total = jnp.full((8, LANES), jnp.sum(total) + shared, F32)
            outs[6][...] = jnp.minimum(1.0, 0.5 * lax.rsqrt(total / count + 1e-30))
            outs[7][...] = jnp.zeros((8, LANES), F32)


def slices(layer, own, a_all, dy_all, wg, wu, wd, before=None, count=None):
    tokens, d = a_all[0].shape
    ff = wg.shape[2]
    rest = ff - 4 * own
    width = own + rest
    any_ = pl.BlockSpec(memory_space=pl.ANY)
    at = lambda s: once(s, lambda i: (0, 0))
    sizes = [(d, own), (d, own), (own, d), (d, rest), (d, rest), (rest, d)]
    return pl.pallas_call(
        lambda *refs: slices_kernel(layer, own, count, *refs),
        grid=(4 * tokens // ROWS,),
        in_specs=[any_] * 9 + [at((8, LANES))] * len(before or ()),
        out_specs=[at(s) for s in sizes] + [at((8, LANES))] * 2,
        scratch_shapes=[pltpu.VMEM((d, width), BF16)] * 2
        + [pltpu.VMEM((width, d), BF16)]
        + [pltpu.VMEM((d, width), F32)] * 3
        + [pltpu.VMEM((2, ROWS, d), BF16)] * 2
        + [pltpu.VMEM((tokens, d), BF16)] * 2
        + [pltpu.VMEM((4, 8, LANES), F32)]
        + [pltpu.SemaphoreType.DMA(n) for n in ((2, 2), (3, 2), (5,), (5,))]
        + [pltpu.VMEM((d, width), BF16)]
        + [pltpu.VMEM((4, d, rest), F32)] * 3,
        out_shape=[jax.ShapeDtypeStruct(s, BF16) for s in sizes] + [jax.ShapeDtypeStruct((8, LANES), F32)] * 2,
        cost_estimate=pl.CostEstimate(
            flops=12 * 4 * tokens * d * width, bytes_accessed=16 * tokens * d, transcendentals=4 * tokens * width
        ),
        compiler_params=pltpu.CompilerParams(vmem_limit_bytes=62 << 20, collective_id=layer, has_side_effects=True),
        name="slices",
    )(*a_all, *dy_all, wg, wu, wd, *(before or ()))


def adam_math(f, w, m, v, g):
    g = g.astype(F32) * f
    m = 0.9 * m + 0.1 * g
    v = 0.95 * v + 0.05 * g * g
    return (0.998 * w.astype(F32) - 0.02 * (m * lax.rsqrt(v + 1e-8))).astype(BF16), m, v


SLOTS, AHEAD = 6, 3


def adam(own, factor, who, arrays, pieces, outs):
    d, _ = arrays[0][0].shape[1:]
    shapes = ((LANES, own), (LANES, d), (d, LANES))
    rows = []
    for n, (which, layer, slot, g) in enumerate(pieces):
        kind = 1 if which == 2 else 2 if slot == 4 else 0
        for r in range(0, g.shape[0], shapes[kind][0]):
            rows.append((kind, which, layer, n, slot, r, *((own, 0) if which == 2 else (0, own))))
    table = np.array(rows, np.int32).T
    total = len(rows)
    kinds = sorted({row[0] for row in rows})
    n_in = 9 + len(pieces)

    def kernel(table_ref, who_ref, f_ref, *refs):
        weights, grads = refs[:9], refs[9:n_in]
        refs = refs[n_in + (9 if outs is not None else 0) :]
        results, scratch = refs[:9], refs[9:]
        buffers = {kind: scratch[4 * n : 4 * n + 4] for n, kind in enumerate(kinds)}
        sem_in, sem_out = scratch[-2:]
        f = f_ref[0]

        def place(step):
            kind, which, layer = (table_ref[n, step] for n in range(3))
            unit = who_ref[table_ref[4, step]]
            row, col = table_ref[5, step] + table_ref[6, step] * unit, table_ref[7, step] * unit
            return kind, which, lambda shape: (layer, pl.ds(pl.multiple_of(row, 16), shape[0]), pl.ds(pl.multiple_of(col, LANES), shape[1]))

        def fetch(step):
            slot = lax.rem(step, SLOTS)
            kind, which, at = place(step)
            for k in range(3):
                its = [q for q in kinds if (q == 1) == (k == 2)]
                for q in its:

                    @pl.when((which == k) & (kind == q))
                    def _():
                        for n in range(3):
                            pltpu.make_async_copy(weights[3 * k + n].at[at(shapes[q])], buffers[q][n].at[slot], sem_in.at[n, slot]).start()

            piece, row = table_ref[3, step], table_ref[5, step]
            for n, (which_, _, slot_, _) in enumerate(pieces):
                q = 1 if which_ == 2 else 2 if slot_ == 4 else 0

                @pl.when(piece == n)
                def _():
                    rows_ = pl.ds(pl.multiple_of(row, 16), shapes[q][0])
                    pltpu.make_async_copy(grads[n].at[rows_, :], buffers[q][3].at[slot], sem_in.at[3, slot]).start()

        def stored(step, do):
            slot = lax.rem(step, SLOTS)
            kind, which, at = place(step)
            for k in range(3):
                for q in [q for q in kinds if (q == 1) == (k == 2)]:

                    @pl.when((which == k) & (kind == q))
                    def _():
                        for n in range(3):
                            do(pltpu.make_async_copy(buffers[q][n].at[slot], results[3 * k + n].at[at(shapes[q])], sem_out.at[n, slot]))

        for step in range(min(AHEAD, total)):
            fetch(jnp.int32(step))

        def body(step, carry):
            @pl.when(step + AHEAD < total)
            def _():
                @pl.when(step + AHEAD >= SLOTS)
                def _():
                    stored(step + AHEAD - SLOTS, lambda copy: copy.wait())

                fetch(step + AHEAD)

            slot = lax.rem(step, SLOTS)
            for q in kinds:

                @pl.when(table_ref[0, step] == q)
                def _():
                    w, m, v, g = buffers[q]
                    for n in range(3):
                        pltpu.make_async_copy(weights[n].at[0, pl.ds(0, shapes[q][0]), pl.ds(0, shapes[q][1])], buffers[q][n].at[slot], sem_in.at[n, slot]).wait()
                    pltpu.make_async_copy(buffers[q][3].at[slot], buffers[q][3].at[slot], sem_in.at[3, slot]).wait()
                    some = 32 if shapes[q][1] > LANES else 224

                    def part(r, carry):
                        at = pl.ds(pl.multiple_of(r * some, some), some)
                        new = adam_math(f, w[slot, at, :], m[slot, at, :], v[slot, at, :], g[slot, at, :])
                        w[slot, at, :], m[slot, at, :], v[slot, at, :] = new
                        return carry

                    lax.fori_loop(0, shapes[q][0] // some, part, 0)

            stored(step, lambda copy: copy.start())
            return carry

        lax.fori_loop(0, total, body, 0)
        for step in range(max(0, total - SLOTS), total):
            stored(jnp.int32(step), lambda copy: copy.wait())

    any_ = pl.BlockSpec(memory_space=pl.ANY)
    given = [a for three in arrays for a in three]
    before = [a for three in outs for a in three] if outs is not None else []
    elements = sum(piece[3].size for piece in pieces)
    new = pl.pallas_call(
        kernel,
        in_specs=[pl.BlockSpec(memory_space=pltpu.SMEM)] * 3 + [any_] * (n_in + len(before)),
        out_specs=[any_] * 9,
        out_shape=[jax.ShapeDtypeStruct(a.shape, a.dtype) for a in given],
        scratch_shapes=[pltpu.VMEM((SLOTS, *shapes[q]), t) for q in kinds for t in (BF16, F32, F32, BF16)]
        + [pltpu.SemaphoreType.DMA((4, SLOTS)), pltpu.SemaphoreType.DMA((3, SLOTS))],
        input_output_aliases={3 + n_in + n: n for n in range(len(before))},
        cost_estimate=pl.CostEstimate(flops=2000 * elements, bytes_accessed=22 * elements, transcendentals=elements),
        compiler_params=params(),
    )(table, who, factor, *given, *(piece[3] for piece in pieces), *before)
    return tuple(tuple(new[3 * n : 3 * n + 3]) for n in range(3))


def solution(mesh):
    def step(x, dy, wg, wu, wd, mg, mu, md, vg, vu, vd):
        me = lax.axis_index("dp")
        places = jnp.arange(5, dtype=jnp.int32)
        who = jnp.where(places < 4, me ^ places, places)
        x, dy = x[0], dy[0]
        ff = wg.shape[2]
        own = ff // LANES // 4 * LANES

        def send(a, perm):
            return perm(a)

        dy_x, dy_d = send(dy, px), send(dy, pd)
        h1, a1, a0 = forward(x, wg, wu, wd)
        a1_x, a1_d = send(a1, px), send(a1, pd)
        a0_x, a0_d = send(a0, px), send(a0, pd)
        dh1 = chain(a1, dy, h1, wg, wu, wd)
        dh1_x, dh1_d = send(dh1, px), send(dh1, pd)
        top = slices(1, own, [a1, a1_d, a1_x], [dy, dy_d, dy_x], wg, wu, wd)
        top_x = [send(top[n], px) for n in range(3)]
        top_d = [send(top[n], pd) for n in range(3)]
        low = slices(0, own, [a0, a0_d, a0_x], [dh1, dh1_d, dh1_x], wg, wu, wd, top[6:8], wg.size + wu.size + wd.size)
        factor = low[6][0, :1]
        low_x = [send(low[n], px) for n in range(3)]
        low_d = [send(low[n], pd) for n in range(3)]

        top_xd = [send(top_x[n], pd) for n in range(3)]
        low_xd = [send(low_x[n], pd) for n in range(2)]
        arrays = ((wg, mg, vg), (wu, mu, vu), (wd, md, vd))

        def pieces(layer, slot, gs, names=(0, 1, 2)):
            return [(n, layer, slot, gs[n]) for n in names]

        first = pieces(1, 0, top) + pieces(1, 1, top_d) + pieces(1, 2, top_x) + pieces(0, 0, low)
        shared = pieces(1, 4, top[3:6]) + pieces(0, 4, low[3:6])
        outs = adam(own, factor, who, arrays, first + shared, None)
        outs = adam(own, factor, who, arrays, pieces(1, 3, top_xd) + pieces(0, 1, low_d), outs)
        outs, low_x[2] = lax.optimization_barrier((outs, low_x[2]))
        low_xd.append(send(low_x[2], pd))
        outs = adam(own, factor, who, arrays, pieces(0, 2, low_x) + pieces(0, 3, low_xd, (0, 1)), outs)
        outs = adam(own, factor, who, arrays, pieces(0, 3, low_xd, (2,)), outs)
        return tuple(outs[name][which] for which in range(3) for name in range(3))

    return jax.shard_map(
        step,
        mesh=mesh,
        in_specs=(P(("rep", "dp"), None, None),) * 2 + (P(None, None, None),) * 9,
        out_specs=(P("rep", None, None),) * 9,
        check_vma=False,
    )
```

```python
import jax
import jax.numpy as jnp
import numpy as np
from jax import lax
from jax.experimental import pallas as pl
from jax.experimental.pallas import tpu as pltpu
from jax.sharding import PartitionSpec as P


F32, BF16 = jnp.float32, jnp.bfloat16
PX = ((0, 2), (2, 0), (1, 3), (3, 1))
PD = ((0, 1), (1, 0), (2, 3), (3, 2))
NN, NT = ((1,), (0,)), ((1,), (1,))

LANES = 128
BLOCK = 512
ROWS = 512


def dot(a, b, dims):
    return lax.dot_general(a, b, (dims, ((), ())), preferred_element_type=F32)


def sigmoid(x):
    return 0.5 * jnp.tanh(0.5 * x) + 0.5


def px(a):
    return lax.ppermute(a, "dp", PX)


def pd(a):
    return lax.ppermute(a, "dp", PD)


def once(shape, index):
    return pl.BlockSpec(shape, index, pipeline_mode=pl.Buffered(1))


def params(mib=62):
    return pltpu.CompilerParams(vmem_limit_bytes=mib << 20)


def norm_scale(wide):
    return lax.rsqrt(jnp.mean(wide * wide, -1, keepdims=True) + 1e-6)


def normed(h):
    wide = h.astype(F32)
    return (wide * norm_scale(wide)).astype(BF16)


def forward_kernel(tail, x_ref, wg_ref, wu_ref, wd_ref, h_ref, a_ref, a0_ref, acc_ref):
    j, last = pl.program_id(0), pl.num_programs(0) - 1
    tokens = x_ref.shape[0]
    chunks = [pl.ds(r, ROWS) for r in range(0, tokens, ROWS)]

    @pl.when(j == 0)
    def _():
        for r in chunks:
            a0_ref[r, :] = normed(x_ref[r, :])
            acc_ref[r, :] = jnp.zeros((ROWS, acc_ref.shape[1]), F32)

    def block(width):
        hid = {}

        def up(r):
            a = a0_ref[chunks[r], :]
            g = dot(a, wg_ref[0, :, :width], NN)
            u = dot(a, wu_ref[0, :, :width], NN)
            hid[r] = (g * sigmoid(g) * u).astype(BF16)

        def down(r):
            acc_ref[chunks[r], :] += dot(hid.pop(r), wd_ref[0, :width, :], NN)

        up(0)
        for r in range(1, len(chunks)):
            up(r)
            down(r - 1)
        down(len(chunks) - 1)

    @pl.when(j < last)
    def _():
        block(wg_ref.shape[2])

    @pl.when(j == last)
    def _():
        block(tail)
        for r in chunks:
            h = (x_ref[r, :].astype(F32) + acc_ref[r, :].astype(BF16).astype(F32)).astype(BF16)
            h_ref[r, :] = h
            a_ref[r, :] = normed(h)


def forward(x, wg, wu, wd):
    tokens, d = x.shape
    ff = wg.shape[2]
    steps = pl.cdiv(ff, BLOCK)
    full = once((tokens, d), lambda j: (0, 0))
    across = pl.BlockSpec((1, d, BLOCK), lambda j: (0, 0, j))
    down = pl.BlockSpec((1, BLOCK, d), lambda j: (0, j, 0))
    return pl.pallas_call(
        lambda *refs: forward_kernel(ff - (steps - 1) * BLOCK, *refs),
        grid=(steps,),
        in_specs=[full, across, across, down],
        out_specs=[full] * 3,
        out_shape=[jax.ShapeDtypeStruct((tokens, d), BF16)] * 3,
        scratch_shapes=[pltpu.VMEM((tokens, d), F32)],
        cost_estimate=pl.CostEstimate(flops=6 * tokens * d * ff, bytes_accessed=6 * d * ff, transcendentals=tokens * ff),
        compiler_params=params(),
        name="forward",
    )(x, wg, wu, wd)


def hidden_back(g, u, dhid):
    dhid = dhid.astype(BF16).astype(F32)
    sig = sigmoid(g)
    act = g * sig
    return (dhid * u * (sig + act * (1 - sig))).astype(BF16), (dhid * act).astype(BF16), (act * u).astype(BF16)


def chain_kernel(tail, a_ref, dy_ref, h_ref, wg_ref, wu_ref, wd_ref, dh_ref, acc_ref, wgt_ref, wut_ref, wdt_ref):
    j, last = pl.program_id(0), pl.num_programs(0) - 1
    tokens = a_ref.shape[0]
    chunks = [pl.ds(r, ROWS) for r in range(0, tokens, ROWS)]

    @pl.when(j == 0)
    def _():
        for r in chunks:
            acc_ref[r, :] = jnp.zeros((ROWS, acc_ref.shape[1]), F32)

    def block(width):
        held = {}
        wdt_ref[:, :width] = wd_ref[0, :width, :].T
        wgt_ref[:width, :] = wg_ref[0, :, :width].T
        wut_ref[:width, :] = wu_ref[0, :, :width].T

        def there(r):
            a, dy = a_ref[chunks[r], :], dy_ref[chunks[r], :]
            g = dot(a, wg_ref[0, :, :width], NN)
            u = dot(a, wu_ref[0, :, :width], NN)
            dhid = dot(dy, wdt_ref[:, :width], NN)
            held[r] = hidden_back(g, u, dhid)[:2]

        def back(r):
            dg, du = held.pop(r)
            acc_ref[chunks[r], :] += dot(dg, wgt_ref[:width, :], NN) + dot(du, wut_ref[:width, :], NN)

        there(0)
        for r in range(1, len(chunks)):
            there(r)
            back(r - 1)
        back(len(chunks) - 1)

    @pl.when(j < last)
    def _():
        block(wg_ref.shape[2])

    @pl.when(j == last)
    def _():
        block(tail)
        for r in chunks:
            wide, da = h_ref[r, :].astype(F32), acc_ref[r, :].astype(BF16).astype(F32)
            scale = norm_scale(wide)
            back = scale * da - wide * (scale * scale * scale * jnp.mean(wide * da, -1, keepdims=True))
            dh_ref[r, :] = (dy_ref[r, :].astype(F32) + back.astype(BF16).astype(F32)).astype(BF16)


def chain(a, dy, h, wg, wu, wd):
    tokens, d = a.shape
    ff = wg.shape[2]
    steps = pl.cdiv(ff, BLOCK)
    full = once((tokens, d), lambda j: (0, 0))
    across = pl.BlockSpec((1, d, BLOCK), lambda j: (1, 0, j))
    down = pl.BlockSpec((1, BLOCK, d), lambda j: (1, j, 0))
    return pl.pallas_call(
        lambda *refs: chain_kernel(ff - (steps - 1) * BLOCK, *refs),
        grid=(steps,),
        in_specs=[full, full, full, across, across, down],
        out_specs=full,
        out_shape=jax.ShapeDtypeStruct((tokens, d), BF16),
        scratch_shapes=[pltpu.VMEM((tokens, d), F32)] + [pltpu.VMEM((BLOCK, d), BF16)] * 2 + [pltpu.VMEM((d, BLOCK), BF16)],
        cost_estimate=pl.CostEstimate(flops=10 * tokens * d * ff, bytes_accessed=6 * d * ff, transcendentals=tokens * ff),
        compiler_params=params(),
        name="chain",
    )(a, dy, h, wg, wu, wd)


def slices_kernel(layer, own, count, *refs):
    me = lax.axis_index("dp")
    chip, core = me // 2, me % 2
    partner = chip * 2 + 1 - core
    others = (partner, (1 - chip) * 2 + core, (1 - chip) * 2 + 1 - core)
    (a_own, a_across), (dy_own, dy_across), (wg_hbm, wu_hbm, wd_hbm) = refs[:2], refs[2:4], refs[4:7]
    final = count is not None
    before = refs[7:9] if final else ()
    refs = refs[9 if final else 7 :]
    outs, landed, scratch = refs[:8], refs[8:10], refs[10:]
    a_refs = (a_own, landed[0].at[0], a_across, landed[0].at[1])
    dy_refs = (dy_own, landed[1].at[0], dy_across, landed[1].at[1])
    wg_ref, wu_ref, wd_ref, accg_ref, accu_ref, accd_ref, a_buf, dy_buf, sums_ref, sems, w_sems, send_sems, recv_sems, *terms = scratch
    i, steps = pl.program_id(0), pl.num_programs(0)
    each = a_refs[0].shape[0] // ROWS
    width = wg_ref.shape[1]

    def fetch(step, do):
        slot, who = lax.rem(step, 2), step // each
        rows = pl.ds(pl.multiple_of(lax.rem(step, each) * ROWS, ROWS), ROWS)
        for k, (a, dy) in enumerate(zip(a_refs, dy_refs, strict=True)):

            @pl.when(who == k)
            def _():
                do(pltpu.make_async_copy(a.at[rows, :], a_buf.at[slot], sems.at[0, slot]))
                do(pltpu.make_async_copy(dy.at[rows, :], dy_buf.at[slot], sems.at[1, slot]))

    def weights():
        parts = ((pl.ds(pl.multiple_of(me * own, LANES), own), pl.ds(0, own)), (pl.ds(4 * own, width - own), pl.ds(own, width - own)))
        return [
            pltpu.make_async_copy(*((hbm.at[layer, there, :], ref.at[here, :]) if n == 2 else (hbm.at[layer, :, there], ref.at[:, here])), w_sems.at[n, m])
            for n, (hbm, ref) in enumerate(((wg_hbm, wg_ref), (wu_hbm, wu_ref), (wd_hbm, wd_ref)))
            for m, (there, here) in enumerate(parts)
        ]

    def onward(which, n):
        return pltpu.make_async_remote_copy(
            src_ref=(a_refs, dy_refs)[n][2 * which],
            dst_ref=landed[n].at[which],
            send_sem=send_sems.at[2 * which + n],
            recv_sem=recv_sems.at[2 * which + n],
            device_id={"dp": partner},
            device_id_type=pl.DeviceIdType.MESH,
        )

    def told(n):
        return pltpu.make_async_remote_copy(
            src_ref=sums_ref.at[0],
            dst_ref=sums_ref.at[1 + n],
            send_sem=send_sems.at[4 + n],
            recv_sem=recv_sems.at[4 + n],
            device_id={"dp": others[n]},
            device_id_type=pl.DeviceIdType.MESH,
        )

    barrier = pltpu.get_barrier_semaphore()
    spoken = others if final else others[:1]

    @pl.when(i == 0)
    def _():
        for other in spoken:
            pl.semaphore_signal(barrier, inc=1, device_id={"dp": other}, device_id_type=pl.DeviceIdType.MESH)
        fetch(i, lambda copy: copy.start())
        for copy in weights():
            copy.start()
        for copy in weights():
            copy.wait()

    @pl.when(i == 1)
    def _():
        pl.semaphore_wait(barrier, len(spoken))
        for which in range(2):
            for n in range(2):
                onward(which, n).start()

    for which in range(2):

        @pl.when(i == (2 * which + 1) * each - 1)
        def _():
            for n in range(2):
                onward(which, n).wait()

    @pl.when(i + 1 < steps)
    def _():
        fetch(i + 1, lambda copy: copy.start())

    slot = lax.rem(i, 2)
    pltpu.make_async_copy(a_refs[0].at[pl.ds(0, ROWS), :], a_buf.at[slot], sems.at[0, slot]).wait()
    pltpu.make_async_copy(dy_refs[0].at[pl.ds(0, ROWS), :], dy_buf.at[slot], sems.at[1, slot]).wait()
    a, dy = a_buf[slot], dy_buf[slot]
    a_t, dy_t = a.T, dy.T
    blocks = [pl.ds(c, min(BLOCK, width - c)) for c in range(0, width, BLOCK)]
    held = {}

    def there(c):
        s = blocks[c]
        held[c] = hidden_back(dot(a, wg_ref[:, s], NN), dot(a, wu_ref[:, s], NN), dot(dy, wd_ref[s, :], NT))

    def back(c):
        s = blocks[c]
        dg, du, hid = held.pop(c)
        for acc, left, right in ((accg_ref, a_t, dg), (accu_ref, a_t, du), (accd_ref, dy_t, hid)):
            acc[:, s] = jnp.where(i == 0, 0.0, acc[:, s]) + dot(left, right, NN)

    there(0)
    for c in range(1, len(blocks)):
        there(c)
        back(c - 1)
    back(len(blocks) - 1)

    rest = pl.ds(own, width - own)

    @pl.when(lax.rem(i, each) == each - 1)
    def _():
        for acc, term in zip((accg_ref, accu_ref, accd_ref), terms, strict=True):
            term[i // each] = acc[:, rest]
            acc[:, rest] = jnp.zeros_like(acc[:, rest])

    @pl.when(i == steps - 1)
    def _():
        sums = [None, None]
        for acc, term, out, out_s, turned in (
            (accg_ref, terms[0], *outs[0:4:3], False),
            (accu_ref, terms[1], *outs[1:5:3], False),
            (accd_ref, terms[2], *outs[2:6:3], True),
        ):
            at = [(core + s) % 2 + 2 * ((chip + s // 2) % 2) for s in range(4)]
            whole = term[at[0]] + term[at[1]] + term[at[2]] + term[at[3]]
            for c in range(0, width, LANES):
                part = (acc[:, c : c + LANES] if c < own else whole[:, c - own : c - own + LANES]).astype(BF16)
                ref, place = (out, pl.ds(c, LANES)) if c < own else (out_s, pl.ds(c - own, LANES))
                if turned:
                    ref[place, :] = part.T
                else:
                    ref[:, place] = part
                square = part.astype(F32)
                square = jnp.sum((square * square).reshape(-1, 8, LANES), 0)
                sums[c >= own] = square if sums[c >= own] is None else sums[c >= own] + square
        if not final:
            outs[6][...], outs[7][...] = sums
        else:
            sums_ref[0] = sums[0] + before[0][...]
            shared = jnp.sum(sums[1] + before[1][...])
            for n in range(3):
                told(n).start()
            for n in range(3):
                told(n).wait()
            total = sums_ref[at[0]] + sums_ref[at[1]] + sums_ref[at[2]] + sums_ref[at[3]]
            total = jnp.full((8, LANES), jnp.sum(total) + shared, F32)
            outs[6][...] = jnp.minimum(1.0, 0.5 * lax.rsqrt(total / count + 1e-30))
            outs[7][...] = jnp.zeros((8, LANES), F32)


def slices(layer, own, a_all, dy_all, wg, wu, wd, before=None, count=None):
    tokens, d = a_all[0].shape
    ff = wg.shape[2]
    rest = ff - 4 * own
    width = own + rest
    any_ = pl.BlockSpec(memory_space=pl.ANY)
    at = lambda s: once(s, lambda i: (0, 0))
    sizes = [(d, own), (d, own), (own, d), (d, rest), (d, rest), (rest, d)]
    return pl.pallas_call(
        lambda *refs: slices_kernel(layer, own, count, *refs),
        grid=(4 * tokens // ROWS,),
        in_specs=[any_] * 7 + [at((8, LANES))] * len(before or ()),
        out_specs=[at(s) for s in sizes] + [at((8, LANES))] * 2 + [any_] * 2,
        scratch_shapes=[pltpu.VMEM((d, width), BF16)] * 2
        + [pltpu.VMEM((width, d), BF16)]
        + [pltpu.VMEM((d, width), F32)] * 3
        + [pltpu.VMEM((2, ROWS, d), BF16)] * 2
        + [pltpu.VMEM((4, 8, LANES), F32)]
        + [pltpu.SemaphoreType.DMA(n) for n in ((2, 2), (3, 2), (7,), (7,))]
        + [pltpu.VMEM((4, d, rest), F32)] * 3,
        out_shape=[jax.ShapeDtypeStruct(s, BF16) for s in sizes] + [jax.ShapeDtypeStruct((8, LANES), F32)] * 2
        + [jax.ShapeDtypeStruct((2, tokens, d), BF16)] * 2,
        cost_estimate=pl.CostEstimate(
            flops=12 * 4 * tokens * d * width, bytes_accessed=16 * tokens * d, transcendentals=4 * tokens * width
        ),
        compiler_params=pltpu.CompilerParams(vmem_limit_bytes=62 << 20, collective_id=layer, has_side_effects=True),
        name="slices",
    )(*a_all, *dy_all, wg, wu, wd, *(before or ()))


def adam_math(f, w, m, v, g):
    g = g.astype(F32) * f
    m = 0.9 * m + 0.1 * g
    v = 0.95 * v + 0.05 * g * g
    return (0.998 * w.astype(F32) - 0.02 * (m * lax.rsqrt(v + 1e-8))).astype(BF16), m, v


SLOTS, AHEAD = 8, 4


def adam(own, factor, arrays, pieces, outs):
    d, _ = arrays[0][0].shape[1:]
    shapes = ((LANES, own), (LANES, d), (d, LANES))
    rows = []
    for n, (which, layer, slot, g) in enumerate(pieces):
        kind = 1 if which == 2 else 2 if slot == 4 else 0
        for r in range(0, g.shape[0], shapes[kind][0]):
            rows.append((kind, which, layer, n, slot, r, *((own, 0) if which == 2 else (0, own))))
    table = np.array(rows, np.int32).T
    total = len(rows)
    kinds = sorted({row[0] for row in rows})
    n_in = 9 + len(pieces)

    def kernel(table_ref, f_ref, *refs):
        weights, grads = refs[:9], refs[9:n_in]
        refs = refs[n_in + (9 if outs is not None else 0) :]
        results, scratch = refs[:9], refs[9:]
        buffers = {kind: scratch[4 * n : 4 * n + 4] for n, kind in enumerate(kinds)}
        sem_in, sem_out = scratch[-2:]
        f = f_ref[:1, :1]
        me = lax.axis_index("dp")

        def place(step):
            kind, which, layer = (table_ref[n, step] for n in range(3))
            slot = table_ref[4, step]
            unit = jnp.where(slot < 4, (me + slot) % 2 + 2 * ((me // 2 + slot // 2) % 2), slot)
            row, col = table_ref[5, step] + table_ref[6, step] * unit, table_ref[7, step] * unit
            return kind, which, lambda shape: (layer, pl.ds(pl.multiple_of(row, 16), shape[0]), pl.ds(pl.multiple_of(col, LANES), shape[1]))

        def fetch(step):
            slot = lax.rem(step, SLOTS)
            kind, which, at = place(step)
            for k in range(3):
                its = [q for q in kinds if (q == 1) == (k == 2)]
                for q in its:

                    @pl.when((which == k) & (kind == q))
                    def _():
                        for n in range(3):
                            pltpu.make_async_copy(weights[3 * k + n].at[at(shapes[q])], buffers[q][n].at[slot], sem_in.at[n, slot]).start()

            piece, row = table_ref[3, step], table_ref[5, step]
            for n, (which_, _, slot_, _) in enumerate(pieces):
                q = 1 if which_ == 2 else 2 if slot_ == 4 else 0

                @pl.when(piece == n)
                def _():
                    rows_ = pl.ds(pl.multiple_of(row, 16), shapes[q][0])
                    pltpu.make_async_copy(grads[n].at[rows_, :], buffers[q][3].at[slot], sem_in.at[3, slot]).start()

        def stored(step, do):
            slot = lax.rem(step, SLOTS)
            kind, which, at = place(step)
            for k in range(3):
                for q in [q for q in kinds if (q == 1) == (k == 2)]:

                    @pl.when((which == k) & (kind == q))
                    def _():
                        for n in range(3):
                            do(pltpu.make_async_copy(buffers[q][n].at[slot], results[3 * k + n].at[at(shapes[q])], sem_out.at[n, slot]))

        for step in range(min(AHEAD, total)):
            fetch(jnp.int32(step))

        def body(step, carry):
            @pl.when(step + AHEAD < total)
            def _():
                @pl.when(step + AHEAD >= SLOTS)
                def _():
                    stored(step + AHEAD - SLOTS, lambda copy: copy.wait())

                fetch(step + AHEAD)

            slot = lax.rem(step, SLOTS)
            for q in kinds:

                @pl.when(table_ref[0, step] == q)
                def _():
                    w, m, v, g = buffers[q]
                    for n in range(3):
                        pltpu.make_async_copy(weights[n].at[0, pl.ds(0, shapes[q][0]), pl.ds(0, shapes[q][1])], buffers[q][n].at[slot], sem_in.at[n, slot]).wait()
                    pltpu.make_async_copy(buffers[q][3].at[slot], buffers[q][3].at[slot], sem_in.at[3, slot]).wait()
                    some = 32 if shapes[q][1] > LANES else 224

                    def part(r, carry):
                        at = pl.ds(pl.multiple_of(r * some, some), some)
                        new = adam_math(f, w[slot, at, :], m[slot, at, :], v[slot, at, :], g[slot, at, :])
                        w[slot, at, :], m[slot, at, :], v[slot, at, :] = new
                        return carry

                    lax.fori_loop(0, shapes[q][0] // some, part, 0)

            stored(step, lambda copy: copy.start())
            return carry

        lax.fori_loop(0, total, body, 0)
        for step in range(max(0, total - SLOTS), total):
            stored(jnp.int32(step), lambda copy: copy.wait())

    any_ = pl.BlockSpec(memory_space=pl.ANY)
    given = [a for three in arrays for a in three]
    before = [a for three in outs for a in three] if outs is not None else []
    elements = sum(piece[3].size for piece in pieces)
    new = pl.pallas_call(
        kernel,
        in_specs=[pl.BlockSpec(memory_space=pltpu.SMEM), pl.BlockSpec(memory_space=pltpu.VMEM)] + [any_] * (n_in + len(before)),
        out_specs=[any_] * 9,
        out_shape=[jax.ShapeDtypeStruct(a.shape, a.dtype) for a in given],
        scratch_shapes=[pltpu.VMEM((SLOTS, *shapes[q]), t) for q in kinds for t in (BF16, F32, F32, BF16)]
        + [pltpu.SemaphoreType.DMA((4, SLOTS)), pltpu.SemaphoreType.DMA((3, SLOTS))],
        input_output_aliases={2 + n_in + n: n for n in range(len(before))},
        cost_estimate=pl.CostEstimate(flops=2000 * elements, bytes_accessed=22 * elements, transcendentals=elements),
        compiler_params=params(),
    )(table, factor, *given, *(piece[3] for piece in pieces), *before)
    return tuple(tuple(new[3 * n : 3 * n + 3]) for n in range(3))


def solution(mesh):
    def step(x, dy, wg, wu, wd, mg, mu, md, vg, vu, vd):
        x, dy = x[0], dy[0]
        ff = wg.shape[2]
        own = ff // LANES // 4 * LANES

        def send(a, perm):
            return perm(a)

        dy_x = send(dy, px)
        h1, a1, a0 = forward(x, wg, wu, wd)
        a1_x = send(a1, px)
        a0_x = send(a0, px)
        dh1 = chain(a1, dy, h1, wg, wu, wd)
        dh1_x = send(dh1, px)
        top = slices(1, own, [a1, a1_x], [dy, dy_x], wg, wu, wd)
        top_x = [send(top[n], px) for n in range(3)]
        top_d = [send(top[n], pd) for n in range(3)]
        low = slices(0, own, [a0, a0_x], [dh1, dh1_x], wg, wu, wd, top[6:8], wg.size + wu.size + wd.size)
        low_x = [send(low[n], px) for n in range(3)]
        low_d = [send(low[n], pd) for n in range(3)]

        top_xd = [send(top_x[n], pd) for n in range(3)]
        low_xd = [send(low_x[n], pd) for n in range(2)]
        arrays = ((wg, mg, vg), (wu, mu, vu), (wd, md, vd))

        def pieces(layer, slot, gs, names=(0, 1, 2)):
            return [(n, layer, slot, gs[n]) for n in names]

        first = pieces(1, 0, top) + pieces(1, 1, top_d) + pieces(1, 2, top_x) + pieces(0, 0, low)
        shared = pieces(1, 4, top[3:6]) + pieces(0, 4, low[3:6])
        outs = adam(own, low[6], arrays, first + shared, None)
        outs = adam(own, low[6], arrays, pieces(1, 3, top_xd) + pieces(0, 1, low_d), outs)
        outs, low_x[2] = lax.optimization_barrier((outs, low_x[2]))
        low_xd.append(send(low_x[2], pd))
        outs = adam(own, low[6], arrays, pieces(0, 2, low_x) + pieces(0, 3, low_xd, (0, 1)), outs)
        outs = adam(own, low[6], arrays, pieces(0, 3, low_xd, (2,)), outs)
        return tuple(outs[name][which] for which in range(3) for name in range(3))

    return jax.shard_map(
        step,
        mesh=mesh,
        in_specs=(P(("rep", "dp"), None, None),) * 2 + (P(None, None, None),) * 9,
        out_specs=(P("rep", None, None),) * 9,
        check_vma=False,
    )
```

```python
import functools

import jax
import jax.numpy as jnp
import numpy as np
from jax import lax
from jax.experimental import pallas as pl
from jax.experimental.pallas import tpu as pltpu
from jax.sharding import PartitionSpec as P


F32, BF16 = jnp.float32, jnp.bfloat16
PX = ((0, 2), (2, 0), (1, 3), (3, 1))
PD = ((0, 1), (1, 0), (2, 3), (3, 2))
NN, NT = ((1,), (0,)), ((1,), (1,))

LANES = 128
BLOCK = 512
ROWS, FEW, TOGETHER = 512, 64, 4


def dot(a, b, dims):
    return lax.dot_general(a, b, (dims, ((), ())), preferred_element_type=F32)


def sigmoid(x):
    return 0.5 * jnp.tanh(0.5 * x) + 0.5


def px(a):
    return lax.ppermute(a, "dp", PX)


def pd(a):
    return lax.ppermute(a, "dp", PD)


def once(shape, index):
    return pl.BlockSpec(shape, index, pipeline_mode=pl.Buffered(1))


def params(mib=62):
    return pltpu.CompilerParams(vmem_limit_bytes=mib << 20)


def norm_scale(wide):
    return lax.rsqrt(jnp.mean(wide * wide, -1, keepdims=True) + 1e-6)


def normed(h):
    wide = h.astype(F32)
    return (wide * norm_scale(wide)).astype(BF16)


def looped(count, rows, body, together=1):
    def one(n, carry):
        for part in range(together):
            body(pl.ds(pl.multiple_of((n * together + part) * rows, rows), rows))
        return carry

    lax.fori_loop(0, count // together, one, 0)


def forward_kernel(tail, x_ref, wg_ref, wu_ref, wd_ref, h_ref, a_ref, a0_ref, acc_ref):
    j, last = pl.program_id(0), pl.num_programs(0) - 1
    tokens = x_ref.shape[0]

    @pl.when(j == 0)
    def _():
        def start(r):
            a0_ref[r, :] = normed(x_ref[r, :])
            acc_ref[r, :] = jnp.zeros((FEW, acc_ref.shape[1]), F32)

        looped(tokens // FEW, FEW, start, TOGETHER)

    def up(r, width):
        a = a0_ref[r, :]
        g = dot(a, wg_ref[0, :, :width], NN)
        u = dot(a, wu_ref[0, :, :width], NN)
        return (g * sigmoid(g) * u).astype(BF16)

    def down(r, hid):
        acc_ref[r, :] += dot(hid, wd_ref[0, : hid.shape[1], :], NN)

    @pl.when(j < last)
    def _():
        chunks = [pl.ds(r, ROWS) for r in range(0, tokens, ROWS)]
        hid = up(chunks[0], wg_ref.shape[2])
        for r, following in zip(chunks, chunks[1:] + [None], strict=True):
            ahead = None if following is None else up(following, wg_ref.shape[2])
            down(r, hid)
            hid = ahead

    @pl.when(j == last)
    def _():
        looped(tokens // ROWS, ROWS, lambda r: down(r, up(r, tail)))

        def end(r):
            h = (x_ref[r, :].astype(F32) + acc_ref[r, :].astype(BF16).astype(F32)).astype(BF16)
            h_ref[r, :] = h
            a_ref[r, :] = normed(h)

        looped(tokens // FEW, FEW, end, TOGETHER)


def forward(x, wg, wu, wd):
    tokens, d = x.shape
    ff = wg.shape[2]
    steps = pl.cdiv(ff, BLOCK)
    full = once((tokens, d), lambda j: (0, 0))
    across = pl.BlockSpec((1, d, BLOCK), lambda j: (0, 0, j))
    down = pl.BlockSpec((1, BLOCK, d), lambda j: (0, j, 0))
    return pl.pallas_call(
        lambda *refs: forward_kernel(ff - (steps - 1) * BLOCK, *refs),
        grid=(steps,),
        in_specs=[full, across, across, down],
        out_specs=[full] * 3,
        out_shape=[jax.ShapeDtypeStruct((tokens, d), BF16)] * 3,
        scratch_shapes=[pltpu.VMEM((tokens, d), F32)],
        cost_estimate=pl.CostEstimate(flops=6 * tokens * d * ff, bytes_accessed=6 * d * ff, transcendentals=tokens * ff),
        compiler_params=params(),
        name="forward",
    )(x, wg, wu, wd)


def hidden_back(g, u, dhid):
    dhid = dhid.astype(BF16).astype(F32)
    sig = sigmoid(g)
    act = g * sig
    return (dhid * u * (sig + act * (1 - sig))).astype(BF16), (dhid * act).astype(BF16), (act * u).astype(BF16)


def chain_kernel(tail, a_ref, dy_ref, h_ref, wg_ref, wu_ref, wd_ref, dh_ref, acc_ref):
    j, last = pl.program_id(0), pl.num_programs(0) - 1
    tokens = a_ref.shape[0]

    @pl.when(j == 0)
    def _():
        def start(r):
            acc_ref[r, :] = jnp.zeros((FEW, acc_ref.shape[1]), F32)

        looped(tokens // FEW, FEW, start, TOGETHER)

    def there(r, width):
        a, dy = a_ref[r, :], dy_ref[r, :]
        g = dot(a, wg_ref[0, :, :width], NN)
        u = dot(a, wu_ref[0, :, :width], NN)
        dhid = dot(dy, wd_ref[0, :width, :], NT)
        return hidden_back(g, u, dhid)[:2]

    def back(r, held):
        dg, du = held
        width = dg.shape[1]
        acc_ref[r, :] += dot(dg, wg_ref[0, :, :width], NT) + dot(du, wu_ref[0, :, :width], NT)

    def two(width, r):
        low, high = (pl.ds(pl.multiple_of(r.start + n * ROWS, ROWS), ROWS) for n in range(2))
        held = there(low, width)
        ahead = there(high, width)
        back(low, held)
        back(high, ahead)

    @pl.when(j < last)
    def _():
        looped(tokens // (2 * ROWS), 2 * ROWS, functools.partial(two, wg_ref.shape[2]))

    @pl.when(j == last)
    def _():
        looped(tokens // (2 * ROWS), 2 * ROWS, functools.partial(two, tail))

        def end(r):
            wide, da = h_ref[r, :].astype(F32), acc_ref[r, :].astype(BF16).astype(F32)
            scale = norm_scale(wide)
            through = scale * da - wide * (scale * scale * scale * jnp.mean(wide * da, -1, keepdims=True))
            dh_ref[r, :] = (dy_ref[r, :].astype(F32) + through.astype(BF16).astype(F32)).astype(BF16)

        looped(tokens // FEW, FEW, end, TOGETHER)


def chain(a, dy, h, wg, wu, wd):
    tokens, d = a.shape
    ff = wg.shape[2]
    steps = pl.cdiv(ff, BLOCK)
    full = once((tokens, d), lambda j: (0, 0))
    across = pl.BlockSpec((1, d, BLOCK), lambda j: (1, 0, j))
    down = pl.BlockSpec((1, BLOCK, d), lambda j: (1, j, 0))
    return pl.pallas_call(
        lambda *refs: chain_kernel(ff - (steps - 1) * BLOCK, *refs),
        grid=(steps,),
        in_specs=[full, full, full, across, across, down],
        out_specs=full,
        out_shape=jax.ShapeDtypeStruct((tokens, d), BF16),
        scratch_shapes=[pltpu.VMEM((tokens, d), F32)],
        cost_estimate=pl.CostEstimate(flops=10 * tokens * d * ff, bytes_accessed=6 * d * ff, transcendentals=tokens * ff),
        compiler_params=params(),
        name="chain",
    )(a, dy, h, wg, wu, wd)


def slices_kernel(layer, own, count, *refs):
    me = lax.axis_index("dp")
    chip, core = me // 2, me % 2
    partner = chip * 2 + 1 - core
    others = (partner, (1 - chip) * 2 + core, (1 - chip) * 2 + 1 - core)
    (a_own, a_across), (dy_own, dy_across), (wg_hbm, wu_hbm, wd_hbm) = refs[:2], refs[2:4], refs[4:7]
    final = count is not None
    before = refs[7:9] if final else ()
    refs = refs[9 if final else 7 :]
    outs, landed, scratch = refs[:8], refs[8:10], refs[10:]
    a_refs = (a_own, landed[0].at[0], a_across, landed[0].at[1])
    dy_refs = (dy_own, landed[1].at[0], dy_across, landed[1].at[1])
    wg_ref, wu_ref, wd_ref, accg_ref, accu_ref, accd_ref, a_buf, dy_buf, sums_ref, sems, w_sems, send_sems, recv_sems, *terms = scratch
    i, steps = pl.program_id(0), pl.num_programs(0)
    each = a_refs[0].shape[0] // ROWS
    width = wg_ref.shape[1]

    def fetch(step, do):
        slot, who = lax.rem(step, 2), step // each
        rows = pl.ds(pl.multiple_of(lax.rem(step, each) * ROWS, ROWS), ROWS)
        for k, (a, dy) in enumerate(zip(a_refs, dy_refs, strict=True)):

            @pl.when(who == k)
            def _():
                do(pltpu.make_async_copy(a.at[rows, :], a_buf.at[slot], sems.at[0, slot]))
                do(pltpu.make_async_copy(dy.at[rows, :], dy_buf.at[slot], sems.at[1, slot]))

    def weights():
        parts = ((pl.ds(pl.multiple_of(me * own, LANES), own), pl.ds(0, own)), (pl.ds(4 * own, width - own), pl.ds(own, width - own)))
        return [
            pltpu.make_async_copy(*((hbm.at[layer, there, :], ref.at[here, :]) if n == 2 else (hbm.at[layer, :, there], ref.at[:, here])), w_sems.at[n, m])
            for n, (hbm, ref) in enumerate(((wg_hbm, wg_ref), (wu_hbm, wu_ref), (wd_hbm, wd_ref)))
            for m, (there, here) in enumerate(parts)
        ]

    def onward(which, n):
        return pltpu.make_async_remote_copy(
            src_ref=(a_refs, dy_refs)[n][2 * which],
            dst_ref=landed[n].at[which],
            send_sem=send_sems.at[2 * which + n],
            recv_sem=recv_sems.at[2 * which + n],
            device_id={"dp": partner},
            device_id_type=pl.DeviceIdType.MESH,
        )

    def told(n):
        return pltpu.make_async_remote_copy(
            src_ref=sums_ref.at[0],
            dst_ref=sums_ref.at[1 + n],
            send_sem=send_sems.at[4 + n],
            recv_sem=recv_sems.at[4 + n],
            device_id={"dp": others[n]},
            device_id_type=pl.DeviceIdType.MESH,
        )

    barrier = pltpu.get_barrier_semaphore()
    spoken = others if final else others[:1]

    @pl.when(i == 0)
    def _():
        for other in spoken:
            pl.semaphore_signal(barrier, inc=1, device_id={"dp": other}, device_id_type=pl.DeviceIdType.MESH)
        fetch(i, lambda copy: copy.start())
        for copy in weights():
            copy.start()
        for copy in weights():
            copy.wait()

    @pl.when(i == 1)
    def _():
        pl.semaphore_wait(barrier, len(spoken))
        for which in range(2):
            for n in range(2):
                onward(which, n).start()

    for which in range(2):

        @pl.when(i == (2 * which + 1) * each - 1)
        def _():
            for n in range(2):
                onward(which, n).wait()

    @pl.when(i + 1 < steps)
    def _():
        fetch(i + 1, lambda copy: copy.start())

    slot = lax.rem(i, 2)
    pltpu.make_async_copy(a_refs[0].at[pl.ds(0, ROWS), :], a_buf.at[slot], sems.at[0, slot]).wait()
    pltpu.make_async_copy(dy_refs[0].at[pl.ds(0, ROWS), :], dy_buf.at[slot], sems.at[1, slot]).wait()
    a, dy = a_buf[slot], dy_buf[slot]
    a_t, dy_t = a.T, dy.T
    blocks = [pl.ds(c, min(BLOCK, width - c)) for c in range(0, width, BLOCK)]
    held = {}

    def there(c):
        s = blocks[c]
        held[c] = hidden_back(dot(a, wg_ref[:, s], NN), dot(a, wu_ref[:, s], NN), dot(dy, wd_ref[s, :], NT))

    def back(c):
        s = blocks[c]
        dg, du, hid = held.pop(c)
        for acc, left, right in ((accg_ref, a_t, dg), (accu_ref, a_t, du), (accd_ref, dy_t, hid)):
            acc[:, s] = jnp.where(i == 0, 0.0, acc[:, s]) + dot(left, right, NN)

    there(0)
    for c in range(1, len(blocks)):
        there(c)
        back(c - 1)
    back(len(blocks) - 1)

    rest = pl.ds(own, width - own)

    @pl.when(lax.rem(i, each) == each - 1)
    def _():
        for acc, term in zip((accg_ref, accu_ref, accd_ref), terms, strict=True):
            term[i // each] = acc[:, rest]
            acc[:, rest] = jnp.zeros_like(acc[:, rest])

    @pl.when(i == steps - 1)
    def _():
        def rounded(part, total):
            part = part.astype(BF16)
            wide = part.astype(F32)
            return part, total + jnp.sum((wide * wide).reshape(-1, 8, LANES), 0)

        accs = (accg_ref, accu_ref, accd_ref)

        def rows(r, total):
            at = pl.ds(pl.multiple_of(r * LANES, LANES), LANES)
            for n, acc in enumerate(accs):
                for c in range(0, own, LANES):
                    part, total = rounded(acc[at, c : c + LANES], total)
                    if n < 2:
                        outs[n][at, c : c + LANES] = part
            return total

        def turn(c, carry):
            at = pl.ds(pl.multiple_of(c * LANES, LANES), LANES)
            for r in range(0, a.shape[1], LANES):
                outs[2][at, r : r + LANES] = accd_ref[r : r + LANES, at].astype(BF16).T
            return carry

        at = [(core + s) % 2 + 2 * ((chip + s // 2) % 2) for s in range(4)]
        sums = [lax.fori_loop(0, a.shape[1] // LANES, rows, jnp.zeros((8, LANES), F32)), jnp.zeros((8, LANES), F32)]
        lax.fori_loop(0, own // LANES, turn, 0)
        for n, term in enumerate(terms):
            part, sums[1] = rounded(term[at[0]] + term[at[1]] + term[at[2]] + term[at[3]], sums[1])
            outs[3 + n][...] = part if n < 2 else part.T
        if not final:
            outs[6][...], outs[7][...] = sums
        else:
            sums_ref[0] = sums[0] + before[0][...]
            shared = jnp.sum(sums[1] + before[1][...])
            for n in range(3):
                told(n).start()
            for n in range(3):
                told(n).wait()
            total = sums_ref[at[0]] + sums_ref[at[1]] + sums_ref[at[2]] + sums_ref[at[3]]
            total = jnp.full((8, LANES), jnp.sum(total) + shared, F32)
            outs[6][...] = jnp.minimum(1.0, 0.5 * lax.rsqrt(total / count + 1e-30))
            outs[7][...] = jnp.zeros((8, LANES), F32)


def slices(layer, own, a_all, dy_all, wg, wu, wd, before=None, count=None):
    tokens, d = a_all[0].shape
    ff = wg.shape[2]
    rest = ff - 4 * own
    width = own + rest
    any_ = pl.BlockSpec(memory_space=pl.ANY)
    at = lambda s: once(s, lambda i: (0, 0))
    sizes = [(d, own), (d, own), (own, d), (d, rest), (d, rest), (rest, d)]
    return pl.pallas_call(
        lambda *refs: slices_kernel(layer, own, count, *refs),
        grid=(4 * tokens // ROWS,),
        in_specs=[any_] * 7 + [at((8, LANES))] * len(before or ()),
        out_specs=[at(s) for s in sizes] + [at((8, LANES))] * 2 + [any_] * 2,
        scratch_shapes=[pltpu.VMEM((d, width), BF16)] * 2
        + [pltpu.VMEM((width, d), BF16)]
        + [pltpu.VMEM((d, width), F32)] * 3
        + [pltpu.VMEM((2, ROWS, d), BF16)] * 2
        + [pltpu.VMEM((4, 8, LANES), F32)]
        + [pltpu.SemaphoreType.DMA(n) for n in ((2, 2), (3, 2), (7,), (7,))]
        + [pltpu.VMEM((4, d, rest), F32)] * 3,
        out_shape=[jax.ShapeDtypeStruct(s, BF16) for s in sizes] + [jax.ShapeDtypeStruct((8, LANES), F32)] * 2
        + [jax.ShapeDtypeStruct((2, tokens, d), BF16)] * 2,
        cost_estimate=pl.CostEstimate(
            flops=12 * 4 * tokens * d * width, bytes_accessed=16 * tokens * d, transcendentals=4 * tokens * width
        ),
        compiler_params=pltpu.CompilerParams(vmem_limit_bytes=62 << 20, collective_id=layer, has_side_effects=True),
        name="slices",
    )(*a_all, *dy_all, wg, wu, wd, *(before or ()))


def adam_math(f, w, m, v, g):
    g = g.astype(F32) * f
    m = 0.9 * m + 0.1 * g
    v = 0.95 * v + 0.05 * g * g
    return (0.998 * w.astype(F32) - 0.02 * (m * lax.rsqrt(v + 1e-8))).astype(BF16), m, v


SLOTS, AHEAD = 8, 4


def adam(own, factor, arrays, pieces, outs):
    d, _ = arrays[0][0].shape[1:]
    shapes = ((LANES, own), (LANES, d), (d, LANES))
    rows = []
    for n, (which, layer, slot, g) in enumerate(pieces):
        kind = 1 if which == 2 else 2 if slot == 4 else 0
        for r in range(0, g.shape[0], shapes[kind][0]):
            rows.append((kind, which, layer, n, slot, r, *((own, 0) if which == 2 else (0, own))))
    table = np.array(rows, np.int32).T
    total = len(rows)
    kinds = sorted({row[0] for row in rows})
    n_in = 9 + len(pieces)

    def kernel(table_ref, f_ref, *refs):
        weights, grads = refs[:9], refs[9:n_in]
        refs = refs[n_in + (9 if outs is not None else 0) :]
        results, scratch = refs[:9], refs[9:]
        buffers = {kind: scratch[4 * n : 4 * n + 4] for n, kind in enumerate(kinds)}
        sem_in, sem_out = scratch[-2:]
        f = f_ref[:1, :1]
        me = lax.axis_index("dp")

        def place(step):
            kind, which, layer = (table_ref[n, step] for n in range(3))
            slot = table_ref[4, step]
            unit = jnp.where(slot < 4, (me + slot) % 2 + 2 * ((me // 2 + slot // 2) % 2), slot)
            row, col = table_ref[5, step] + table_ref[6, step] * unit, table_ref[7, step] * unit
            return kind, which, lambda shape: (layer, pl.ds(pl.multiple_of(row, 16), shape[0]), pl.ds(pl.multiple_of(col, LANES), shape[1]))

        def fetch(step):
            slot = lax.rem(step, SLOTS)
            kind, which, at = place(step)
            for k in range(3):
                its = [q for q in kinds if (q == 1) == (k == 2)]
                for q in its:

                    @pl.when((which == k) & (kind == q))
                    def _():
                        for n in range(3):
                            pltpu.make_async_copy(weights[3 * k + n].at[at(shapes[q])], buffers[q][n].at[slot], sem_in.at[n, slot]).start()

            piece, row = table_ref[3, step], table_ref[5, step]
            for n, (which_, _, slot_, _) in enumerate(pieces):
                q = 1 if which_ == 2 else 2 if slot_ == 4 else 0

                @pl.when(piece == n)
                def _():
                    rows_ = pl.ds(pl.multiple_of(row, 16), shapes[q][0])
                    pltpu.make_async_copy(grads[n].at[rows_, :], buffers[q][3].at[slot], sem_in.at[3, slot]).start()

        def stored(step, do):
            slot = lax.rem(step, SLOTS)
            kind, which, at = place(step)
            for k in range(3):
                for q in [q for q in kinds if (q == 1) == (k == 2)]:

                    @pl.when((which == k) & (kind == q))
                    def _():
                        for n in range(3):
                            do(pltpu.make_async_copy(buffers[q][n].at[slot], results[3 * k + n].at[at(shapes[q])], sem_out.at[n, slot]))

        for step in range(min(AHEAD, total)):
            fetch(jnp.int32(step))

        def body(step, carry):
            @pl.when(step + AHEAD < total)
            def _():
                @pl.when(step + AHEAD >= SLOTS)
                def _():
                    stored(step + AHEAD - SLOTS, lambda copy: copy.wait())

                fetch(step + AHEAD)

            slot = lax.rem(step, SLOTS)
            for q in kinds:

                @pl.when(table_ref[0, step] == q)
                def _():
                    w, m, v, g = buffers[q]
                    for n in range(3):
                        pltpu.make_async_copy(weights[n].at[0, pl.ds(0, shapes[q][0]), pl.ds(0, shapes[q][1])], buffers[q][n].at[slot], sem_in.at[n, slot]).wait()
                    pltpu.make_async_copy(buffers[q][3].at[slot], buffers[q][3].at[slot], sem_in.at[3, slot]).wait()
                    some = 32 if shapes[q][1] > LANES else 224

                    def part(r, carry):
                        at = pl.ds(pl.multiple_of(r * some, some), some)
                        new = adam_math(f, w[slot, at, :], m[slot, at, :], v[slot, at, :], g[slot, at, :])
                        w[slot, at, :], m[slot, at, :], v[slot, at, :] = new
                        return carry

                    lax.fori_loop(0, shapes[q][0] // some, part, 0)

            stored(step, lambda copy: copy.start())
            return carry

        lax.fori_loop(0, total, body, 0)
        for step in range(max(0, total - SLOTS), total):
            stored(jnp.int32(step), lambda copy: copy.wait())

    any_ = pl.BlockSpec(memory_space=pl.ANY)
    given = [a for three in arrays for a in three]
    before = [a for three in outs for a in three] if outs is not None else []
    elements = sum(piece[3].size for piece in pieces)
    new = pl.pallas_call(
        kernel,
        in_specs=[pl.BlockSpec(memory_space=pltpu.SMEM), pl.BlockSpec(memory_space=pltpu.VMEM)] + [any_] * (n_in + len(before)),
        out_specs=[any_] * 9,
        out_shape=[jax.ShapeDtypeStruct(a.shape, a.dtype) for a in given],
        scratch_shapes=[pltpu.VMEM((SLOTS, *shapes[q]), t) for q in kinds for t in (BF16, F32, F32, BF16)]
        + [pltpu.SemaphoreType.DMA((4, SLOTS)), pltpu.SemaphoreType.DMA((3, SLOTS))],
        input_output_aliases={2 + n_in + n: n for n in range(len(before))},
        cost_estimate=pl.CostEstimate(flops=2000 * elements, bytes_accessed=22 * elements, transcendentals=elements),
        compiler_params=params(),
    )(table, factor, *given, *(piece[3] for piece in pieces), *before)
    return tuple(tuple(new[3 * n : 3 * n + 3]) for n in range(3))


def solution(mesh):
    def step(x, dy, wg, wu, wd, mg, mu, md, vg, vu, vd):
        x, dy = x[0], dy[0]
        ff = wg.shape[2]
        own = ff // LANES // 4 * LANES

        def send(a, perm):
            return perm(a)

        dy_x = send(dy, px)
        h1, a1, a0 = forward(x, wg, wu, wd)
        a1_x = send(a1, px)
        a0_x = send(a0, px)
        dh1 = chain(a1, dy, h1, wg, wu, wd)
        dh1_x = send(dh1, px)
        top = slices(1, own, [a1, a1_x], [dy, dy_x], wg, wu, wd)
        top_x = [send(top[n], px) for n in range(3)]
        top_d = [send(top[n], pd) for n in range(3)]
        low = slices(0, own, [a0, a0_x], [dh1, dh1_x], wg, wu, wd, top[6:8], wg.size + wu.size + wd.size)
        low_x = [send(low[n], px) for n in range(3)]
        low_d = [send(low[n], pd) for n in range(3)]

        top_xd = [send(top_x[n], pd) for n in range(3)]
        low_xd = [send(low_x[n], pd) for n in range(2)]
        arrays = ((wg, mg, vg), (wu, mu, vu), (wd, md, vd))

        def pieces(layer, slot, gs, names=(0, 1, 2)):
            return [(n, layer, slot, gs[n]) for n in names]

        first = pieces(1, 0, top) + pieces(1, 1, top_d) + pieces(1, 2, top_x) + pieces(0, 0, low)
        shared = pieces(1, 4, top[3:6]) + pieces(0, 4, low[3:6])
        outs = adam(own, low[6], arrays, first + shared, None)
        outs = adam(own, low[6], arrays, pieces(1, 3, top_xd) + pieces(0, 1, low_d), outs)
        outs, low_x[2] = lax.optimization_barrier((outs, low_x[2]))
        low_xd.append(send(low_x[2], pd))
        outs = adam(own, low[6], arrays, pieces(0, 2, low_x) + pieces(0, 3, low_xd, (0, 1)), outs)
        outs = adam(own, low[6], arrays, pieces(0, 3, low_xd, (2,)), outs)
        return tuple(outs[name][which] for which in range(3) for name in range(3))

    return jax.shard_map(
        step,
        mesh=mesh,
        in_specs=(P(("rep", "dp"), None, None),) * 2 + (P(None, None, None),) * 9,
        out_specs=(P("rep", None, None),) * 9,
        check_vma=False,
    )
```

```python
import functools

import jax
import jax.numpy as jnp
import numpy as np
from jax import lax
from jax.experimental import pallas as pl
from jax.experimental.pallas import tpu as pltpu
from jax.sharding import PartitionSpec as P


F32, BF16 = jnp.float32, jnp.bfloat16
PX = ((0, 2), (2, 0), (1, 3), (3, 1))
PD = ((0, 1), (1, 0), (2, 3), (3, 2))
NN, NT = ((1,), (0,)), ((1,), (1,))

LANES = 128
BLOCK = 512
ROWS, FEW, TOGETHER = 512, 64, 4


def dot(a, b, dims):
    return lax.dot_general(a, b, (dims, ((), ())), preferred_element_type=F32)


def sigmoid(x):
    return 0.5 * jnp.tanh(0.5 * x) + 0.5


def px(a):
    return lax.ppermute(a, "dp", PX)


def pd(a):
    return lax.ppermute(a, "dp", PD)


def once(shape, index):
    return pl.BlockSpec(shape, index, pipeline_mode=pl.Buffered(1))


def params(mib=62):
    return pltpu.CompilerParams(vmem_limit_bytes=mib << 20)


def norm_scale(wide):
    return lax.rsqrt(jnp.mean(wide * wide, -1, keepdims=True) + 1e-6)


def normed(h):
    wide = h.astype(F32)
    return (wide * norm_scale(wide)).astype(BF16)


def looped(count, rows, body, together=1):
    def one(n, carry):
        for part in range(together):
            body(pl.ds(pl.multiple_of((n * together + part) * rows, rows), rows))
        return carry

    lax.fori_loop(0, count // together, one, 0)


def forward_kernel(tail, x_ref, wg_ref, wu_ref, wd_ref, h_ref, a_ref, a0_ref, acc_ref):
    j, last = pl.program_id(0), pl.num_programs(0) - 1
    tokens = x_ref.shape[0]

    @pl.when(j == 0)
    def _():
        def start(r):
            a0_ref[r, :] = normed(x_ref[r, :])
            acc_ref[r, :] = jnp.zeros((FEW, acc_ref.shape[1]), F32)

        looped(tokens // FEW, FEW, start, TOGETHER)

    def up(r, width):
        a = a0_ref[r, :]
        g = dot(a, wg_ref[0, :, :width], NN)
        u = dot(a, wu_ref[0, :, :width], NN)
        return (g * sigmoid(g) * u).astype(BF16)

    def down(r, hid):
        acc_ref[r, :] += dot(hid, wd_ref[0, : hid.shape[1], :], NN)

    def two(width, r):
        low, high = (pl.ds(pl.multiple_of(r.start + n * ROWS, ROWS), ROWS) for n in range(2))
        hid = up(low, width)
        ahead = up(high, width)
        down(low, hid)
        down(high, ahead)

    @pl.when(j < last)
    def _():
        looped(tokens // (2 * ROWS), 2 * ROWS, functools.partial(two, wg_ref.shape[2]))

    @pl.when(j == last)
    def _():
        looped(tokens // ROWS, ROWS, lambda r: down(r, up(r, tail)))

        def end(r):
            h = (x_ref[r, :].astype(F32) + acc_ref[r, :].astype(BF16).astype(F32)).astype(BF16)
            h_ref[r, :] = h
            a_ref[r, :] = normed(h)

        looped(tokens // FEW, FEW, end, TOGETHER)


def forward(x, wg, wu, wd):
    tokens, d = x.shape
    ff = wg.shape[2]
    steps = pl.cdiv(ff, BLOCK)
    full = once((tokens, d), lambda j: (0, 0))
    across = pl.BlockSpec((1, d, BLOCK), lambda j: (0, 0, j))
    down = pl.BlockSpec((1, BLOCK, d), lambda j: (0, j, 0))
    return pl.pallas_call(
        lambda *refs: forward_kernel(ff - (steps - 1) * BLOCK, *refs),
        grid=(steps,),
        in_specs=[full, across, across, down],
        out_specs=[full] * 3,
        out_shape=[jax.ShapeDtypeStruct((tokens, d), BF16)] * 3,
        scratch_shapes=[pltpu.VMEM((tokens, d), F32)],
        cost_estimate=pl.CostEstimate(flops=6 * tokens * d * ff, bytes_accessed=6 * d * ff, transcendentals=tokens * ff),
        compiler_params=params(),
        name="forward",
    )(x, wg, wu, wd)


def hidden_back(g, u, dhid):
    dhid = dhid.astype(BF16).astype(F32)
    sig = sigmoid(g)
    act = g * sig
    return (dhid * u * (sig + act * (1 - sig))).astype(BF16), (dhid * act).astype(BF16), (act * u).astype(BF16)


def chain_kernel(tail, own, a_ref, dy_ref, h_ref, wg_ref, wu_ref, wd_ref, dh_ref, mine_ref, theirs_ref, acc_ref, stage_ref, sems):
    j, last = pl.program_id(0), pl.num_programs(0) - 1
    tokens = a_ref.shape[0]
    me = lax.axis_index("dp")
    holders = (me, me // 2 * 2 + 1 - me % 2)
    blocks = own // BLOCK
    extra = own - blocks * BLOCK

    @pl.when(j == 0)
    def _():
        def start(r):
            acc_ref[r, :] = jnp.zeros((FEW, acc_ref.shape[1]), F32)

        looped(tokens // FEW, FEW, start, TOGETHER)

    def written(step, half, do):
        rows = pl.ds(pl.multiple_of(half * 2 * ROWS, 2 * ROWS), 2 * ROWS)
        for n, (out, holder) in enumerate(zip((mine_ref, theirs_ref), holders, strict=True)):

            def copy(here, there):
                do(pltpu.make_async_copy(stage_ref.at[half, :, :, here], out.at[:, rows, there], sems.at[n, half]))

            @pl.when((step < 4 * blocks) & (step // blocks == holder))
            def _():
                copy(pl.ds(0, BLOCK), pl.ds(pl.multiple_of(lax.rem(step, blocks) * BLOCK, BLOCK), BLOCK))

            @pl.when(step == 4 * blocks)
            def _():
                copy(pl.ds(pl.multiple_of(holder * extra, LANES), extra), pl.ds(blocks * BLOCK, extra))

            @pl.when(step == last)
            def _():
                copy(pl.ds(0, tail), pl.ds(own, tail))

    def there(half, n, r, width):
        a, dy = a_ref[r, :], dy_ref[r, :]
        g = dot(a, wg_ref[0, :, :width], NN)
        u = dot(a, wu_ref[0, :, :width], NN)
        held = hidden_back(g, u, dot(dy, wd_ref[0, :width, :], NT))
        for k in range(3):
            stage_ref[half, k, n * ROWS : (n + 1) * ROWS, :width] = held[k]
        return held[:2]

    def back(r, held):
        dg, du = held
        width = dg.shape[1]
        acc_ref[r, :] += dot(dg, wg_ref[0, :, :width], NT) + dot(du, wu_ref[0, :, :width], NT)

    def block(width):
        def two(half, carry):
            @pl.when(j > 0)
            def _():
                written(j - 1, half, lambda copy: copy.wait())

            low, high = (pl.ds(pl.multiple_of((2 * half + n) * ROWS, ROWS), ROWS) for n in range(2))
            held = there(half, 0, low, width)
            ahead = there(half, 1, high, width)
            back(low, held)
            back(high, ahead)
            written(j, half, lambda copy: copy.start())
            return carry

        lax.fori_loop(0, tokens // (2 * ROWS), two, 0)

    @pl.when(j < last)
    def _():
        block(wg_ref.shape[2])

    @pl.when(j == last)
    def _():
        block(tail)

        def end(r):
            wide, da = h_ref[r, :].astype(F32), acc_ref[r, :].astype(BF16).astype(F32)
            scale = norm_scale(wide)
            through = scale * da - wide * (scale * scale * scale * jnp.mean(wide * da, -1, keepdims=True))
            dh_ref[r, :] = (dy_ref[r, :].astype(F32) + through.astype(BF16).astype(F32)).astype(BF16)

        looped(tokens // FEW, FEW, end, TOGETHER)
        for half in range(tokens // (2 * ROWS)):
            written(j, half, lambda copy: copy.wait())


def chain(own, a, dy, h, wg, wu, wd):
    tokens, d = a.shape
    ff = wg.shape[2]
    steps = pl.cdiv(ff, BLOCK)
    tail = ff - (steps - 1) * BLOCK
    full = once((tokens, d), lambda j: (0, 0))
    across = pl.BlockSpec((1, d, BLOCK), lambda j: (1, 0, j))
    down = pl.BlockSpec((1, BLOCK, d), lambda j: (1, j, 0))
    kept = jax.ShapeDtypeStruct((3, tokens, own + tail), BF16)
    return pl.pallas_call(
        lambda *refs: chain_kernel(tail, own, *refs),
        grid=(steps,),
        in_specs=[full, full, full, across, across, down],
        out_specs=[full] + [pl.BlockSpec(memory_space=pl.ANY)] * 2,
        out_shape=[jax.ShapeDtypeStruct((tokens, d), BF16), kept, kept],
        scratch_shapes=[
            pltpu.VMEM((tokens, d), F32),
            pltpu.VMEM((tokens // (2 * ROWS), 3, 2 * ROWS, BLOCK), BF16),
            pltpu.SemaphoreType.DMA((2, tokens // (2 * ROWS))),
        ],
        cost_estimate=pl.CostEstimate(flops=10 * tokens * d * ff, bytes_accessed=6 * d * ff, transcendentals=tokens * ff),
        compiler_params=params(),
        name="chain",
    )(a, dy, h, wg, wu, wd)


def slices_kernel(layer, own, kept, count, *refs):
    me = lax.axis_index("dp")
    chip, core = me // 2, me % 2
    partner = chip * 2 + 1 - core
    others = (partner, (1 - chip) * 2 + core, (1 - chip) * 2 + 1 - core)
    final = count is not None

    def take(n):
        nonlocal refs
        taken, refs = refs[:n], refs[n:]
        return taken

    a_own, a_across, dy_own, dy_across, wg_hbm, wu_hbm, wd_hbm = take(7)
    mine, theirs = take(2) if kept else (None, None)
    before = take(2) if final else ()
    outs, (a_land, dy_land), held_land = take(8), take(2), take(1) if kept else ()
    wg_ref, wu_ref, wd_ref, accg_ref, accu_ref, accd_ref, a_buf, dy_buf, sums_ref = take(9)
    sems, w_sems, send_sems, recv_sems = take(4)
    terms, held_buf = take(3), take(1)[0] if kept else None
    a_refs = (a_own, a_across, a_land.at[0], a_land.at[1])
    dy_refs = (dy_own, dy_across, dy_land.at[0], dy_land.at[1])
    held_refs = (mine, None, held_land[0], None) if kept else (None,) * 4
    i, steps = pl.program_id(0), pl.num_programs(0)
    each = a_own.shape[0] // ROWS
    width = wg_ref.shape[1]
    main = own // BLOCK * BLOCK

    def fetch(step, do):
        slot, who = lax.rem(step, 2), step // each
        rows = pl.ds(pl.multiple_of(lax.rem(step, each) * ROWS, ROWS), ROWS)
        for k, (a, dy, held) in enumerate(zip(a_refs, dy_refs, held_refs, strict=True)):

            @pl.when(who == k)
            def _():
                do(pltpu.make_async_copy(a.at[rows, :], a_buf.at[slot], sems.at[0, slot]))
                do(pltpu.make_async_copy(dy.at[rows, :], dy_buf.at[slot], sems.at[1, slot]))
                if held is not None:
                    do(pltpu.make_async_copy(held.at[:, rows, :], held_buf.at[slot], sems.at[2, slot]))

    def weights():
        extra = own - main
        parts = (
            (pl.ds(pl.multiple_of(me * main, LANES), main), pl.ds(0, main)),
            (pl.ds(pl.multiple_of(4 * main + me * extra, LANES), extra), pl.ds(main, extra)),
            (pl.ds(4 * own, width - own), pl.ds(own, width - own)),
        )
        return [
            pltpu.make_async_copy(*((hbm.at[layer, there, :], ref.at[here, :]) if n == 2 else (hbm.at[layer, :, there], ref.at[:, here])), w_sems.at[n, m])
            for n, (hbm, ref) in enumerate(((wg_hbm, wg_ref), (wu_hbm, wu_ref), (wd_hbm, wd_ref)))
            for m, (there, here) in enumerate(parts)
        ]

    def onward(which):
        pairs = [(a_refs[which], a_land.at[which]), (dy_refs[which], dy_land.at[which])]
        if kept and which == 0:
            pairs.append((theirs, held_land[0]))
        return [
            pltpu.make_async_remote_copy(
                src_ref=src,
                dst_ref=dst,
                send_sem=send_sems.at[3 * which + n],
                recv_sem=recv_sems.at[3 * which + n],
                device_id={"dp": partner},
                device_id_type=pl.DeviceIdType.MESH,
            )
            for n, (src, dst) in enumerate(pairs)
        ]

    def told(n):
        return pltpu.make_async_remote_copy(
            src_ref=sums_ref.at[0],
            dst_ref=sums_ref.at[1 + n],
            send_sem=send_sems.at[6 + n],
            recv_sem=recv_sems.at[6 + n],
            device_id={"dp": others[n]},
            device_id_type=pl.DeviceIdType.MESH,
        )

    barrier = pltpu.get_barrier_semaphore()
    spoken = others if final else others[:1]

    @pl.when(i == 0)
    def _():
        for other in spoken:
            pl.semaphore_signal(barrier, inc=1, device_id={"dp": other}, device_id_type=pl.DeviceIdType.MESH)
        fetch(i, lambda copy: copy.start())
        for copy in weights():
            copy.start()
        for copy in weights():
            copy.wait()

    @pl.when(i == 1)
    def _():
        pl.semaphore_wait(barrier, len(spoken))
        for which in range(2):
            for copy in onward(which):
                copy.start()

    for which in range(2):

        @pl.when(i == (2 + which) * each - 1)
        def _():
            for copy in onward(which):
                copy.wait()

    @pl.when(i + 1 < steps)
    def _():
        fetch(i + 1, lambda copy: copy.start())

    slot = lax.rem(i, 2)
    pltpu.make_async_copy(a_own.at[pl.ds(0, ROWS), :], a_buf.at[slot], sems.at[0, slot]).wait()
    pltpu.make_async_copy(dy_own.at[pl.ds(0, ROWS), :], dy_buf.at[slot], sems.at[1, slot]).wait()
    blocks = [pl.ds(c, min(BLOCK, width - c)) for c in range(0, width, BLOCK)]

    def through(there, first):
        a_t, dy_t = a_buf[slot].T, dy_buf[slot].T

        def back(s, held):
            dg, du, hid = held
            for acc, left, right in ((accg_ref, a_t, dg), (accu_ref, a_t, du), (accd_ref, dy_t, hid)):
                acc[:, s] = (jnp.where(i == 0, 0.0, acc[:, s]) if first else acc[:, s]) + dot(left, right, NN)

        held = there(blocks[0])
        for s, following in zip(blocks, blocks[1:] + [None], strict=True):
            ahead = None if following is None else there(following)
            back(s, held)
            held = ahead

    def anew(s):
        a, dy = a_buf[slot], dy_buf[slot]
        return hidden_back(dot(a, wg_ref[:, s], NN), dot(a, wu_ref[:, s], NN), dot(dy, wd_ref[s, :], NT))

    if kept:
        known = lax.rem(i // each, 2) == 0

        @pl.when(known)
        def _():
            pltpu.make_async_copy(mine.at[:, pl.ds(0, ROWS), :], held_buf.at[slot], sems.at[2, slot]).wait()
            through(lambda s: [held_buf[slot, n, :, s] for n in range(3)], True)

        @pl.when(jnp.logical_not(known))
        def _():
            through(anew, False)

    else:
        through(anew, True)

    rest = pl.ds(own, width - own)

    @pl.when(lax.rem(i, each) == each - 1)
    def _():
        for acc, term in zip((accg_ref, accu_ref, accd_ref), terms, strict=True):
            term[i // each] = acc[:, rest]
            acc[:, rest] = jnp.zeros_like(acc[:, rest])

    @pl.when(i == steps - 1)
    def _():
        def rounded(part, total):
            part = part.astype(BF16)
            wide = part.astype(F32)
            return part, total + jnp.sum((wide * wide).reshape(-1, 8, LANES), 0)

        accs = (accg_ref, accu_ref, accd_ref)

        def rows(r, total):
            at = pl.ds(pl.multiple_of(r * LANES, LANES), LANES)
            for n, acc in enumerate(accs):
                for c in range(0, own, LANES):
                    part, total = rounded(acc[at, c : c + LANES], total)
                    if n < 2:
                        outs[n][at, c : c + LANES] = part
            return total

        def turn(c, carry):
            at = pl.ds(pl.multiple_of(c * LANES, LANES), LANES)
            for r in range(0, a_buf.shape[2], LANES):
                outs[2][at, r : r + LANES] = accd_ref[r : r + LANES, at].astype(BF16).T
            return carry

        at = [(chip + s // 2) % 2 + 2 * ((core + s) % 2) for s in range(4)]
        place = [(core + s) % 2 + 2 * ((chip + s // 2) % 2) for s in range(4)]
        sums = [lax.fori_loop(0, a_buf.shape[2] // LANES, rows, jnp.zeros((8, LANES), F32)), jnp.zeros((8, LANES), F32)]
        lax.fori_loop(0, own // LANES, turn, 0)
        for n, term in enumerate(terms):
            part, sums[1] = rounded(term[at[0]] + term[at[1]] + term[at[2]] + term[at[3]], sums[1])
            outs[3 + n][...] = part if n < 2 else part.T
        if not final:
            outs[6][...], outs[7][...] = sums
        else:
            sums_ref[0] = sums[0] + before[0][...]
            shared = jnp.sum(sums[1] + before[1][...])
            for n in range(3):
                told(n).start()
            for n in range(3):
                told(n).wait()
            total = sums_ref[place[0]] + sums_ref[place[1]] + sums_ref[place[2]] + sums_ref[place[3]]
            total = jnp.full((8, LANES), jnp.sum(total) + shared, F32)
            outs[6][...] = jnp.minimum(1.0, 0.5 * lax.rsqrt(total / count + 1e-30))
            outs[7][...] = jnp.zeros((8, LANES), F32)


def slices(layer, own, a_all, dy_all, wg, wu, wd, kept=(), before=(), count=None):
    tokens, d = a_all[0].shape
    ff = wg.shape[2]
    rest = ff - 4 * own
    width = own + rest
    any_ = pl.BlockSpec(memory_space=pl.ANY)
    at = lambda s: once(s, lambda i: (0, 0))
    sizes = [(d, own), (d, own), (own, d), (d, rest), (d, rest), (rest, d)]
    landed = [(2, tokens, d)] * 2 + ([(3, tokens, width)] if kept else [])
    return pl.pallas_call(
        lambda *refs: slices_kernel(layer, own, bool(kept), count, *refs),
        grid=(4 * tokens // ROWS,),
        in_specs=[any_] * (7 + len(kept)) + [at((8, LANES))] * len(before),
        out_specs=[at(s) for s in sizes] + [at((8, LANES))] * 2 + [any_] * len(landed),
        scratch_shapes=[pltpu.VMEM((d, width), BF16)] * 2
        + [pltpu.VMEM((width, d), BF16)]
        + [pltpu.VMEM((d, width), F32)] * 3
        + [pltpu.VMEM((2, ROWS, d), BF16)] * 2
        + [pltpu.VMEM((4, 8, LANES), F32)]
        + [pltpu.SemaphoreType.DMA(n) for n in ((3, 2), (3, 3), (9,), (9,))]
        + [pltpu.VMEM((4, d, rest), F32)] * 3
        + ([pltpu.VMEM((2, 3, ROWS, width), BF16)] if kept else []),
        out_shape=[jax.ShapeDtypeStruct(s, BF16) for s in sizes]
        + [jax.ShapeDtypeStruct((8, LANES), F32)] * 2
        + [jax.ShapeDtypeStruct(s, BF16) for s in landed],
        cost_estimate=pl.CostEstimate(
            flops=12 * 4 * tokens * d * width, bytes_accessed=16 * tokens * d, transcendentals=4 * tokens * width
        ),
        compiler_params=pltpu.CompilerParams(vmem_limit_bytes=62 << 20, collective_id=layer, has_side_effects=True),
        name="slices",
    )(*a_all, *dy_all, wg, wu, wd, *kept, *before)


def adam_math(f, w, m, v, g):
    g = g.astype(F32) * f
    m = 0.9 * m + 0.1 * g
    v = 0.95 * v + 0.05 * g * g
    return (0.998 * w.astype(F32) - 0.02 * (m * lax.rsqrt(v + 1e-8))).astype(BF16), m, v


SLOTS, AHEAD = 8, 4


def adam(own, factor, arrays, pieces, outs):
    d, _ = arrays[0][0].shape[1:]
    main, extra = own // BLOCK * BLOCK, own % BLOCK
    shapes = ((LANES, own), (LANES, d), (d, LANES))
    rows = []
    for n, (which, layer, slot, g) in enumerate(pieces):
        kind = 1 if which == 2 else 2 if slot == 4 else 0
        for r in range(0, g.shape[0], shapes[kind][0]):
            if kind != 1:
                first = (r, 0)
            elif slot == 4:
                first = (4 * own + r, 0)
            else:
                first = (r, main) if r < main else (4 * main + r - main, extra)
            rows.append((kind, which, layer, n, slot, r, *first))
    table = np.array(rows, np.int32).T
    total = len(rows)
    kinds = sorted({row[0] for row in rows})
    n_in = 9 + len(pieces)

    def kernel(table_ref, f_ref, *refs):
        weights, grads = refs[:9], refs[9:n_in]
        refs = refs[n_in + (9 if outs is not None else 0) :]
        results, scratch = refs[:9], refs[9:]
        buffers = {kind: scratch[4 * n : 4 * n + 4] for n, kind in enumerate(kinds)}
        sem_in, sem_out = scratch[-2:]
        f = f_ref[:1, :1]
        me = lax.axis_index("dp")

        def moved(step, do):
            kind, which, layer = (table_ref[n, step] for n in range(3))
            slot = table_ref[4, step]
            unit = (me + slot) % 2 + 2 * ((me // 2 + slot // 2) % 2)
            row = table_ref[6, step] + table_ref[7, step] * unit
            for k in range(3):
                for q in [q for q in kinds if (q == 1) == (k == 2)]:
                    if q == 0:
                        columns = ((unit * main, 0, main), (4 * main + unit * extra, main, extra))
                    else:
                        columns = ((0 if q == 1 else 4 * own, 0, shapes[q][1]),)

                    @pl.when((which == k) & (kind == q))
                    def _():
                        for first, here, size in columns:
                            first = first if isinstance(first, int) else pl.multiple_of(first, LANES)
                            there = (layer, pl.ds(pl.multiple_of(row, LANES), shapes[q][0]), pl.ds(first, size))
                            do(3 * k, there, buffers[q], (lax.rem(step, SLOTS), slice(None), pl.ds(here, size)))

        def fetch(step):
            slot = lax.rem(step, SLOTS)

            def get(k, there, buffer, here):
                for n in range(3):
                    pltpu.make_async_copy(weights[k + n].at[there], buffer[n].at[here], sem_in.at[n, slot]).start()

            moved(step, get)
            piece, row = table_ref[3, step], table_ref[5, step]
            for n, (which_, _, slot_, _) in enumerate(pieces):
                q = 1 if which_ == 2 else 2 if slot_ == 4 else 0

                @pl.when(piece == n)
                def _():
                    rows_ = pl.ds(pl.multiple_of(row, 16), shapes[q][0])
                    pltpu.make_async_copy(grads[n].at[rows_, :], buffers[q][3].at[slot], sem_in.at[3, slot]).start()

        def stored(step, do):
            slot = lax.rem(step, SLOTS)

            def put(k, there, buffer, here):
                for n in range(3):
                    do(pltpu.make_async_copy(buffer[n].at[here], results[k + n].at[there], sem_out.at[n, slot]))

            moved(step, put)

        def early(step, carry):
            fetch(step)
            return carry

        lax.fori_loop(0, min(AHEAD, total), early, 0)

        def body(step, carry):
            @pl.when(step + AHEAD < total)
            def _():
                @pl.when(step + AHEAD >= SLOTS)
                def _():
                    stored(step + AHEAD - SLOTS, lambda copy: copy.wait())

                fetch(step + AHEAD)

            slot = lax.rem(step, SLOTS)
            for q in kinds:

                @pl.when(table_ref[0, step] == q)
                def _():
                    w, m, v, g = buffers[q]
                    for n in range(4):
                        pltpu.make_async_copy(buffers[q][n].at[slot], buffers[q][n].at[slot], sem_in.at[n, slot]).wait()
                    some = 32 if shapes[q][1] > LANES else 224

                    def part(r, carry):
                        at = pl.ds(pl.multiple_of(r * some, some), some)
                        new = adam_math(f, w[slot, at, :], m[slot, at, :], v[slot, at, :], g[slot, at, :])
                        w[slot, at, :], m[slot, at, :], v[slot, at, :] = new
                        return carry

                    lax.fori_loop(0, shapes[q][0] // some, part, 0)

            stored(step, lambda copy: copy.start())
            return carry

        lax.fori_loop(0, total, body, 0)

        def late(step, carry):
            stored(step, lambda copy: copy.wait())
            return carry

        lax.fori_loop(max(0, total - SLOTS), total, late, 0)

    any_ = pl.BlockSpec(memory_space=pl.ANY)
    given = [a for three in arrays for a in three]
    before = [a for three in outs for a in three] if outs is not None else []
    elements = sum(piece[3].size for piece in pieces)
    new = pl.pallas_call(
        kernel,
        in_specs=[pl.BlockSpec(memory_space=pltpu.SMEM), pl.BlockSpec(memory_space=pltpu.VMEM)] + [any_] * (n_in + len(before)),
        out_specs=[any_] * 9,
        out_shape=[jax.ShapeDtypeStruct(a.shape, a.dtype) for a in given],
        scratch_shapes=[pltpu.VMEM((SLOTS, *shapes[q]), t) for q in kinds for t in (BF16, F32, F32, BF16)]
        + [pltpu.SemaphoreType.DMA((4, SLOTS)), pltpu.SemaphoreType.DMA((3, SLOTS))],
        input_output_aliases={2 + n_in + n: n for n in range(len(before))},
        cost_estimate=pl.CostEstimate(flops=2000 * elements, bytes_accessed=22 * elements, transcendentals=elements),
        compiler_params=params(),
    )(table, factor, *given, *(piece[3] for piece in pieces), *before)
    return tuple(tuple(new[3 * n : 3 * n + 3]) for n in range(3))


def solution(mesh):
    def step(x, dy, wg, wu, wd, mg, mu, md, vg, vu, vd):
        x, dy = x[0], dy[0]
        ff = wg.shape[2]
        own = ff // LANES // 4 * LANES

        def send(a, perm):
            return perm(a)

        dy_x = send(dy, px)
        h1, a1, a0 = forward(x, wg, wu, wd)
        a1_x = send(a1, px)
        a0_x = send(a0, px)
        dh1, *kept = chain(own, a1, dy, h1, wg, wu, wd)
        dh1_x = send(dh1, px)
        top = slices(1, own, [a1, a1_x], [dy, dy_x], wg, wu, wd, kept)
        top_x = [send(top[n], px) for n in range(3)]
        top_d = [send(top[n], pd) for n in range(3)]
        low = slices(0, own, [a0, a0_x], [dh1, dh1_x], wg, wu, wd, (), top[6:8], wg.size + wu.size + wd.size)
        low_x = [send(low[n], px) for n in range(3)]
        low_d = [send(low[n], pd) for n in range(3)]

        top_xd = [send(top_x[n], pd) for n in range(3)]
        low_xd = [send(low_x[n], pd) for n in range(2)]
        arrays = ((wg, mg, vg), (wu, mu, vu), (wd, md, vd))

        def pieces(layer, slot, gs, names=(0, 1, 2)):
            return [(n, layer, slot, gs[n]) for n in names]

        first = pieces(1, 0, top) + pieces(1, 1, top_d) + pieces(1, 2, top_x) + pieces(0, 0, low)
        shared = pieces(1, 4, top[3:6]) + pieces(0, 4, low[3:6])
        outs = adam(own, low[6], arrays, first + shared, None)
        outs = adam(own, low[6], arrays, pieces(1, 3, top_xd) + pieces(0, 1, low_d), outs)
        outs, low_x[2] = lax.optimization_barrier((outs, low_x[2]))
        low_xd.append(send(low_x[2], pd))
        outs = adam(own, low[6], arrays, pieces(0, 2, low_x) + pieces(0, 3, low_xd, (0, 1)), outs)
        outs = adam(own, low[6], arrays, pieces(0, 3, low_xd, (2,)), outs)
        return tuple(outs[name][which] for which in range(3) for name in range(3))

    return jax.shard_map(
        step,
        mesh=mesh,
        in_specs=(P(("rep", "dp"), None, None),) * 2 + (P(None, None, None),) * 9,
        out_specs=(P("rep", None, None),) * 9,
        check_vma=False,
    )
```

```python
import jax
import jax.numpy as jnp
import numpy as np
from jax import lax
from jax.experimental import pallas as pl
from jax.experimental.pallas import tpu as pltpu
from jax.sharding import PartitionSpec as P


F32, BF16 = jnp.float32, jnp.bfloat16
PX = ((0, 2), (2, 0), (1, 3), (3, 1))
PD = ((0, 1), (1, 0), (2, 3), (3, 2))
NN, NT = ((1,), (0,)), ((1,), (1,))

LANES = 128
BLOCK = 512
ROWS, FEW, TOGETHER = 512, 64, 4


def dot(a, b, dims):
    return lax.dot_general(a, b, (dims, ((), ())), preferred_element_type=F32)


def sigmoid(x):
    return 0.5 * jnp.tanh(0.5 * x) + 0.5


def px(a):
    return lax.ppermute(a, "dp", PX)


def pd(a):
    return lax.ppermute(a, "dp", PD)


def once(shape, index):
    return pl.BlockSpec(shape, index, pipeline_mode=pl.Buffered(1))


def params(mib=62):
    return pltpu.CompilerParams(vmem_limit_bytes=mib << 20)


def norm_scale(wide):
    return lax.rsqrt(jnp.mean(wide * wide, -1, keepdims=True) + 1e-6)


def normed(h):
    wide = h.astype(F32)
    return (wide * norm_scale(wide)).astype(BF16)


def looped(count, rows, body, together=1):
    def one(n, carry):
        for part in range(together):
            body(pl.ds(pl.multiple_of((n * together + part) * rows, rows), rows))
        return carry

    lax.fori_loop(0, count // together, one, 0)


def written(step, last, half, own, tail, stage_ref, outs, sems, do):
    me = lax.axis_index("dp")
    blocks = own // BLOCK
    extra = own - blocks * BLOCK
    rows = pl.ds(pl.multiple_of(half * 2 * ROWS, 2 * ROWS), 2 * ROWS)
    for n, (out, holder) in enumerate(zip(outs, (me, me // 2 * 2 + 1 - me % 2), strict=True)):

        def copy(here, there):
            do(pltpu.make_async_copy(stage_ref.at[half, :, :, here], out.at[:, rows, there], sems.at[n, half]))

        @pl.when((step < 4 * blocks) & (step // blocks == holder))
        def _():
            copy(pl.ds(0, BLOCK), pl.ds(pl.multiple_of(lax.rem(step, blocks) * BLOCK, BLOCK), BLOCK))

        @pl.when(step == 4 * blocks)
        def _():
            copy(pl.ds(pl.multiple_of(holder * extra, LANES), extra), pl.ds(blocks * BLOCK, extra))

        @pl.when(step == last)
        def _():
            copy(pl.ds(0, tail), pl.ds(own, tail))


def halves(tokens, width, moved, there, back):
    j = pl.program_id(0)

    def two(half, carry):
        @pl.when(j > 0)
        def _():
            moved(j - 1, half, lambda copy: copy.wait())

        low, high = (pl.ds(pl.multiple_of((2 * half + n) * ROWS, ROWS), ROWS) for n in range(2))
        held = there(half, 0, low, width)
        ahead = there(half, 1, high, width)
        back(half, 0, low, width, held)
        back(half, 1, high, width, ahead)
        moved(j, half, lambda copy: copy.start())
        return carry

    lax.fori_loop(0, tokens // (2 * ROWS), two, 0)


def forward_kernel(tail, own, x_ref, wg_ref, wu_ref, wd_ref, h_ref, a_ref, a0_ref, mine_ref, theirs_ref, acc_ref, stage_ref, sems):
    j, last = pl.program_id(0), pl.num_programs(0) - 1
    tokens = x_ref.shape[0]

    def moved(step, half, do):
        written(step, last, half, own, tail, stage_ref, (mine_ref, theirs_ref), sems, do)

    @pl.when(j == 0)
    def _():
        def start(r):
            a0_ref[r, :] = normed(x_ref[r, :])
            acc_ref[r, :] = jnp.zeros((FEW, acc_ref.shape[1]), F32)

        looped(tokens // FEW, FEW, start, TOGETHER)

    def up(half, n, r, width):
        a = a0_ref[r, :]
        g = dot(a, wg_ref[0, :, :width], NN)
        u = dot(a, wu_ref[0, :, :width], NN)
        for k, value in enumerate((g, u)):
            stage_ref[half, k, n * ROWS : (n + 1) * ROWS, :width] = value
        return (g * sigmoid(g) * u).astype(BF16)

    def down(half, n, r, width, hid):
        acc_ref[r, :] += dot(hid, wd_ref[0, :width, :], NN)

    @pl.when(j < last)
    def _():
        halves(tokens, wg_ref.shape[2], moved, up, down)

    @pl.when(j == last)
    def _():
        halves(tokens, tail, moved, up, down)

        def end(r):
            h = (x_ref[r, :].astype(F32) + acc_ref[r, :].astype(BF16).astype(F32)).astype(BF16)
            h_ref[r, :] = h
            a_ref[r, :] = normed(h)

        looped(tokens // FEW, FEW, end, TOGETHER)
        for half in range(tokens // (2 * ROWS)):
            moved(j, half, lambda copy: copy.wait())


def keeping(tokens, count, columns, dtype):
    kept = [jax.ShapeDtypeStruct((count, tokens, columns), dtype)] * 2
    parts = tokens // (2 * ROWS)
    return kept, [pltpu.VMEM((parts, count, 2 * ROWS, BLOCK), dtype), pltpu.SemaphoreType.DMA((2, parts))]


def forward(own, x, wg, wu, wd):
    tokens, d = x.shape
    ff = wg.shape[2]
    steps = pl.cdiv(ff, BLOCK)
    tail = ff - (steps - 1) * BLOCK
    full = once((tokens, d), lambda j: (0, 0))
    across = pl.BlockSpec((1, d, BLOCK), lambda j: (0, 0, j))
    down = pl.BlockSpec((1, BLOCK, d), lambda j: (0, j, 0))
    kept, stage = keeping(tokens, 2, own + tail, F32)
    return pl.pallas_call(
        lambda *refs: forward_kernel(tail, own, *refs),
        grid=(steps,),
        in_specs=[full, across, across, down],
        out_specs=[full] * 3 + [pl.BlockSpec(memory_space=pl.ANY)] * 2,
        out_shape=[jax.ShapeDtypeStruct((tokens, d), BF16)] * 3 + kept,
        scratch_shapes=[pltpu.VMEM((tokens, d), F32)] + stage,
        cost_estimate=pl.CostEstimate(flops=6 * tokens * d * ff, bytes_accessed=6 * d * ff, transcendentals=tokens * ff),
        compiler_params=params(),
        name="forward",
    )(x, wg, wu, wd)


def hidden_back(g, u, dhid):
    dhid = dhid.astype(BF16).astype(F32)
    sig = sigmoid(g)
    act = g * sig
    return (dhid * u * (sig + act * (1 - sig))).astype(BF16), (dhid * act).astype(BF16), (act * u).astype(BF16)


def chain_kernel(tail, own, a_ref, dy_ref, h_ref, wg_ref, wu_ref, wd_ref, dh_ref, mine_ref, theirs_ref, acc_ref, stage_ref, sems):
    j, last = pl.program_id(0), pl.num_programs(0) - 1
    tokens = a_ref.shape[0]

    def moved(step, half, do):
        written(step, last, half, own, tail, stage_ref, (mine_ref, theirs_ref), sems, do)

    @pl.when(j == 0)
    def _():
        def start(r):
            acc_ref[r, :] = jnp.zeros((FEW, acc_ref.shape[1]), F32)

        looped(tokens // FEW, FEW, start, TOGETHER)

    def there(half, n, r, width):
        a, dy = a_ref[r, :], dy_ref[r, :]
        g = dot(a, wg_ref[0, :, :width], NN)
        u = dot(a, wu_ref[0, :, :width], NN)
        for k, value in enumerate(hidden_back(g, u, dot(dy, wd_ref[0, :width, :], NT))):
            stage_ref[half, k, n * ROWS : (n + 1) * ROWS, :width] = value

    def back(half, n, r, width, held):
        dg, du = (stage_ref[half, k, n * ROWS : (n + 1) * ROWS, :width] for k in range(2))
        acc_ref[r, :] += dot(dg, wg_ref[0, :, :width], NT) + dot(du, wu_ref[0, :, :width], NT)

    @pl.when(j < last)
    def _():
        halves(tokens, wg_ref.shape[2], moved, there, back)

    @pl.when(j == last)
    def _():
        halves(tokens, tail, moved, there, back)

        def end(r):
            wide, da = h_ref[r, :].astype(F32), acc_ref[r, :].astype(BF16).astype(F32)
            scale = norm_scale(wide)
            through = scale * da - wide * (scale * scale * scale * jnp.mean(wide * da, -1, keepdims=True))
            dh_ref[r, :] = (dy_ref[r, :].astype(F32) + through.astype(BF16).astype(F32)).astype(BF16)

        looped(tokens // FEW, FEW, end, TOGETHER)
        for half in range(tokens // (2 * ROWS)):
            moved(j, half, lambda copy: copy.wait())


def chain(own, a, dy, h, wg, wu, wd):
    tokens, d = a.shape
    ff = wg.shape[2]
    steps = pl.cdiv(ff, BLOCK)
    tail = ff - (steps - 1) * BLOCK
    full = once((tokens, d), lambda j: (0, 0))
    across = pl.BlockSpec((1, d, BLOCK), lambda j: (1, 0, j))
    down = pl.BlockSpec((1, BLOCK, d), lambda j: (1, j, 0))
    kept, stage = keeping(tokens, 3, own + tail, BF16)
    return pl.pallas_call(
        lambda *refs: chain_kernel(tail, own, *refs),
        grid=(steps,),
        in_specs=[full, full, full, across, across, down],
        out_specs=[full] + [pl.BlockSpec(memory_space=pl.ANY)] * 2,
        out_shape=[jax.ShapeDtypeStruct((tokens, d), BF16)] + kept,
        scratch_shapes=[pltpu.VMEM((tokens, d), F32)] + stage,
        cost_estimate=pl.CostEstimate(flops=10 * tokens * d * ff, bytes_accessed=6 * d * ff, transcendentals=tokens * ff),
        compiler_params=params(),
        name="chain",
    )(a, dy, h, wg, wu, wd)


def slices_kernel(layer, own, kept, count, *refs):
    me = lax.axis_index("dp")
    chip, core = me // 2, me % 2
    partner = chip * 2 + 1 - core
    others = (partner, (1 - chip) * 2 + core, (1 - chip) * 2 + 1 - core)
    final = count is not None

    def take(n):
        nonlocal refs
        taken, refs = refs[:n], refs[n:]
        return taken

    a_own, a_across, dy_own, dy_across, wg_hbm, wu_hbm, wd_hbm = take(7)
    mine, theirs = take(2)
    before = take(2) if final else ()
    outs, (a_land, dy_land, held_land) = take(8), take(3)
    wg_ref, wu_ref, wd_ref, accg_ref, accu_ref, accd_ref, a_buf, dy_buf, sums_ref = take(9)
    sems, w_sems, send_sems, recv_sems = take(4)
    terms, (held_buf,) = take(3), take(1)
    a_refs = (a_own, a_across, a_land.at[0], a_land.at[1])
    dy_refs = (dy_own, dy_across, dy_land.at[0], dy_land.at[1])
    held_refs = (mine, None, held_land, None)
    i, steps = pl.program_id(0), pl.num_programs(0)
    each = a_own.shape[0] // ROWS
    width = wg_ref.shape[1]
    main = own // BLOCK * BLOCK

    def fetch(step, do):
        slot, who = lax.rem(step, 2), step // each
        rows = pl.ds(pl.multiple_of(lax.rem(step, each) * ROWS, ROWS), ROWS)
        for k, (a, dy, held) in enumerate(zip(a_refs, dy_refs, held_refs, strict=True)):

            @pl.when(who == k)
            def _():
                do(pltpu.make_async_copy(a.at[rows, :], a_buf.at[slot], sems.at[0, slot]))
                do(pltpu.make_async_copy(dy.at[rows, :], dy_buf.at[slot], sems.at[1, slot]))
                if held is not None:
                    do(pltpu.make_async_copy(held.at[:, rows, :], held_buf.at[slot], sems.at[2, slot]))

    def weights():
        extra = own - main
        parts = (
            (pl.ds(pl.multiple_of(me * main, LANES), main), pl.ds(0, main)),
            (pl.ds(pl.multiple_of(4 * main + me * extra, LANES), extra), pl.ds(main, extra)),
            (pl.ds(4 * own, width - own), pl.ds(own, width - own)),
        )
        return [
            pltpu.make_async_copy(*((hbm.at[layer, there, :], ref.at[here, :]) if n == 2 else (hbm.at[layer, :, there], ref.at[:, here])), w_sems.at[n, m])
            for n, (hbm, ref) in enumerate(((wg_hbm, wg_ref), (wu_hbm, wu_ref), (wd_hbm, wd_ref)))
            for m, (there, here) in enumerate(parts)
        ]

    def onward(which):
        pairs = [(a_refs[which], a_land.at[which]), (dy_refs[which], dy_land.at[which])]
        if which == 0:
            pairs.append((theirs, held_land))
        return [
            pltpu.make_async_remote_copy(
                src_ref=src,
                dst_ref=dst,
                send_sem=send_sems.at[3 * which + n],
                recv_sem=recv_sems.at[3 * which + n],
                device_id={"dp": partner},
                device_id_type=pl.DeviceIdType.MESH,
            )
            for n, (src, dst) in enumerate(pairs)
        ]

    def told(n):
        return pltpu.make_async_remote_copy(
            src_ref=sums_ref.at[0],
            dst_ref=sums_ref.at[1 + n],
            send_sem=send_sems.at[6 + n],
            recv_sem=recv_sems.at[6 + n],
            device_id={"dp": others[n]},
            device_id_type=pl.DeviceIdType.MESH,
        )

    barrier = pltpu.get_barrier_semaphore()
    spoken = others if final else others[:1]

    @pl.when(i == 0)
    def _():
        for other in spoken:
            pl.semaphore_signal(barrier, inc=1, device_id={"dp": other}, device_id_type=pl.DeviceIdType.MESH)
        fetch(i, lambda copy: copy.start())
        for copy in weights():
            copy.start()
        for copy in weights():
            copy.wait()

    @pl.when(i == 1)
    def _():
        pl.semaphore_wait(barrier, len(spoken))
        for which in range(2):
            for copy in onward(which):
                copy.start()

    for which in range(2):

        @pl.when(i == (2 + which) * each - 1)
        def _():
            for copy in onward(which):
                copy.wait()

    @pl.when(i + 1 < steps)
    def _():
        fetch(i + 1, lambda copy: copy.start())

    slot = lax.rem(i, 2)
    pltpu.make_async_copy(a_own.at[pl.ds(0, ROWS), :], a_buf.at[slot], sems.at[0, slot]).wait()
    pltpu.make_async_copy(dy_own.at[pl.ds(0, ROWS), :], dy_buf.at[slot], sems.at[1, slot]).wait()
    blocks = [pl.ds(c, min(BLOCK, width - c)) for c in range(0, width, BLOCK)]

    def through(there, first):
        a_t, dy_t = a_buf[slot].T, dy_buf[slot].T

        def back(s, held):
            dg, du, hid = held
            for acc, left, right in ((accg_ref, a_t, dg), (accu_ref, a_t, du), (accd_ref, dy_t, hid)):
                acc[:, s] = (jnp.where(i == 0, 0.0, acc[:, s]) if first else acc[:, s]) + dot(left, right, NN)

        held = there(blocks[0])
        for s, following in zip(blocks, blocks[1:] + [None], strict=True):
            ahead = None if following is None else there(following)
            back(s, held)
            held = ahead

    known = lax.rem(i // each, 2) == 0

    @pl.when(known)
    def _():
        pltpu.make_async_copy(mine.at[:, pl.ds(0, ROWS), :], held_buf.at[slot], sems.at[2, slot]).wait()

    if kept == 2:

        @pl.when(jnp.logical_not(known))
        def _():
            for s in blocks:
                held_buf[slot, 0, :, s] = dot(a_buf[slot], wg_ref[:, s], NN)
                held_buf[slot, 1, :, s] = dot(a_buf[slot], wu_ref[:, s], NN)

        through(lambda s: hidden_back(held_buf[slot, 0, :, s], held_buf[slot, 1, :, s], dot(dy_buf[slot], wd_ref[s, :], NT)), True)
    else:

        @pl.when(known)
        def _():
            through(lambda s: [held_buf[slot, n, :, s] for n in range(3)], True)

        @pl.when(jnp.logical_not(known))
        def _():
            a, dy = a_buf[slot], dy_buf[slot]
            through(lambda s: hidden_back(dot(a, wg_ref[:, s], NN), dot(a, wu_ref[:, s], NN), dot(dy, wd_ref[s, :], NT)), False)

    rest = pl.ds(own, width - own)

    @pl.when(lax.rem(i, each) == each - 1)
    def _():
        for acc, term in zip((accg_ref, accu_ref, accd_ref), terms, strict=True):
            term[i // each] = acc[:, rest]
            acc[:, rest] = jnp.zeros_like(acc[:, rest])

    @pl.when(i == steps - 1)
    def _():
        def rounded(part, total):
            part = part.astype(BF16)
            wide = part.astype(F32)
            return part, total + jnp.sum((wide * wide).reshape(-1, 8, LANES), 0)

        accs = (accg_ref, accu_ref, accd_ref)

        def rows(r, total):
            at = pl.ds(pl.multiple_of(r * LANES, LANES), LANES)
            for n, acc in enumerate(accs):
                for c in range(0, own, LANES):
                    part, total = rounded(acc[at, c : c + LANES], total)
                    if n < 2:
                        outs[n][at, c : c + LANES] = part
            return total

        def turn(c, carry):
            at = pl.ds(pl.multiple_of(c * LANES, LANES), LANES)
            for r in range(0, a_buf.shape[2], LANES):
                outs[2][at, r : r + LANES] = accd_ref[r : r + LANES, at].astype(BF16).T
            return carry

        at = [(chip + s // 2) % 2 + 2 * ((core + s) % 2) for s in range(4)]
        place = [(core + s) % 2 + 2 * ((chip + s // 2) % 2) for s in range(4)]
        sums = [lax.fori_loop(0, a_buf.shape[2] // LANES, rows, jnp.zeros((8, LANES), F32)), jnp.zeros((8, LANES), F32)]
        lax.fori_loop(0, own // LANES, turn, 0)
        for n, term in enumerate(terms):
            part, sums[1] = rounded(term[at[0]] + term[at[1]] + term[at[2]] + term[at[3]], sums[1])
            outs[3 + n][...] = part if n < 2 else part.T
        if not final:
            outs[6][...], outs[7][...] = sums
        else:
            sums_ref[0] = sums[0] + before[0][...]
            shared = jnp.sum(sums[1] + before[1][...])
            for n in range(3):
                told(n).start()
            for n in range(3):
                told(n).wait()
            total = sums_ref[place[0]] + sums_ref[place[1]] + sums_ref[place[2]] + sums_ref[place[3]]
            total = jnp.full((8, LANES), jnp.sum(total) + shared, F32)
            outs[6][...] = jnp.minimum(1.0, 0.5 * lax.rsqrt(total / count + 1e-30))
            outs[7][...] = jnp.zeros((8, LANES), F32)


def slices(layer, own, a_all, dy_all, wg, wu, wd, kept, before=(), count=None):
    tokens, d = a_all[0].shape
    ff = wg.shape[2]
    rest = ff - 4 * own
    width = own + rest
    any_ = pl.BlockSpec(memory_space=pl.ANY)
    at = lambda s: once(s, lambda i: (0, 0))
    sizes = [(d, own), (d, own), (own, d), (d, rest), (d, rest), (rest, d)]
    landed = [jax.ShapeDtypeStruct((2, tokens, d), BF16)] * 2 + [kept[0]]
    return pl.pallas_call(
        lambda *refs: slices_kernel(layer, own, kept[0].shape[0], count, *refs),
        grid=(4 * tokens // ROWS,),
        in_specs=[any_] * (7 + len(kept)) + [at((8, LANES))] * len(before),
        out_specs=[at(s) for s in sizes] + [at((8, LANES))] * 2 + [any_] * len(landed),
        scratch_shapes=[pltpu.VMEM((d, width), BF16)] * 2
        + [pltpu.VMEM((width, d), BF16)]
        + [pltpu.VMEM((d, width), F32)] * 3
        + [pltpu.VMEM((2, ROWS, d), BF16)] * 2
        + [pltpu.VMEM((4, 8, LANES), F32)]
        + [pltpu.SemaphoreType.DMA(n) for n in ((3, 2), (3, 3), (9,), (9,))]
        + [pltpu.VMEM((4, d, rest), F32)] * 3
        + [pltpu.VMEM((2, kept[0].shape[0], ROWS, width), kept[0].dtype)],
        out_shape=[jax.ShapeDtypeStruct(s, BF16) for s in sizes]
        + [jax.ShapeDtypeStruct((8, LANES), F32)] * 2
        + [jax.ShapeDtypeStruct(s.shape, s.dtype) for s in landed],
        cost_estimate=pl.CostEstimate(
            flops=12 * 4 * tokens * d * width, bytes_accessed=16 * tokens * d, transcendentals=4 * tokens * width
        ),
        compiler_params=pltpu.CompilerParams(vmem_limit_bytes=62 << 20, collective_id=layer, has_side_effects=True),
        name="slices",
    )(*a_all, *dy_all, wg, wu, wd, *kept, *before)


def adam_math(f, w, m, v, g):
    g = g.astype(F32) * f
    m = 0.9 * m + 0.1 * g
    v = 0.95 * v + 0.05 * g * g
    return (0.998 * w.astype(F32) - 0.02 * (m * lax.rsqrt(v + 1e-8))).astype(BF16), m, v


SLOTS, AHEAD = 8, 4


def adam(own, factor, arrays, pieces, outs):
    d, _ = arrays[0][0].shape[1:]
    main, extra = own // BLOCK * BLOCK, own % BLOCK
    shapes = ((LANES, own), (LANES, d), (d, LANES))
    rows = []
    for n, (which, layer, slot, g) in enumerate(pieces):
        kind = 1 if which == 2 else 2 if slot == 4 else 0
        for r in range(0, g.shape[0], shapes[kind][0]):
            if kind != 1:
                first = (r, 0)
            elif slot == 4:
                first = (4 * own + r, 0)
            else:
                first = (r, main) if r < main else (4 * main + r - main, extra)
            rows.append((kind, which, layer, n, slot, r, *first))
    table = np.array(rows, np.int32).T
    total = len(rows)
    kinds = sorted({row[0] for row in rows})
    n_in = 9 + len(pieces)

    def kernel(table_ref, f_ref, *refs):
        weights, grads = refs[:9], refs[9:n_in]
        refs = refs[n_in + (9 if outs is not None else 0) :]
        results, scratch = refs[:9], refs[9:]
        buffers = {kind: scratch[4 * n : 4 * n + 4] for n, kind in enumerate(kinds)}
        sem_in, sem_out = scratch[-2:]
        f = f_ref[:1, :1]
        me = lax.axis_index("dp")

        def moved(step, do):
            kind, which, layer = (table_ref[n, step] for n in range(3))
            slot = table_ref[4, step]
            unit = (me + slot) % 2 + 2 * ((me // 2 + slot // 2) % 2)
            row = table_ref[6, step] + table_ref[7, step] * unit
            for k in range(3):
                for q in [q for q in kinds if (q == 1) == (k == 2)]:
                    if q == 0:
                        columns = ((unit * main, 0, main), (4 * main + unit * extra, main, extra))
                    else:
                        columns = ((0 if q == 1 else 4 * own, 0, shapes[q][1]),)

                    @pl.when((which == k) & (kind == q))
                    def _():
                        for first, here, size in columns:
                            first = first if isinstance(first, int) else pl.multiple_of(first, LANES)
                            there = (layer, pl.ds(pl.multiple_of(row, LANES), shapes[q][0]), pl.ds(first, size))
                            do(3 * k, there, buffers[q], (lax.rem(step, SLOTS), slice(None), pl.ds(here, size)))

        def fetch(step):
            slot = lax.rem(step, SLOTS)

            def get(k, there, buffer, here):
                for n in range(3):
                    pltpu.make_async_copy(weights[k + n].at[there], buffer[n].at[here], sem_in.at[n, slot]).start()

            moved(step, get)
            piece, row = table_ref[3, step], table_ref[5, step]
            for n, (which_, _, slot_, _) in enumerate(pieces):
                q = 1 if which_ == 2 else 2 if slot_ == 4 else 0

                @pl.when(piece == n)
                def _():
                    rows_ = pl.ds(pl.multiple_of(row, 16), shapes[q][0])
                    pltpu.make_async_copy(grads[n].at[rows_, :], buffers[q][3].at[slot], sem_in.at[3, slot]).start()

        def stored(step, do):
            slot = lax.rem(step, SLOTS)

            def put(k, there, buffer, here):
                for n in range(3):
                    do(pltpu.make_async_copy(buffer[n].at[here], results[k + n].at[there], sem_out.at[n, slot]))

            moved(step, put)

        def early(step, carry):
            fetch(step)
            return carry

        lax.fori_loop(0, min(AHEAD, total), early, 0)

        def body(step, carry):
            @pl.when(step + AHEAD < total)
            def _():
                @pl.when(step + AHEAD >= SLOTS)
                def _():
                    stored(step + AHEAD - SLOTS, lambda copy: copy.wait())

                fetch(step + AHEAD)

            slot = lax.rem(step, SLOTS)
            for q in kinds:

                @pl.when(table_ref[0, step] == q)
                def _():
                    w, m, v, g = buffers[q]
                    for n in range(4):
                        pltpu.make_async_copy(buffers[q][n].at[slot], buffers[q][n].at[slot], sem_in.at[n, slot]).wait()
                    some = 32 if shapes[q][1] > LANES else 224

                    def part(r, carry):
                        at = pl.ds(pl.multiple_of(r * some, some), some)
                        new = adam_math(f, w[slot, at, :], m[slot, at, :], v[slot, at, :], g[slot, at, :])
                        w[slot, at, :], m[slot, at, :], v[slot, at, :] = new
                        return carry

                    lax.fori_loop(0, shapes[q][0] // some, part, 0)

            stored(step, lambda copy: copy.start())
            return carry

        lax.fori_loop(0, total, body, 0)

        def late(step, carry):
            stored(step, lambda copy: copy.wait())
            return carry

        lax.fori_loop(max(0, total - SLOTS), total, late, 0)

    any_ = pl.BlockSpec(memory_space=pl.ANY)
    given = [a for three in arrays for a in three]
    before = [a for three in outs for a in three] if outs is not None else []
    elements = sum(piece[3].size for piece in pieces)
    new = pl.pallas_call(
        kernel,
        in_specs=[pl.BlockSpec(memory_space=pltpu.SMEM), pl.BlockSpec(memory_space=pltpu.VMEM)] + [any_] * (n_in + len(before)),
        out_specs=[any_] * 9,
        out_shape=[jax.ShapeDtypeStruct(a.shape, a.dtype) for a in given],
        scratch_shapes=[pltpu.VMEM((SLOTS, *shapes[q]), t) for q in kinds for t in (BF16, F32, F32, BF16)]
        + [pltpu.SemaphoreType.DMA((4, SLOTS)), pltpu.SemaphoreType.DMA((3, SLOTS))],
        input_output_aliases={2 + n_in + n: n for n in range(len(before))},
        cost_estimate=pl.CostEstimate(flops=2000 * elements, bytes_accessed=22 * elements, transcendentals=elements),
        compiler_params=params(),
    )(table, factor, *given, *(piece[3] for piece in pieces), *before)
    return tuple(tuple(new[3 * n : 3 * n + 3]) for n in range(3))


def solution(mesh):
    def step(x, dy, wg, wu, wd, mg, mu, md, vg, vu, vd):
        x, dy = x[0], dy[0]
        ff = wg.shape[2]
        own = ff // LANES // 4 * LANES

        def send(a, perm):
            return perm(a)

        dy_x = send(dy, px)
        h1, a1, a0, *made = forward(own, x, wg, wu, wd)
        a1_x = send(a1, px)
        a0_x = send(a0, px)
        dh1, *kept = chain(own, a1, dy, h1, wg, wu, wd)
        dh1_x = send(dh1, px)
        top = slices(1, own, [a1, a1_x], [dy, dy_x], wg, wu, wd, kept)
        top_x = [send(top[n], px) for n in range(3)]
        top_d = [send(top[n], pd) for n in range(3)]
        low = slices(0, own, [a0, a0_x], [dh1, dh1_x], wg, wu, wd, made, top[6:8], wg.size + wu.size + wd.size)
        low_x = [send(low[n], px) for n in range(3)]
        low_d = [send(low[n], pd) for n in range(3)]

        top_xd = [send(top_x[n], pd) for n in range(3)]
        low_xd = [send(low_x[n], pd) for n in range(2)]
        arrays = ((wg, mg, vg), (wu, mu, vu), (wd, md, vd))

        def pieces(layer, slot, gs, names=(0, 1, 2)):
            return [(n, layer, slot, gs[n]) for n in names]

        first = pieces(1, 0, top) + pieces(1, 1, top_d) + pieces(1, 2, top_x) + pieces(0, 0, low)
        shared = pieces(1, 4, top[3:6]) + pieces(0, 4, low[3:6])
        outs = adam(own, low[6], arrays, first + shared, None)
        outs = adam(own, low[6], arrays, pieces(1, 3, top_xd) + pieces(0, 1, low_d), outs)
        outs, low_x[2] = lax.optimization_barrier((outs, low_x[2]))
        low_xd.append(send(low_x[2], pd))
        outs = adam(own, low[6], arrays, pieces(0, 2, low_x) + pieces(0, 3, low_xd, (0, 1)), outs)
        outs = adam(own, low[6], arrays, pieces(0, 3, low_xd, (2,)), outs)
        return tuple(outs[name][which] for which in range(3) for name in range(3))

    return jax.shard_map(
        step,
        mesh=mesh,
        in_specs=(P(("rep", "dp"), None, None),) * 2 + (P(None, None, None),) * 9,
        out_specs=(P("rep", None, None),) * 9,
        check_vma=False,
    )
```

```python
import jax
import jax.numpy as jnp
import numpy as np
from jax import lax
from jax.experimental import pallas as pl
from jax.experimental.pallas import tpu as pltpu
from jax.sharding import PartitionSpec as P


F32, BF16 = jnp.float32, jnp.bfloat16
PX = ((0, 2), (2, 0), (1, 3), (3, 1))
PD = ((0, 1), (1, 0), (2, 3), (3, 2))
NN, NT = ((1,), (0,)), ((1,), (1,))

LANES = 128
BLOCK = 512
ROWS, FEW, TOGETHER = 512, 64, 4


def dot(a, b, dims):
    return lax.dot_general(a, b, (dims, ((), ())), preferred_element_type=F32)


def sigmoid(x):
    return 0.5 * jnp.tanh(0.5 * x) + 0.5


def px(a):
    return lax.ppermute(a, "dp", PX)


def pd(a):
    return lax.ppermute(a, "dp", PD)


def once(shape, index):
    return pl.BlockSpec(shape, index, pipeline_mode=pl.Buffered(1))


def params(mib=62):
    return pltpu.CompilerParams(vmem_limit_bytes=mib << 20)


def norm_scale(wide):
    return lax.rsqrt(jnp.mean(wide * wide, -1, keepdims=True) + 1e-6)


def normed(h):
    wide = h.astype(F32)
    return (wide * norm_scale(wide)).astype(BF16)


def looped(count, rows, body, together=1, after=None):
    def one(n, carry):
        for part in range(together):
            body(pl.ds(pl.multiple_of((n * together + part) * rows, rows), rows))
        if after is not None:
            after(pl.ds(pl.multiple_of(n * together * rows, together * rows), together * rows))
        return carry

    lax.fori_loop(0, count // together, one, 0)


def written(step, last, half, own, tail, stage_ref, outs, sems, do):
    me = lax.axis_index("dp")
    blocks = own // BLOCK
    extra = own - blocks * BLOCK
    rows = pl.ds(pl.multiple_of(half * 2 * ROWS, 2 * ROWS), 2 * ROWS)
    for n, (out, holder) in enumerate(zip(outs, (me, me // 2 * 2 + 1 - me % 2), strict=True)):

        def copy(here, there):
            do(pltpu.make_async_copy(stage_ref.at[half, :, :, here], out.at[:, rows, there], sems.at[n, half]))

        @pl.when((step < 4 * blocks) & (step // blocks == holder))
        def _():
            copy(pl.ds(0, BLOCK), pl.ds(pl.multiple_of(lax.rem(step, blocks) * BLOCK, BLOCK), BLOCK))

        @pl.when(step == 4 * blocks)
        def _():
            copy(pl.ds(pl.multiple_of(holder * extra, LANES), extra), pl.ds(blocks * BLOCK, extra))

        @pl.when(step == last)
        def _():
            copy(pl.ds(0, tail), pl.ds(own, tail))


def halves(tokens, width, moved, there, back):
    j = pl.program_id(0)

    def two(half, carry):
        @pl.when(j > 0)
        def _():
            moved(j - 1, half, lambda copy: copy.wait())

        low, high = (pl.ds(pl.multiple_of((2 * half + n) * ROWS, ROWS), ROWS) for n in range(2))
        held = there(half, 0, low, width)
        ahead = there(half, 1, high, width)
        back(half, 0, low, width, held)
        back(half, 1, high, width, ahead)
        moved(j, half, lambda copy: copy.start())
        return carry

    lax.fori_loop(0, tokens // (2 * ROWS), two, 0)


def forward_kernel(tail, own, x_ref, wg_ref, wu_ref, wd_ref, *refs):
    h_out, a_out, a0_out, mine_ref, theirs_ref, acc_ref, stage_ref, sems, h_ref, a_ref, a0_ref, out_sems = refs
    j, last = pl.program_id(0), pl.num_programs(0) - 1
    tokens = x_ref.shape[0]

    def moved(step, half, do):
        written(step, last, half, own, tail, stage_ref, (mine_ref, theirs_ref), sems, do)

    @pl.when(j == 0)
    def _():
        def start(r):
            a0_ref[r, :] = normed(x_ref[r, :])
            acc_ref[r, :] = jnp.zeros((FEW, acc_ref.shape[1]), F32)

        looped(tokens // FEW, FEW, start, TOGETHER)

    early = pltpu.make_async_copy(a0_ref, a0_out, out_sems.at[2])

    @pl.when(j == 1)
    def _():
        early.start()

    def up(half, n, r, width):
        a = a0_ref[r, :]
        g = dot(a, wg_ref[0, :, :width], NN)
        u = dot(a, wu_ref[0, :, :width], NN)
        for k, value in enumerate((g, u)):
            stage_ref[half, k, n * ROWS : (n + 1) * ROWS, :width] = value
        return (g * sigmoid(g) * u).astype(BF16)

    def down(half, n, r, width, hid):
        acc_ref[r, :] += dot(hid, wd_ref[0, :width, :], NN)

    @pl.when(j < last)
    def _():
        halves(tokens, wg_ref.shape[2], moved, up, down)

    @pl.when(j == last)
    def _():
        halves(tokens, tail, moved, up, down)

        def end(r):
            h = (x_ref[r, :].astype(F32) + acc_ref[r, :].astype(BF16).astype(F32)).astype(BF16)
            h_ref[r, :] = h
            a_ref[r, :] = normed(h)

        def leave(n, r):
            return pltpu.make_async_copy((a_ref, h_ref)[n].at[r, :], (a_out, h_out)[n].at[r, :], out_sems.at[n])

        looped(tokens // FEW, FEW, end, TOGETHER, lambda r: [leave(n, r).start() for n in range(2)])
        for n in range(2):
            leave(n, pl.ds(0, tokens)).wait()
        early.wait()
        for half in range(tokens // (2 * ROWS)):
            moved(j, half, lambda copy: copy.wait())


def keeping(tokens, count, columns, dtype):
    kept = [jax.ShapeDtypeStruct((count, tokens, columns), dtype)] * 2
    parts = tokens // (2 * ROWS)
    return kept, [pltpu.VMEM((parts, count, 2 * ROWS, BLOCK), dtype), pltpu.SemaphoreType.DMA((2, parts))]


def forward(own, x, wg, wu, wd):
    tokens, d = x.shape
    ff = wg.shape[2]
    steps = pl.cdiv(ff, BLOCK)
    tail = ff - (steps - 1) * BLOCK
    full = once((tokens, d), lambda j: (0, 0))
    across = pl.BlockSpec((1, d, BLOCK), lambda j: (0, 0, j))
    down = pl.BlockSpec((1, BLOCK, d), lambda j: (0, j, 0))
    kept, stage = keeping(tokens, 2, own + tail, F32)
    return pl.pallas_call(
        lambda *refs: forward_kernel(tail, own, *refs),
        grid=(steps,),
        in_specs=[full, across, across, down],
        out_specs=[pl.BlockSpec(memory_space=pl.ANY)] * 5,
        out_shape=[jax.ShapeDtypeStruct((tokens, d), BF16)] * 3 + kept,
        scratch_shapes=[pltpu.VMEM((tokens, d), F32)] + stage + [pltpu.VMEM((tokens, d), BF16)] * 3 + [pltpu.SemaphoreType.DMA((3,))],
        cost_estimate=pl.CostEstimate(flops=6 * tokens * d * ff, bytes_accessed=6 * d * ff, transcendentals=tokens * ff),
        compiler_params=params(),
        name="forward",
    )(x, wg, wu, wd)


def hidden_back(g, u, dhid):
    dhid = dhid.astype(BF16).astype(F32)
    sig = sigmoid(g)
    act = g * sig
    return (dhid * u * (sig + act * (1 - sig))).astype(BF16), (dhid * act).astype(BF16), (act * u).astype(BF16)


def chain_kernel(tail, own, a_ref, dy_ref, h_in, wg_ref, wu_ref, wd_ref, dh_out, mine_ref, theirs_ref, *scratch):
    acc_ref, stage_ref, sems, h_ref, dh_ref, out_sems = scratch
    j, last = pl.program_id(0), pl.num_programs(0) - 1
    tokens = a_ref.shape[0]

    def moved(step, half, do):
        written(step, last, half, own, tail, stage_ref, (mine_ref, theirs_ref), sems, do)

    late = pltpu.make_async_copy(h_in, h_ref, out_sems.at[0])

    @pl.when(j == 0)
    def _():
        def start(r):
            acc_ref[r, :] = jnp.zeros((FEW, acc_ref.shape[1]), F32)

        looped(tokens // FEW, FEW, start, TOGETHER)
        late.start()

    def there(half, n, r, width):
        a, dy = a_ref[r, :], dy_ref[r, :]
        g = dot(a, wg_ref[0, :, :width], NN)
        u = dot(a, wu_ref[0, :, :width], NN)
        for k, value in enumerate(hidden_back(g, u, dot(dy, wd_ref[0, :width, :], NT))):
            stage_ref[half, k, n * ROWS : (n + 1) * ROWS, :width] = value

    def back(half, n, r, width, held):
        dg, du = (stage_ref[half, k, n * ROWS : (n + 1) * ROWS, :width] for k in range(2))
        acc_ref[r, :] += dot(dg, wg_ref[0, :, :width], NT) + dot(du, wu_ref[0, :, :width], NT)

    @pl.when(j < last)
    def _():
        halves(tokens, wg_ref.shape[2], moved, there, back)

    @pl.when(j == last)
    def _():
        halves(tokens, tail, moved, there, back)
        late.wait()

        def end(r):
            wide, da = h_ref[r, :].astype(F32), acc_ref[r, :].astype(BF16).astype(F32)
            scale = norm_scale(wide)
            through = scale * da - wide * (scale * scale * scale * jnp.mean(wide * da, -1, keepdims=True))
            dh_ref[r, :] = (dy_ref[r, :].astype(F32) + through.astype(BF16).astype(F32)).astype(BF16)

        def leave(r):
            return pltpu.make_async_copy(dh_ref.at[r, :], dh_out.at[r, :], out_sems.at[1])

        looped(tokens // FEW, FEW, end, TOGETHER, lambda r: leave(r).start())
        leave(pl.ds(0, tokens)).wait()
        for half in range(tokens // (2 * ROWS)):
            moved(j, half, lambda copy: copy.wait())


def chain(own, a, dy, h, wg, wu, wd):
    tokens, d = a.shape
    ff = wg.shape[2]
    steps = pl.cdiv(ff, BLOCK)
    tail = ff - (steps - 1) * BLOCK
    full = once((tokens, d), lambda j: (0, 0))
    across = pl.BlockSpec((1, d, BLOCK), lambda j: (1, 0, j))
    down = pl.BlockSpec((1, BLOCK, d), lambda j: (1, j, 0))
    kept, stage = keeping(tokens, 3, own + tail, BF16)
    return pl.pallas_call(
        lambda *refs: chain_kernel(tail, own, *refs),
        grid=(steps,),
        in_specs=[full, full, pl.BlockSpec(memory_space=pl.ANY), across, across, down],
        out_specs=[pl.BlockSpec(memory_space=pl.ANY)] * 3,
        out_shape=[jax.ShapeDtypeStruct((tokens, d), BF16)] + kept,
        scratch_shapes=[pltpu.VMEM((tokens, d), F32)] + stage + [pltpu.VMEM((tokens, d), BF16)] * 2 + [pltpu.SemaphoreType.DMA((2,))],
        cost_estimate=pl.CostEstimate(flops=10 * tokens * d * ff, bytes_accessed=6 * d * ff, transcendentals=tokens * ff),
        compiler_params=params(),
        name="chain",
    )(a, dy, h, wg, wu, wd)


def slices_kernel(layer, own, kept, count, *refs):
    me = lax.axis_index("dp")
    chip, core = me // 2, me % 2
    partner = chip * 2 + 1 - core
    others = (partner, (1 - chip) * 2 + core, (1 - chip) * 2 + 1 - core)
    final = count is not None

    def take(n):
        nonlocal refs
        taken, refs = refs[:n], refs[n:]
        return taken

    a_own, a_across, dy_own, dy_across, wg_hbm, wu_hbm, wd_hbm = take(7)
    mine, theirs = take(2)
    before = take(2) if final else ()
    outs, (a_land, dy_land, held_land) = take(8), take(3)
    wg_ref, wu_ref, wd_ref, accg_ref, accu_ref, accd_ref, a_buf, dy_buf, sums_ref = take(9)
    sems, w_sems, send_sems, recv_sems = take(4)
    terms, (held_buf,), results = take(3), take(1), take(3)
    a_refs = (a_own, a_across, a_land.at[1], a_land.at[0])
    dy_refs = (dy_own, dy_across, dy_land.at[1], dy_land.at[0])
    held_refs = (mine, None, None, held_land)
    i, steps = pl.program_id(0), pl.num_programs(0)
    each = a_own.shape[0] // ROWS
    width = wg_ref.shape[1]
    main = own // BLOCK * BLOCK

    def fetch(step, do):
        slot, who = lax.rem(step, 2), step // each
        rows = pl.ds(pl.multiple_of(lax.rem(step, each) * ROWS, ROWS), ROWS)
        for k, (a, dy, held) in enumerate(zip(a_refs, dy_refs, held_refs, strict=True)):

            @pl.when(who == k)
            def _():
                do(pltpu.make_async_copy(a.at[rows, :], a_buf.at[slot], sems.at[0, slot]))
                do(pltpu.make_async_copy(dy.at[rows, :], dy_buf.at[slot], sems.at[1, slot]))
                if held is not None:
                    do(pltpu.make_async_copy(held.at[:, rows, :], held_buf.at[slot], sems.at[2, slot]))

    def weights():
        extra = own - main
        parts = (
            (pl.ds(pl.multiple_of(me * main, LANES), main), pl.ds(0, main)),
            (pl.ds(pl.multiple_of(4 * main + me * extra, LANES), extra), pl.ds(main, extra)),
            (pl.ds(4 * own, width - own), pl.ds(own, width - own)),
        )
        return [
            pltpu.make_async_copy(*((hbm.at[layer, there, :], ref.at[here, :]) if n == 2 else (hbm.at[layer, :, there], ref.at[:, here])), w_sems.at[n, m])
            for n, (hbm, ref) in enumerate(((wg_hbm, wg_ref), (wu_hbm, wu_ref), (wd_hbm, wd_ref)))
            for m, (there, here) in enumerate(parts)
        ]

    def onward(which):
        pairs = [(a_refs[which], a_land.at[which]), (dy_refs[which], dy_land.at[which])]
        if which == 0:
            pairs.append((theirs, held_land))
        return [
            pltpu.make_async_remote_copy(
                src_ref=src,
                dst_ref=dst,
                send_sem=send_sems.at[3 * which + n],
                recv_sem=recv_sems.at[3 * which + n],
                device_id={"dp": partner},
                device_id_type=pl.DeviceIdType.MESH,
            )
            for n, (src, dst) in enumerate(pairs)
        ]

    def told(n):
        return pltpu.make_async_remote_copy(
            src_ref=sums_ref.at[0],
            dst_ref=sums_ref.at[1 + n],
            send_sem=send_sems.at[6 + n],
            recv_sem=recv_sems.at[6 + n],
            device_id={"dp": others[n]},
            device_id_type=pl.DeviceIdType.MESH,
        )

    barrier = pltpu.get_barrier_semaphore()
    spoken = others if final else others[:1]

    @pl.when(i == 0)
    def _():
        for other in spoken:
            pl.semaphore_signal(barrier, inc=1, device_id={"dp": other}, device_id_type=pl.DeviceIdType.MESH)
        fetch(i, lambda copy: copy.start())
        for copy in weights():
            copy.start()
        for copy in weights():
            copy.wait()

    @pl.when(i == 1)
    def _():
        pl.semaphore_wait(barrier, len(spoken))
        for which in (1, 0):
            for copy in onward(which):
                copy.start()

    for which in range(2):

        @pl.when(i == (3 - which) * each - 1)
        def _():
            for copy in onward(which):
                copy.wait()

    @pl.when(i + 1 < steps)
    def _():
        fetch(i + 1, lambda copy: copy.start())

    slot = lax.rem(i, 2)
    pltpu.make_async_copy(a_own.at[pl.ds(0, ROWS), :], a_buf.at[slot], sems.at[0, slot]).wait()
    pltpu.make_async_copy(dy_own.at[pl.ds(0, ROWS), :], dy_buf.at[slot], sems.at[1, slot]).wait()
    blocks = [pl.ds(c, min(BLOCK, width - c)) for c in range(0, width, BLOCK)]

    def through(there, first):
        a_t, dy_t = a_buf[slot].T, dy_buf[slot].T

        def back(s, held):
            dg, du, hid = held
            for acc, left, right in ((accg_ref, a_t, dg), (accu_ref, a_t, du), (accd_ref, dy_t, hid)):
                acc[:, s] = (jnp.where(i == 0, 0.0, acc[:, s]) if first else acc[:, s]) + dot(left, right, NN)

        held = there(blocks[0])
        for s, following in zip(blocks, blocks[1:] + [None], strict=True):
            ahead = None if following is None else there(following)
            back(s, held)
            held = ahead

    known = (i // each == 0) | (i // each == 3)

    @pl.when(known)
    def _():
        pltpu.make_async_copy(mine.at[:, pl.ds(0, ROWS), :], held_buf.at[slot], sems.at[2, slot]).wait()

    if kept == 2:

        @pl.when(jnp.logical_not(known))
        def _():
            for s in blocks:
                held_buf[slot, 0, :, s] = dot(a_buf[slot], wg_ref[:, s], NN)
                held_buf[slot, 1, :, s] = dot(a_buf[slot], wu_ref[:, s], NN)

        through(lambda s: hidden_back(held_buf[slot, 0, :, s], held_buf[slot, 1, :, s], dot(dy_buf[slot], wd_ref[s, :], NT)), True)
    else:

        @pl.when(known)
        def _():
            through(lambda s: [held_buf[slot, n, :, s] for n in range(3)], True)

        @pl.when(jnp.logical_not(known))
        def _():
            a, dy = a_buf[slot], dy_buf[slot]
            through(lambda s: hidden_back(dot(a, wg_ref[:, s], NN), dot(a, wu_ref[:, s], NN), dot(dy, wd_ref[s, :], NT)), False)

    rest = pl.ds(own, width - own)

    @pl.when(lax.rem(i, each) == each - 1)
    def _():
        for acc, term in zip((accg_ref, accu_ref, accd_ref), terms, strict=True):
            term[i // each] = acc[:, rest]
            acc[:, rest] = jnp.zeros_like(acc[:, rest])

    @pl.when(i == steps - 1)
    def _():
        def rounded(part, total):
            part = part.astype(BF16)
            wide = part.astype(F32)
            return part, total + jnp.sum((wide * wide).reshape(-1, 8, LANES), 0)

        accs = (accg_ref, accu_ref, accd_ref)

        def leave(n, at):
            return pltpu.make_async_copy(results[n].at[at, :], outs[n].at[at, :], w_sems.at[n, 0])

        def rows(r, total):
            at = pl.ds(pl.multiple_of(r * LANES, LANES), LANES)
            for n, acc in enumerate(accs):
                for c in range(0, own, LANES):
                    part, total = rounded(acc[at, c : c + LANES], total)
                    if n < 2:
                        results[n][at, c : c + LANES] = part
            for n in range(2):
                leave(n, at).start()
            return total

        def turn(c, carry):
            at = pl.ds(pl.multiple_of(c * LANES, LANES), LANES)
            for r in range(0, a_buf.shape[2], LANES):
                results[2][at, r : r + LANES] = accd_ref[r : r + LANES, at].astype(BF16).T
            leave(2, at).start()
            return carry

        at = [3 * ((core + s) % 2) + (chip + s // 2) % 2 * (1 - 2 * ((core + s) % 2)) for s in range(4)]
        place = [(core + s) % 2 + 2 * ((chip + s // 2) % 2) for s in range(4)]
        sums = [lax.fori_loop(0, a_buf.shape[2] // LANES, rows, jnp.zeros((8, LANES), F32)), jnp.zeros((8, LANES), F32)]
        lax.fori_loop(0, own // LANES, turn, 0)
        for n, term in enumerate(terms):
            part, sums[1] = rounded(term[at[0]] + term[at[1]] + term[at[2]] + term[at[3]], sums[1])
            outs[3 + n][...] = part if n < 2 else part.T
        for n, result in enumerate(results):
            leave(n, pl.ds(0, result.shape[0])).wait()
        if not final:
            outs[6][...], outs[7][...] = sums
        else:
            sums_ref[0] = sums[0] + before[0][...]
            shared = jnp.sum(sums[1] + before[1][...])
            for n in range(3):
                told(n).start()
            for n in range(3):
                told(n).wait()
            total = sums_ref[place[0]] + sums_ref[place[1]] + sums_ref[place[2]] + sums_ref[place[3]]
            total = jnp.full((8, LANES), jnp.sum(total) + shared, F32)
            outs[6][...] = jnp.minimum(1.0, 0.5 * lax.rsqrt(total / count + 1e-30))
            outs[7][...] = jnp.zeros((8, LANES), F32)


def slices(layer, own, a_all, dy_all, wg, wu, wd, kept, before=(), count=None):
    tokens, d = a_all[0].shape
    ff = wg.shape[2]
    rest = ff - 4 * own
    width = own + rest
    any_ = pl.BlockSpec(memory_space=pl.ANY)
    at = lambda s: once(s, lambda i: (0, 0))
    sizes = [(d, own), (d, own), (own, d), (d, rest), (d, rest), (rest, d)]
    landed = [jax.ShapeDtypeStruct((2, tokens, d), BF16)] * 2 + [kept[0]]
    return pl.pallas_call(
        lambda *refs: slices_kernel(layer, own, kept[0].shape[0], count, *refs),
        grid=(4 * tokens // ROWS,),
        in_specs=[any_] * (7 + len(kept)) + [at((8, LANES))] * len(before),
        out_specs=[any_] * 3 + [at(s) for s in sizes[3:]] + [at((8, LANES))] * 2 + [any_] * len(landed),
        scratch_shapes=[pltpu.VMEM((d, width), BF16)] * 2
        + [pltpu.VMEM((width, d), BF16)]
        + [pltpu.VMEM((d, width), F32)] * 3
        + [pltpu.VMEM((2, ROWS, d), BF16)] * 2
        + [pltpu.VMEM((4, 8, LANES), F32)]
        + [pltpu.SemaphoreType.DMA(n) for n in ((3, 2), (3, 3), (9,), (9,))]
        + [pltpu.VMEM((4, d, rest), F32)] * 3
        + [pltpu.VMEM((2, kept[0].shape[0], ROWS, width), kept[0].dtype)]
        + [pltpu.VMEM(s, BF16) for s in sizes[:3]],
        out_shape=[jax.ShapeDtypeStruct(s, BF16) for s in sizes]
        + [jax.ShapeDtypeStruct((8, LANES), F32)] * 2
        + [jax.ShapeDtypeStruct(s.shape, s.dtype) for s in landed],
        cost_estimate=pl.CostEstimate(
            flops=12 * 4 * tokens * d * width, bytes_accessed=16 * tokens * d, transcendentals=4 * tokens * width
        ),
        compiler_params=pltpu.CompilerParams(vmem_limit_bytes=62 << 20, collective_id=layer, has_side_effects=True),
        name="slices",
    )(*a_all, *dy_all, wg, wu, wd, *kept, *before)


def adam_math(f, w, m, v, g):
    g = g.astype(F32) * f
    m = 0.9 * m + 0.1 * g
    v = 0.95 * v + 0.05 * g * g
    return (0.998 * w.astype(F32) - 0.02 * (m * lax.rsqrt(v + 1e-8))).astype(BF16), m, v


SLOTS, AHEAD = 8, 4


def adam(own, factor, arrays, pieces, outs):
    d, _ = arrays[0][0].shape[1:]
    main, extra = own // BLOCK * BLOCK, own % BLOCK
    shapes = ((LANES, own), (LANES, d), (d, LANES))
    rows = []
    for n, (which, layer, slot, g) in enumerate(pieces):
        kind = 1 if which == 2 else 2 if slot == 4 else 0
        for r in range(0, g.shape[0], shapes[kind][0]):
            if kind != 1:
                first = (r, 0)
            elif slot == 4:
                first = (4 * own + r, 0)
            else:
                first = (r, main) if r < main else (4 * main + r - main, extra)
            rows.append((kind, which, layer, n, slot, r, *first))
    table = np.array(rows, np.int32).T
    total = len(rows)
    kinds = sorted({row[0] for row in rows})
    n_in = 9 + len(pieces)

    def kernel(table_ref, f_ref, *refs):
        weights, grads = refs[:9], refs[9:n_in]
        refs = refs[n_in + (9 if outs is not None else 0) :]
        results, scratch = refs[:9], refs[9:]
        buffers = {kind: scratch[4 * n : 4 * n + 4] for n, kind in enumerate(kinds)}
        sem_in, sem_out = scratch[-2:]
        f = f_ref[:1, :1]
        me = lax.axis_index("dp")

        def moved(step, do):
            kind, which, layer = (table_ref[n, step] for n in range(3))
            slot = table_ref[4, step]
            unit = (me + slot) % 2 + 2 * ((me // 2 + slot // 2) % 2)
            row = table_ref[6, step] + table_ref[7, step] * unit
            for k in range(3):
                for q in [q for q in kinds if (q == 1) == (k == 2)]:
                    if q == 0:
                        columns = ((unit * main, 0, main), (4 * main + unit * extra, main, extra))
                    else:
                        columns = ((0 if q == 1 else 4 * own, 0, shapes[q][1]),)

                    @pl.when((which == k) & (kind == q))
                    def _():
                        for first, here, size in columns:
                            first = first if isinstance(first, int) else pl.multiple_of(first, LANES)
                            there = (layer, pl.ds(pl.multiple_of(row, LANES), shapes[q][0]), pl.ds(first, size))
                            do(3 * k, there, buffers[q], (lax.rem(step, SLOTS), slice(None), pl.ds(here, size)))

        def fetch(step):
            slot = lax.rem(step, SLOTS)

            def get(k, there, buffer, here):
                for n in range(3):
                    pltpu.make_async_copy(weights[k + n].at[there], buffer[n].at[here], sem_in.at[n, slot]).start()

            moved(step, get)
            piece, row = table_ref[3, step], table_ref[5, step]
            for n, (which_, _, slot_, _) in enumerate(pieces):
                q = 1 if which_ == 2 else 2 if slot_ == 4 else 0

                @pl.when(piece == n)
                def _():
                    rows_ = pl.ds(pl.multiple_of(row, 16), shapes[q][0])
                    pltpu.make_async_copy(grads[n].at[rows_, :], buffers[q][3].at[slot], sem_in.at[3, slot]).start()

        def stored(step, do):
            slot = lax.rem(step, SLOTS)

            def put(k, there, buffer, here):
                for n in range(3):
                    do(pltpu.make_async_copy(buffer[n].at[here], results[k + n].at[there], sem_out.at[n, slot]))

            moved(step, put)

        def early(step, carry):
            fetch(step)
            return carry

        lax.fori_loop(0, min(AHEAD, total), early, 0)

        def body(step, carry):
            @pl.when(step + AHEAD < total)
            def _():
                @pl.when(step + AHEAD >= SLOTS)
                def _():
                    stored(step + AHEAD - SLOTS, lambda copy: copy.wait())

                fetch(step + AHEAD)

            slot = lax.rem(step, SLOTS)
            for q in kinds:

                @pl.when(table_ref[0, step] == q)
                def _():
                    w, m, v, g = buffers[q]
                    for n in range(4):
                        pltpu.make_async_copy(buffers[q][n].at[slot], buffers[q][n].at[slot], sem_in.at[n, slot]).wait()
                    some = 32 if shapes[q][1] > LANES else 224

                    def part(r, carry):
                        at = pl.ds(pl.multiple_of(r * some, some), some)
                        new = adam_math(f, w[slot, at, :], m[slot, at, :], v[slot, at, :], g[slot, at, :])
                        w[slot, at, :], m[slot, at, :], v[slot, at, :] = new
                        return carry

                    lax.fori_loop(0, shapes[q][0] // some, part, 0)

            stored(step, lambda copy: copy.start())
            return carry

        lax.fori_loop(0, total, body, 0)

        def late(step, carry):
            stored(step, lambda copy: copy.wait())
            return carry

        lax.fori_loop(max(0, total - SLOTS), total, late, 0)

    any_ = pl.BlockSpec(memory_space=pl.ANY)
    given = [a for three in arrays for a in three]
    before = [a for three in outs for a in three] if outs is not None else []
    elements = sum(piece[3].size for piece in pieces)
    new = pl.pallas_call(
        kernel,
        in_specs=[pl.BlockSpec(memory_space=pltpu.SMEM), pl.BlockSpec(memory_space=pltpu.VMEM)] + [any_] * (n_in + len(before)),
        out_specs=[any_] * 9,
        out_shape=[jax.ShapeDtypeStruct(a.shape, a.dtype) for a in given],
        scratch_shapes=[pltpu.VMEM((SLOTS, *shapes[q]), t) for q in kinds for t in (BF16, F32, F32, BF16)]
        + [pltpu.SemaphoreType.DMA((4, SLOTS)), pltpu.SemaphoreType.DMA((3, SLOTS))],
        input_output_aliases={2 + n_in + n: n for n in range(len(before))},
        cost_estimate=pl.CostEstimate(flops=2000 * elements, bytes_accessed=22 * elements, transcendentals=elements),
        compiler_params=params(),
    )(table, factor, *given, *(piece[3] for piece in pieces), *before)
    return tuple(tuple(new[3 * n : 3 * n + 3]) for n in range(3))


def solution(mesh):
    def step(x, dy, wg, wu, wd, mg, mu, md, vg, vu, vd):
        x, dy = x[0], dy[0]
        ff = wg.shape[2]
        own = ff // LANES // 4 * LANES

        def send(a, perm):
            return perm(a)

        dy_x = send(dy, px)
        h1, a1, a0, *made = forward(own, x, wg, wu, wd)
        a1_x = send(a1, px)
        a0_x = send(a0, px)
        dh1, *kept = chain(own, a1, dy, h1, wg, wu, wd)
        dh1_x = send(dh1, px)
        top = slices(1, own, [a1, a1_x], [dy, dy_x], wg, wu, wd, kept)
        top_x = [send(top[n], px) for n in range(3)]
        top_d = [send(top[n], pd) for n in range(3)]
        low = slices(0, own, [a0, a0_x], [dh1, dh1_x], wg, wu, wd, made, top[6:8], wg.size + wu.size + wd.size)
        low_x = [send(low[n], px) for n in range(3)]
        low_d = [send(low[n], pd) for n in range(3)]

        top_xd = [send(top_x[n], pd) for n in range(3)]
        low_xd = [send(low_x[n], pd) for n in range(2)]
        arrays = ((wg, mg, vg), (wu, mu, vu), (wd, md, vd))

        def pieces(layer, slot, gs, names=(0, 1, 2)):
            return [(n, layer, slot, gs[n]) for n in names]

        first = pieces(1, 0, top) + pieces(1, 1, top_d) + pieces(1, 2, top_x) + pieces(0, 0, low)
        shared = pieces(1, 4, top[3:6]) + pieces(0, 4, low[3:6])
        outs = adam(own, low[6], arrays, first + shared, None)
        outs = adam(own, low[6], arrays, pieces(1, 3, top_xd) + pieces(0, 1, low_d), outs)
        outs, low_x[2] = lax.optimization_barrier((outs, low_x[2]))
        low_xd.append(send(low_x[2], pd))
        outs = adam(own, low[6], arrays, pieces(0, 2, low_x) + pieces(0, 3, low_xd, (0, 1)), outs)
        outs = adam(own, low[6], arrays, pieces(0, 3, low_xd, (2,)), outs)
        return tuple(outs[name][which] for which in range(3) for name in range(3))

    return jax.shard_map(
        step,
        mesh=mesh,
        in_specs=(P(("rep", "dp"), None, None),) * 2 + (P(None, None, None),) * 9,
        out_specs=(P("rep", None, None),) * 9,
        check_vma=False,
    )
```

```python
import jax
import jax.numpy as jnp
import numpy as np
from jax import lax
from jax.experimental import pallas as pl
from jax.experimental.pallas import tpu as pltpu
from jax.sharding import PartitionSpec as P


F32, BF16 = jnp.float32, jnp.bfloat16
PX, PD = (tuple((device, device ^ bit) for device in range(4)) for bit in (2, 1))
NN, NT = ((1,), (0,)), ((1,), (1,))

LANES = 128
BLOCK = 512
ROWS, FEW, TOGETHER = 512, 64, 4
HALF = 2 * ROWS


def dot(a, b, dims):
    return lax.dot_general(a, b, (dims, ((), ())), preferred_element_type=F32)


def sigmoid(x):
    return 0.5 * jnp.tanh(0.5 * x) + 0.5


def px(a):
    return lax.ppermute(a, "dp", PX)


def pd(a):
    return lax.ppermute(a, "dp", PD)


def once(shape, index):
    return pl.BlockSpec(shape, index, pipeline_mode=pl.Buffered(1))


def params(mib=62):
    return pltpu.CompilerParams(vmem_limit_bytes=mib << 20)


def norm_scale(wide):
    return lax.rsqrt(jnp.mean(wide * wide, -1, keepdims=True) + 1e-6)


def normed(h):
    wide = h.astype(F32)
    return (wide * norm_scale(wide)).astype(BF16)


def looped(count, rows, body, together=1, after=None):
    def one(n, carry):
        for part in range(together):
            body(pl.ds(pl.multiple_of((n * together + part) * rows, rows), rows))
        if after is not None:
            after(pl.ds(pl.multiple_of(n * together * rows, together * rows), together * rows))
        return carry

    lax.fori_loop(0, count // together, one, 0)


def written(step, last, half, own, tail, stage_ref, outs, sems, do):
    me = lax.axis_index("dp")
    blocks = own // BLOCK
    extra = own - blocks * BLOCK
    rows = pl.ds(pl.multiple_of(half * HALF, HALF), HALF)
    for n, (out, holder) in enumerate(zip(outs, (me, me // 2 * 2 + 1 - me % 2), strict=True)):

        def copy(here, there):
            do(pltpu.make_async_copy(stage_ref.at[half, :, :, here], out.at[:, rows, there], sems.at[n, half]))

        @pl.when((step < 4 * blocks) & (step // blocks == holder))
        def _():
            copy(pl.ds(0, BLOCK), pl.ds(pl.multiple_of(lax.rem(step, blocks) * BLOCK, BLOCK), BLOCK))

        @pl.when(step == 4 * blocks)
        def _():
            copy(pl.ds(pl.multiple_of(holder * extra, LANES), extra), pl.ds(blocks * BLOCK, extra))

        @pl.when(step == last)
        def _():
            copy(pl.ds(0, tail), pl.ds(own, tail))


def halves(tokens, width, moved, there, back):
    j = pl.program_id(0)

    def two(half, carry):
        @pl.when(j > 0)
        def _():
            moved(j - 1, half, lambda copy: copy.wait())

        def run(n):
            return half, n, pl.ds(pl.multiple_of(half * HALF + n * ROWS, ROWS), ROWS), width

        def one(n, carry):
            back(*run(n), there(*run(n)))
            return carry

        if width < BLOCK:
            lax.fori_loop(0, HALF // ROWS, one, 0)
        else:
            held = there(*run(0))
            ahead = there(*run(1))
            back(*run(0), held)
            back(*run(1), ahead)
        moved(j, half, lambda copy: copy.start())
        return carry

    lax.fori_loop(0, tokens // HALF, two, 0)


def forward_kernel(tail, own, x_ref, wg_ref, wu_ref, wd_ref, *refs):
    h_out, a_out, a0_out, mine_ref, theirs_ref, acc_ref, stage_ref, sems, h_ref, a_ref, a0_ref, out_sems = refs
    j, last = pl.program_id(0), pl.num_programs(0) - 1
    tokens = x_ref.shape[0]

    def moved(step, half, do):
        written(step, last, half, own, tail, stage_ref, (mine_ref, theirs_ref), sems, do)

    @pl.when(j == 0)
    def _():
        def start(r):
            a0_ref[r, :] = normed(x_ref[r, :])
            acc_ref[r, :] = jnp.zeros((FEW, acc_ref.shape[1]), F32)

        looped(tokens // FEW, FEW, start, TOGETHER)

    early = pltpu.make_async_copy(a0_ref, a0_out, out_sems.at[2])

    @pl.when(j == 1)
    def _():
        early.start()

    def up(half, n, r, width):
        a = a0_ref[r, :]
        g = dot(a, wg_ref[0, :, :width], NN)
        u = dot(a, wu_ref[0, :, :width], NN)
        for k, value in enumerate((g, u)):
            stage_ref[half, k, pl.ds(pl.multiple_of(n * ROWS, ROWS), ROWS), :width] = value
        return (g * sigmoid(g) * u).astype(BF16)

    def down(half, n, r, width, hid):
        acc_ref[r, :] += dot(hid, wd_ref[0, :width, :], NN)

    @pl.when(j < last)
    def _():
        halves(tokens, wg_ref.shape[2], moved, up, down)

    @pl.when(j == last)
    def _():
        halves(tokens, tail, moved, up, down)

        def end(r):
            h = (x_ref[r, :].astype(F32) + acc_ref[r, :].astype(BF16).astype(F32)).astype(BF16)
            h_ref[r, :] = h
            a_ref[r, :] = normed(h)

        def leave(n, r):
            return pltpu.make_async_copy((a_ref, h_ref)[n].at[r, :], (a_out, h_out)[n].at[r, :], out_sems.at[n])

        looped(tokens // FEW, FEW, end, TOGETHER, lambda r: [leave(n, r).start() for n in range(2)])
        for n in range(2):
            leave(n, pl.ds(0, tokens)).wait()
        early.wait()
        for half in range(tokens // (HALF)):
            moved(j, half, lambda copy: copy.wait())


def keeping(tokens, count, columns, dtype):
    kept = [jax.ShapeDtypeStruct((count, tokens, columns), dtype)] * 2
    parts = tokens // (HALF)
    return kept, [pltpu.VMEM((parts, count, HALF, BLOCK), dtype), pltpu.SemaphoreType.DMA((2, parts))]


def forward(own, x, wg, wu, wd):
    tokens, d = x.shape
    ff = wg.shape[2]
    steps = pl.cdiv(ff, BLOCK)
    tail = ff - (steps - 1) * BLOCK
    full = once((tokens, d), lambda j: (0, 0))
    across = pl.BlockSpec((1, d, BLOCK), lambda j: (0, 0, j))
    down = pl.BlockSpec((1, BLOCK, d), lambda j: (0, j, 0))
    kept, stage = keeping(tokens, 2, own + tail, F32)
    return pl.pallas_call(
        lambda *refs: forward_kernel(tail, own, *refs),
        grid=(steps,),
        in_specs=[full, across, across, down],
        out_specs=[pl.BlockSpec(memory_space=pl.ANY)] * 5,
        out_shape=[jax.ShapeDtypeStruct((tokens, d), BF16)] * 3 + kept,
        scratch_shapes=[pltpu.VMEM((tokens, d), F32)] + stage + [pltpu.VMEM((tokens, d), BF16)] * 3 + [pltpu.SemaphoreType.DMA((3,))],
        cost_estimate=pl.CostEstimate(flops=6 * tokens * d * ff, bytes_accessed=6 * d * ff, transcendentals=tokens * ff),
        compiler_params=params(),
        name="forward",
    )(x, wg, wu, wd)


def hidden_back(g, u, dhid):
    dhid = dhid.astype(BF16).astype(F32)
    sig = sigmoid(g)
    act = g * sig
    return (dhid * u * (sig + act * (1 - sig))).astype(BF16), (dhid * act).astype(BF16), (act * u).astype(BF16)


def chain_kernel(tail, own, a_ref, dy_ref, h_in, wg_ref, wu_ref, wd_ref, dh_out, mine_ref, theirs_ref, *scratch):
    acc_ref, stage_ref, sems, h_ref, dh_ref, out_sems = scratch
    j, last = pl.program_id(0), pl.num_programs(0) - 1
    tokens = a_ref.shape[0]

    def moved(step, half, do):
        written(step, last, half, own, tail, stage_ref, (mine_ref, theirs_ref), sems, do)

    late = pltpu.make_async_copy(h_in, h_ref, out_sems.at[0])

    @pl.when(j == 0)
    def _():
        def start(r):
            acc_ref[r, :] = jnp.zeros((FEW, acc_ref.shape[1]), F32)

        looped(tokens // FEW, FEW, start, TOGETHER)
        late.start()

    def there(half, n, r, width):
        a, dy = a_ref[r, :], dy_ref[r, :]
        g = dot(a, wg_ref[0, :, :width], NN)
        u = dot(a, wu_ref[0, :, :width], NN)
        for k, value in enumerate(hidden_back(g, u, dot(dy, wd_ref[0, :width, :], NT))):
            stage_ref[half, k, pl.ds(pl.multiple_of(n * ROWS, ROWS), ROWS), :width] = value

    def back(half, n, r, width, held):
        dg, du = (stage_ref[half, k, pl.ds(pl.multiple_of(n * ROWS, ROWS), ROWS), :width] for k in range(2))
        acc_ref[r, :] += dot(dg, wg_ref[0, :, :width], NT) + dot(du, wu_ref[0, :, :width], NT)

    @pl.when(j < last)
    def _():
        halves(tokens, wg_ref.shape[2], moved, there, back)

    @pl.when(j == last)
    def _():
        halves(tokens, tail, moved, there, back)
        late.wait()

        def end(r):
            wide, da = h_ref[r, :].astype(F32), acc_ref[r, :].astype(BF16).astype(F32)
            scale = norm_scale(wide)
            through = scale * da - wide * (scale * scale * scale * jnp.mean(wide * da, -1, keepdims=True))
            dh_ref[r, :] = (dy_ref[r, :].astype(F32) + through.astype(BF16).astype(F32)).astype(BF16)

        def leave(r):
            return pltpu.make_async_copy(dh_ref.at[r, :], dh_out.at[r, :], out_sems.at[1])

        looped(tokens // FEW, FEW, end, TOGETHER, lambda r: leave(r).start())
        leave(pl.ds(0, tokens)).wait()
        for half in range(tokens // (HALF)):
            moved(j, half, lambda copy: copy.wait())


def chain(own, a, dy, h, wg, wu, wd):
    tokens, d = a.shape
    ff = wg.shape[2]
    steps = pl.cdiv(ff, BLOCK)
    tail = ff - (steps - 1) * BLOCK
    full = once((tokens, d), lambda j: (0, 0))
    across = pl.BlockSpec((1, d, BLOCK), lambda j: (1, 0, j))
    down = pl.BlockSpec((1, BLOCK, d), lambda j: (1, j, 0))
    kept, stage = keeping(tokens, 3, own + tail, BF16)
    return pl.pallas_call(
        lambda *refs: chain_kernel(tail, own, *refs),
        grid=(steps,),
        in_specs=[full, full, pl.BlockSpec(memory_space=pl.ANY), across, across, down],
        out_specs=[pl.BlockSpec(memory_space=pl.ANY)] * 3,
        out_shape=[jax.ShapeDtypeStruct((tokens, d), BF16)] + kept,
        scratch_shapes=[pltpu.VMEM((tokens, d), F32)] + stage + [pltpu.VMEM((tokens, d), BF16)] * 2 + [pltpu.SemaphoreType.DMA((2,))],
        cost_estimate=pl.CostEstimate(flops=10 * tokens * d * ff, bytes_accessed=6 * d * ff, transcendentals=tokens * ff),
        compiler_params=params(),
        name="chain",
    )(a, dy, h, wg, wu, wd)


def slices_kernel(layer, own, kept, count, *refs):
    me = lax.axis_index("dp")
    chip, core = me // 2, me % 2
    partner = chip * 2 + 1 - core
    others = (partner, (1 - chip) * 2 + core, (1 - chip) * 2 + 1 - core)
    final = count is not None

    def take(n):
        nonlocal refs
        taken, refs = refs[:n], refs[n:]
        return taken

    a_own, a_across, dy_own, dy_across, wg_hbm, wu_hbm, wd_hbm = take(7)
    mine, theirs = take(2)
    before = take(2) if final else ()
    outs, (a_land, dy_land, held_land) = take(8), take(3)
    wg_ref, wu_ref, wd_ref, accg_ref, accu_ref, accd_ref, a_buf, dy_buf, sums_ref = take(9)
    sems, w_sems, send_sems, recv_sems = take(4)
    terms, (held_buf,), results = take(3), take(1), take(3)
    a_refs = (a_own, a_across, a_land.at[1], a_land.at[0])
    dy_refs = (dy_own, dy_across, dy_land.at[1], dy_land.at[0])
    held_refs = (mine, None, None, held_land)
    i, steps = pl.program_id(0), pl.num_programs(0)
    each = a_own.shape[0] // ROWS
    width = wg_ref.shape[1]
    main = own // BLOCK * BLOCK

    def fetch(step, do):
        slot, who = lax.rem(step, 2), step // each
        rows = pl.ds(pl.multiple_of(lax.rem(step, each) * ROWS, ROWS), ROWS)
        for k, (a, dy, held) in enumerate(zip(a_refs, dy_refs, held_refs, strict=True)):

            @pl.when(who == k)
            def _():
                do(pltpu.make_async_copy(a.at[rows, :], a_buf.at[slot], sems.at[0, slot]))
                do(pltpu.make_async_copy(dy.at[rows, :], dy_buf.at[slot], sems.at[1, slot]))
                if held is not None:
                    do(pltpu.make_async_copy(held.at[:, rows, :], held_buf.at[slot], sems.at[2, slot]))

    def weights():
        extra = own - main
        parts = (
            (pl.ds(pl.multiple_of(me * main, LANES), main), pl.ds(0, main)),
            (pl.ds(pl.multiple_of(4 * main + me * extra, LANES), extra), pl.ds(main, extra)),
            (pl.ds(4 * own, width - own), pl.ds(own, width - own)),
        )
        return [
            pltpu.make_async_copy(*((hbm.at[layer, there, :], ref.at[here, :]) if n == 2 else (hbm.at[layer, :, there], ref.at[:, here])), w_sems.at[n, m])
            for n, (hbm, ref) in enumerate(((wg_hbm, wg_ref), (wu_hbm, wu_ref), (wd_hbm, wd_ref)))
            for m, (there, here) in enumerate(parts)
        ]

    def onward(which):
        pairs = [(a_refs[which], a_land.at[which]), (dy_refs[which], dy_land.at[which])]
        if which == 0:
            pairs.append((theirs, held_land))
        return [
            pltpu.make_async_remote_copy(
                src_ref=src,
                dst_ref=dst,
                send_sem=send_sems.at[3 * which + n],
                recv_sem=recv_sems.at[3 * which + n],
                device_id={"dp": partner},
                device_id_type=pl.DeviceIdType.MESH,
            )
            for n, (src, dst) in enumerate(pairs)
        ]

    def told(n):
        return pltpu.make_async_remote_copy(
            src_ref=sums_ref.at[0],
            dst_ref=sums_ref.at[1 + n],
            send_sem=send_sems.at[6 + n],
            recv_sem=recv_sems.at[6 + n],
            device_id={"dp": others[n]},
            device_id_type=pl.DeviceIdType.MESH,
        )

    barrier = pltpu.get_barrier_semaphore()
    spoken = others if final else others[:1]

    @pl.when(i == 0)
    def _():
        for other in spoken:
            pl.semaphore_signal(barrier, inc=1, device_id={"dp": other}, device_id_type=pl.DeviceIdType.MESH)
        fetch(i, lambda copy: copy.start())
        for copy in weights():
            copy.start()
        for copy in weights():
            copy.wait()

    @pl.when(i == 1)
    def _():
        pl.semaphore_wait(barrier, len(spoken))
        for which in (1, 0):
            for copy in onward(which):
                copy.start()

    for which in range(2):

        @pl.when(i == (3 - which) * each - 1)
        def _():
            for copy in onward(which):
                copy.wait()

    @pl.when(i + 1 < steps)
    def _():
        fetch(i + 1, lambda copy: copy.start())

    slot = lax.rem(i, 2)
    pltpu.make_async_copy(a_own.at[pl.ds(0, ROWS), :], a_buf.at[slot], sems.at[0, slot]).wait()
    pltpu.make_async_copy(dy_own.at[pl.ds(0, ROWS), :], dy_buf.at[slot], sems.at[1, slot]).wait()
    blocks = [pl.ds(c, min(BLOCK, width - c)) for c in range(0, width, BLOCK)]

    def through(there, first):
        a_t, dy_t = a_buf[slot].T, dy_buf[slot].T

        def back(s, held):
            dg, du, hid = held
            for acc, left, right in ((accg_ref, a_t, dg), (accu_ref, a_t, du), (accd_ref, dy_t, hid)):
                acc[:, s] = (jnp.where(i == 0, 0.0, acc[:, s]) if first else acc[:, s]) + dot(left, right, NN)

        held = there(blocks[0])
        for s, following in zip(blocks, blocks[1:] + [None], strict=True):
            ahead = None if following is None else there(following)
            back(s, held)
            held = ahead

    known = (i // each == 0) | (i // each == 3)

    @pl.when(known)
    def _():
        pltpu.make_async_copy(mine.at[:, pl.ds(0, ROWS), :], held_buf.at[slot], sems.at[2, slot]).wait()

    if kept == 2:

        @pl.when(jnp.logical_not(known))
        def _():
            for s in blocks:
                held_buf[slot, 0, :, s] = dot(a_buf[slot], wg_ref[:, s], NN)
                held_buf[slot, 1, :, s] = dot(a_buf[slot], wu_ref[:, s], NN)

        through(lambda s: hidden_back(held_buf[slot, 0, :, s], held_buf[slot, 1, :, s], dot(dy_buf[slot], wd_ref[s, :], NT)), True)
    else:

        @pl.when(known)
        def _():
            through(lambda s: [held_buf[slot, n, :, s] for n in range(3)], True)

        @pl.when(jnp.logical_not(known))
        def _():
            a, dy = a_buf[slot], dy_buf[slot]
            through(lambda s: hidden_back(dot(a, wg_ref[:, s], NN), dot(a, wu_ref[:, s], NN), dot(dy, wd_ref[s, :], NT)), False)

    rest = pl.ds(own, width - own)

    @pl.when(lax.rem(i, each) == each - 1)
    def _():
        for acc, term in zip((accg_ref, accu_ref, accd_ref), terms, strict=True):
            term[i // each] = acc[:, rest]
            acc[:, rest] = jnp.zeros_like(acc[:, rest])

    @pl.when(i == steps - 1)
    def _():
        def rounded(part, total):
            part = part.astype(BF16)
            wide = part.astype(F32)
            return part, total + jnp.sum((wide * wide).reshape(-1, 8, LANES), 0)

        accs = (accg_ref, accu_ref, accd_ref)

        def leave(n, at):
            return pltpu.make_async_copy(results[n].at[at, :], outs[n].at[at, :], w_sems.at[n, 0])

        def rows(r, total):
            at = pl.ds(pl.multiple_of(r * LANES, LANES), LANES)
            for n, acc in enumerate(accs):
                for c in range(0, own, LANES):
                    part, total = rounded(acc[at, c : c + LANES], total)
                    if n < 2:
                        results[n][at, c : c + LANES] = part
            for n in range(2):
                leave(n, at).start()
            return total

        def turn(c, carry):
            at = pl.ds(pl.multiple_of(c * LANES, LANES), LANES)
            for r in range(0, a_buf.shape[2], LANES):
                results[2][at, r : r + LANES] = accd_ref[r : r + LANES, at].astype(BF16).T
            leave(2, at).start()
            return carry

        at = [3 * ((core + s) % 2) + (chip + s // 2) % 2 * (1 - 2 * ((core + s) % 2)) for s in range(4)]
        place = [(core + s) % 2 + 2 * ((chip + s // 2) % 2) for s in range(4)]
        sums = [lax.fori_loop(0, a_buf.shape[2] // LANES, rows, jnp.zeros((8, LANES), F32)), jnp.zeros((8, LANES), F32)]
        lax.fori_loop(0, own // LANES, turn, 0)
        for n, term in enumerate(terms):
            part, sums[1] = rounded(term[at[0]] + term[at[1]] + term[at[2]] + term[at[3]], sums[1])
            outs[3 + n][...] = part if n < 2 else part.T
        for n, result in enumerate(results):
            leave(n, pl.ds(0, result.shape[0])).wait()
        if not final:
            outs[6][...], outs[7][...] = sums
        else:
            sums_ref[0] = sums[0] + before[0][...]
            shared = jnp.sum(sums[1] + before[1][...])
            for n in range(3):
                told(n).start()
            for n in range(3):
                told(n).wait()
            total = sums_ref[place[0]] + sums_ref[place[1]] + sums_ref[place[2]] + sums_ref[place[3]]
            total = jnp.full((8, LANES), jnp.sum(total) + shared, F32)
            outs[6][...] = jnp.minimum(1.0, 0.5 * lax.rsqrt(total / count + 1e-30))
            outs[7][...] = jnp.zeros((8, LANES), F32)


def slices(layer, own, a_all, dy_all, wg, wu, wd, kept, before=(), count=None):
    tokens, d = a_all[0].shape
    ff = wg.shape[2]
    rest = ff - 4 * own
    width = own + rest
    any_ = pl.BlockSpec(memory_space=pl.ANY)
    at = lambda s: once(s, lambda i: (0, 0))
    sizes = [(d, own), (d, own), (own, d), (d, rest), (d, rest), (rest, d)]
    landed = [jax.ShapeDtypeStruct((2, tokens, d), BF16)] * 2 + [kept[0]]
    return pl.pallas_call(
        lambda *refs: slices_kernel(layer, own, kept[0].shape[0], count, *refs),
        grid=(4 * tokens // ROWS,),
        in_specs=[any_] * (7 + len(kept)) + [at((8, LANES))] * len(before),
        out_specs=[any_] * 3 + [at(s) for s in sizes[3:]] + [at((8, LANES))] * 2 + [any_] * len(landed),
        scratch_shapes=[pltpu.VMEM((d, width), BF16)] * 2
        + [pltpu.VMEM((width, d), BF16)]
        + [pltpu.VMEM((d, width), F32)] * 3
        + [pltpu.VMEM((2, ROWS, d), BF16)] * 2
        + [pltpu.VMEM((4, 8, LANES), F32)]
        + [pltpu.SemaphoreType.DMA(n) for n in ((3, 2), (3, 3), (9,), (9,))]
        + [pltpu.VMEM((4, d, rest), F32)] * 3
        + [pltpu.VMEM((2, kept[0].shape[0], ROWS, width), kept[0].dtype)]
        + [pltpu.VMEM(s, BF16) for s in sizes[:3]],
        out_shape=[jax.ShapeDtypeStruct(s, BF16) for s in sizes]
        + [jax.ShapeDtypeStruct((8, LANES), F32)] * 2
        + [jax.ShapeDtypeStruct(s.shape, s.dtype) for s in landed],
        cost_estimate=pl.CostEstimate(
            flops=12 * 4 * tokens * d * width, bytes_accessed=16 * tokens * d, transcendentals=4 * tokens * width
        ),
        compiler_params=pltpu.CompilerParams(vmem_limit_bytes=62 << 20, collective_id=layer, has_side_effects=True),
        name="slices",
    )(*a_all, *dy_all, wg, wu, wd, *kept, *before)


def adam_math(f, w, m, v, g):
    g = g.astype(F32) * f
    m = 0.9 * m + 0.1 * g
    v = 0.95 * v + 0.05 * g * g
    return (0.998 * w.astype(F32) - 0.02 * (m * lax.rsqrt(v + 1e-8))).astype(BF16), m, v


SLOTS, AHEAD = 8, 4


def adam(own, factor, arrays, pieces, outs):
    d, _ = arrays[0][0].shape[1:]
    main, extra = own // BLOCK * BLOCK, own % BLOCK
    shapes = ((LANES, own), (LANES, d), (d // 2, LANES))
    rows = []
    for n, (which, layer, slot, g) in enumerate(pieces):
        kind = 1 if which == 2 else 2 if slot == 4 else 0
        for r in range(0, g.shape[0], shapes[kind][0]):
            if kind != 1:
                first = (r, 0)
            elif slot == 4:
                first = (4 * own + r, 0)
            else:
                first = (r, main) if r < main else (4 * main + r - main, extra)
            rows.append((kind, which, layer, n, slot, r, *first))
    table = np.array(rows, np.int32).T
    total = len(rows)
    kinds = sorted({row[0] for row in rows})
    n_in = 9 + len(pieces)

    def kernel(table_ref, f_ref, *refs):
        weights, grads = refs[:9], refs[9:n_in]
        refs = refs[n_in + (9 if outs is not None else 0) :]
        results, scratch = refs[:9], refs[9:]
        buffers = {kind: scratch[4 * n : 4 * n + 4] for n, kind in enumerate(kinds)}
        sem_in, sem_out = scratch[-2:]
        f = f_ref[:1, :1]
        me = lax.axis_index("dp")

        def moved(step, do):
            kind, which, layer = (table_ref[n, step] for n in range(3))
            slot = table_ref[4, step]
            unit = (me + slot) % 2 + 2 * ((me // 2 + slot // 2) % 2)
            row = table_ref[6, step] + table_ref[7, step] * unit
            for k in range(3):
                for q in [q for q in kinds if (q == 1) == (k == 2)]:
                    if q == 0:
                        columns = ((unit * main, 0, main), (4 * main + unit * extra, main, extra))
                    else:
                        columns = ((0 if q == 1 else 4 * own, 0, shapes[q][1]),)

                    @pl.when((which == k) & (kind == q))
                    def _():
                        for first, here, size in columns:
                            first = first if isinstance(first, int) else pl.multiple_of(first, LANES)
                            there = (layer, pl.ds(pl.multiple_of(row, LANES), shapes[q][0]), pl.ds(first, size))
                            do(3 * k, there, buffers[q], (lax.rem(step, SLOTS), slice(None), pl.ds(here, size)))

        def fetch(step):
            slot = lax.rem(step, SLOTS)

            def get(k, there, buffer, here):
                for n in range(3):
                    pltpu.make_async_copy(weights[k + n].at[there], buffer[n].at[here], sem_in.at[n, slot]).start()

            moved(step, get)
            piece, row = table_ref[3, step], table_ref[5, step]
            for n, (which_, _, slot_, _) in enumerate(pieces):
                q = 1 if which_ == 2 else 2 if slot_ == 4 else 0

                @pl.when(piece == n)
                def _():
                    rows_ = pl.ds(pl.multiple_of(row, 16), shapes[q][0])
                    pltpu.make_async_copy(grads[n].at[rows_, :], buffers[q][3].at[slot], sem_in.at[3, slot]).start()

        def stored(step, do):
            slot = lax.rem(step, SLOTS)

            def put(k, there, buffer, here):
                for n in range(3):
                    do(pltpu.make_async_copy(buffer[n].at[here], results[k + n].at[there], sem_out.at[n, slot]))

            moved(step, put)

        def early(step, carry):
            fetch(step)
            return carry

        lax.fori_loop(0, min(AHEAD, total), early, 0)

        def body(step, carry):
            @pl.when(step + AHEAD < total)
            def _():
                @pl.when(step + AHEAD >= SLOTS)
                def _():
                    stored(step + AHEAD - SLOTS, lambda copy: copy.wait())

                fetch(step + AHEAD)

            slot = lax.rem(step, SLOTS)
            for q in kinds:

                @pl.when(table_ref[0, step] == q)
                def _():
                    w, m, v, g = buffers[q]
                    for n in range(4):
                        pltpu.make_async_copy(buffers[q][n].at[slot], buffers[q][n].at[slot], sem_in.at[n, slot]).wait()
                    some = 32 if shapes[q][1] > LANES else 224

                    def part(r, carry):
                        at = pl.ds(pl.multiple_of(r * some, some), some)
                        new = adam_math(f, w[slot, at, :], m[slot, at, :], v[slot, at, :], g[slot, at, :])
                        w[slot, at, :], m[slot, at, :], v[slot, at, :] = new
                        return carry

                    lax.fori_loop(0, shapes[q][0] // some, part, 0)

            stored(step, lambda copy: copy.start())
            return carry

        lax.fori_loop(0, total, body, 0)

        def late(step, carry):
            stored(step, lambda copy: copy.wait())
            return carry

        lax.fori_loop(max(0, total - SLOTS), total, late, 0)

    any_ = pl.BlockSpec(memory_space=pl.ANY)
    given = [a for three in arrays for a in three]
    given = [pltpu.with_memory_space_constraint(a, pltpu.HBM) for a in given]
    if outs is None:
        pieces = [(*piece[:3], pltpu.with_memory_space_constraint(piece[3], pltpu.HBM)) for piece in pieces]
    before = [a for three in outs for a in three] if outs is not None else []
    elements = sum(piece[3].size for piece in pieces)
    new = pl.pallas_call(
        kernel,
        in_specs=[pl.BlockSpec(memory_space=pltpu.SMEM), pl.BlockSpec(memory_space=pltpu.VMEM)] + [any_] * (n_in + len(before)),
        out_specs=[any_] * 9,
        out_shape=[jax.ShapeDtypeStruct(a.shape, a.dtype) for a in given],
        scratch_shapes=[pltpu.VMEM((SLOTS, *shapes[q]), t) for q in kinds for t in (BF16, F32, F32, BF16)]
        + [pltpu.SemaphoreType.DMA((4, SLOTS)), pltpu.SemaphoreType.DMA((3, SLOTS))],
        input_output_aliases={2 + n_in + n: n for n in range(len(before))},
        cost_estimate=pl.CostEstimate(flops=2000 * elements, bytes_accessed=22 * elements, transcendentals=elements),
        compiler_params=params(30),
    )(table, factor, *given, *(piece[3] for piece in pieces), *before)
    return tuple(tuple(new[3 * n : 3 * n + 3]) for n in range(3))


def solution(mesh):
    def step(x, dy, wg, wu, wd, mg, mu, md, vg, vu, vd):
        x, dy = x[0], dy[0]
        ff = wg.shape[2]
        own = ff // LANES // 4 * LANES

        def send(a, perm):
            return perm(a)

        dy_x = send(dy, px)
        h1, a1, a0, *made = forward(own, x, wg, wu, wd)
        a1_x = send(a1, px)
        a0_x = send(a0, px)
        dh1, *kept = chain(own, a1, dy, h1, wg, wu, wd)
        dh1_x = send(dh1, px)
        top = slices(1, own, [a1, a1_x], [dy, dy_x], wg, wu, wd, kept)
        top_x = [send(top[n], px) for n in range(3)]
        top_d = [send(top[n], pd) for n in range(3)]
        low = slices(0, own, [a0, a0_x], [dh1, dh1_x], wg, wu, wd, made, top[6:8], wg.size + wu.size + wd.size)
        low_x = [send(low[n], px) for n in range(3)]
        low_d = [send(low[n], pd) for n in range(3)]

        top_xd = [send(top_x[n], pd) for n in range(3)]
        low_xd = [send(low_x[n], pd) for n in range(2)]
        arrays = ((wg, mg, vg), (wu, mu, vu), (wd, md, vd))

        def pieces(layer, slot, gs, names=(0, 1, 2)):
            return [(n, layer, slot, gs[n]) for n in names]

        first = pieces(1, 0, top) + pieces(1, 1, top_d) + pieces(1, 2, top_x) + pieces(0, 0, low)
        shared = pieces(1, 4, top[3:6]) + pieces(0, 4, low[3:6])
        outs = adam(own, low[6], arrays, first + shared, None)
        outs = adam(own, low[6], arrays, pieces(1, 3, top_xd) + pieces(0, 1, low_d), outs)
        outs, low_x[2] = lax.optimization_barrier((outs, low_x[2]))
        low_xd.append(send(low_x[2], pd))
        outs = adam(own, low[6], arrays, pieces(0, 2, low_x) + pieces(0, 3, low_xd, (0, 1)), outs)
        outs = adam(own, low[6], arrays, pieces(0, 3, low_xd, (2,)), outs)
        return tuple(outs[name][which] for which in range(3) for name in range(3))

    return jax.shard_map(
        step,
        mesh=mesh,
        in_specs=(P(("rep", "dp"), None, None),) * 2 + (P(None, None, None),) * 9,
        out_specs=(P("rep", None, None),) * 9,
        check_vma=False,
    )
```

```python
import jax
import jax.numpy as jnp
import numpy as np
from jax import lax
from jax.experimental import pallas as pl
from jax.experimental.pallas import tpu as pltpu
from jax.sharding import PartitionSpec as P


F32, BF16 = jnp.float32, jnp.bfloat16
PX, PD = (tuple((device, device ^ bit) for device in range(4)) for bit in (2, 1))
NN, NT = ((1,), (0,)), ((1,), (1,))

LANES = 128
BLOCK = 512
ROWS, FEW, TOGETHER = 512, 64, 4
HALF = 2 * ROWS


def dot(a, b, dims):
    return lax.dot_general(a, b, (dims, ((), ())), preferred_element_type=F32)


def sigmoid(x):
    return 0.5 * jnp.tanh(0.5 * x) + 0.5


def px(a):
    return lax.ppermute(a, "dp", PX)


def pd(a):
    return lax.ppermute(a, "dp", PD)


def once(shape, index):
    return pl.BlockSpec(shape, index, pipeline_mode=pl.Buffered(1))


def params(mib=62):
    return pltpu.CompilerParams(vmem_limit_bytes=mib << 20)


def norm_scale(wide):
    return lax.rsqrt(jnp.mean(wide * wide, -1, keepdims=True) + 1e-6)


def normed(h):
    wide = h.astype(F32)
    return (wide * norm_scale(wide)).astype(BF16)


def looped(count, rows, body, together=1, after=None):
    def one(n, carry):
        for part in range(together):
            body(pl.ds(pl.multiple_of((n * together + part) * rows, rows), rows))
        if after is not None:
            after(pl.ds(pl.multiple_of(n * together * rows, together * rows), together * rows))
        return carry

    lax.fori_loop(0, count // together, one, 0)


def written(step, last, half, own, tail, stage_ref, outs, sems, do):
    me = lax.axis_index("dp")
    blocks = own // BLOCK
    extra = own - blocks * BLOCK
    rows = pl.ds(pl.multiple_of(half * HALF, HALF), HALF)
    for n, (out, holder) in enumerate(zip(outs, (me, me // 2 * 2 + 1 - me % 2), strict=True)):

        def copy(here, there):
            do(pltpu.make_async_copy(stage_ref.at[half, :, :, here], out.at[:, rows, there], sems.at[n, half]))

        @pl.when((step < 4 * blocks) & (step // blocks == holder))
        def _():
            copy(pl.ds(0, BLOCK), pl.ds(pl.multiple_of(lax.rem(step, blocks) * BLOCK, BLOCK), BLOCK))

        @pl.when(step == 4 * blocks)
        def _():
            copy(pl.ds(pl.multiple_of(holder * extra, LANES), extra), pl.ds(blocks * BLOCK, extra))

        @pl.when(step == last)
        def _():
            copy(pl.ds(0, tail), pl.ds(own, tail))


def halves(tokens, width, moved, there, back):
    j = pl.program_id(0)

    def two(half, carry):
        @pl.when(j > 0)
        def _():
            moved(j - 1, half, lambda copy: copy.wait())

        def run(n):
            return half, n, pl.ds(pl.multiple_of(half * HALF + n * ROWS, ROWS), ROWS), width

        def one(n, carry):
            back(*run(n), there(*run(n)))
            return carry

        if width < BLOCK:
            lax.fori_loop(0, HALF // ROWS, one, 0)
        else:
            held = there(*run(0))
            ahead = there(*run(1))
            back(*run(0), held)
            back(*run(1), ahead)
        moved(j, half, lambda copy: copy.start())
        return carry

    lax.fori_loop(0, tokens // HALF, two, 0)


def forward_kernel(tail, own, x_ref, wg_ref, wu_ref, wd_ref, *refs):
    h_out, a_out, a0_out, mine_ref, theirs_ref, acc_ref, stage_ref, sems, h_ref, a_ref, a0_ref, out_sems = refs
    j, last = pl.program_id(0), pl.num_programs(0) - 1
    tokens = x_ref.shape[0]

    def moved(step, half, do):
        written(step, last, half, own, tail, stage_ref, (mine_ref, theirs_ref), sems, do)

    @pl.when(j == 0)
    def _():
        def start(r):
            a0_ref[r, :] = normed(x_ref[r, :])
            acc_ref[r, :] = jnp.zeros((FEW, acc_ref.shape[1]), F32)

        looped(tokens // FEW, FEW, start, TOGETHER)

    early = pltpu.make_async_copy(a0_ref, a0_out, out_sems.at[2])

    @pl.when(j == 1)
    def _():
        early.start()

    def up(half, n, r, width):
        a = a0_ref[r, :]
        g = dot(a, wg_ref[0, :, :width], NN)
        u = dot(a, wu_ref[0, :, :width], NN)
        for k, value in enumerate((g, u)):
            stage_ref[half, k, pl.ds(pl.multiple_of(n * ROWS, ROWS), ROWS), :width] = value
        return (g * sigmoid(g) * u).astype(BF16)

    def down(half, n, r, width, hid):
        acc_ref[r, :] += dot(hid, wd_ref[0, :width, :], NN)

    @pl.when(j < last)
    def _():
        halves(tokens, wg_ref.shape[2], moved, up, down)

    @pl.when(j == last)
    def _():
        halves(tokens, tail, moved, up, down)

        def end(r):
            h = (x_ref[r, :].astype(F32) + acc_ref[r, :].astype(BF16).astype(F32)).astype(BF16)
            h_ref[r, :] = h
            a_ref[r, :] = normed(h)

        def leave(n, r):
            return pltpu.make_async_copy((a_ref, h_ref)[n].at[r, :], (a_out, h_out)[n].at[r, :], out_sems.at[n])

        looped(tokens // FEW, FEW, end, TOGETHER, lambda r: [leave(n, r).start() for n in range(2)])
        for n in range(2):
            leave(n, pl.ds(0, tokens)).wait()
        early.wait()
        for half in range(tokens // (HALF)):
            moved(j, half, lambda copy: copy.wait())


def keeping(tokens, count, columns, dtype):
    kept = [jax.ShapeDtypeStruct((count, tokens, columns), dtype)] * 2
    parts = tokens // (HALF)
    return kept, [pltpu.VMEM((parts, count, HALF, BLOCK), dtype), pltpu.SemaphoreType.DMA((2, parts))]


def forward(own, x, wg, wu, wd):
    tokens, d = x.shape
    ff = wg.shape[2]
    steps = pl.cdiv(ff, BLOCK)
    tail = ff - (steps - 1) * BLOCK
    full = once((tokens, d), lambda j: (0, 0))
    across = pl.BlockSpec((1, d, BLOCK), lambda j: (0, 0, j))
    down = pl.BlockSpec((1, BLOCK, d), lambda j: (0, j, 0))
    kept, stage = keeping(tokens, 2, own + tail, F32)
    return pl.pallas_call(
        lambda *refs: forward_kernel(tail, own, *refs),
        grid=(steps,),
        in_specs=[full, across, across, down],
        out_specs=[pl.BlockSpec(memory_space=pl.ANY)] * 5,
        out_shape=[jax.ShapeDtypeStruct((tokens, d), BF16)] * 3 + kept,
        scratch_shapes=[pltpu.VMEM((tokens, d), F32)] + stage + [pltpu.VMEM((tokens, d), BF16)] * 3 + [pltpu.SemaphoreType.DMA((3,))],
        cost_estimate=pl.CostEstimate(flops=6 * tokens * d * ff, bytes_accessed=6 * d * ff, transcendentals=tokens * ff),
        compiler_params=params(),
        name="forward",
    )(x, wg, wu, wd)


def hidden_back(g, u, dhid):
    dhid = dhid.astype(BF16).astype(F32)
    sig = sigmoid(g)
    act = g * sig
    return (dhid * u * (sig + act * (1 - sig))).astype(BF16), (dhid * act).astype(BF16), (act * u).astype(BF16)


def chain_kernel(tail, own, a_ref, dy_ref, h_in, wg_ref, wu_ref, wd_ref, dh_out, mine_ref, theirs_ref, *scratch):
    acc_ref, stage_ref, sems, h_ref, dh_ref, out_sems = scratch
    j, last = pl.program_id(0), pl.num_programs(0) - 1
    tokens = a_ref.shape[0]

    def moved(step, half, do):
        written(step, last, half, own, tail, stage_ref, (mine_ref, theirs_ref), sems, do)

    late = pltpu.make_async_copy(h_in, h_ref, out_sems.at[0])

    @pl.when(j == 0)
    def _():
        def start(r):
            acc_ref[r, :] = jnp.zeros((FEW, acc_ref.shape[1]), F32)

        looped(tokens // FEW, FEW, start, TOGETHER)
        late.start()

    def there(half, n, r, width):
        a, dy = a_ref[r, :], dy_ref[r, :]
        g = dot(a, wg_ref[0, :, :width], NN)
        u = dot(a, wu_ref[0, :, :width], NN)
        for k, value in enumerate(hidden_back(g, u, dot(dy, wd_ref[0, :width, :], NT))):
            stage_ref[half, k, pl.ds(pl.multiple_of(n * ROWS, ROWS), ROWS), :width] = value

    def back(half, n, r, width, held):
        dg, du = (stage_ref[half, k, pl.ds(pl.multiple_of(n * ROWS, ROWS), ROWS), :width] for k in range(2))
        acc_ref[r, :] += dot(dg, wg_ref[0, :, :width], NT) + dot(du, wu_ref[0, :, :width], NT)

    @pl.when(j < last)
    def _():
        halves(tokens, wg_ref.shape[2], moved, there, back)

    @pl.when(j == last)
    def _():
        halves(tokens, tail, moved, there, back)
        late.wait()

        def end(r):
            wide, da = h_ref[r, :].astype(F32), acc_ref[r, :].astype(BF16).astype(F32)
            scale = norm_scale(wide)
            through = scale * da - wide * (scale * scale * scale * jnp.mean(wide * da, -1, keepdims=True))
            dh_ref[r, :] = (dy_ref[r, :].astype(F32) + through.astype(BF16).astype(F32)).astype(BF16)

        def leave(r):
            return pltpu.make_async_copy(dh_ref.at[r, :], dh_out.at[r, :], out_sems.at[1])

        looped(tokens // FEW, FEW, end, TOGETHER, lambda r: leave(r).start())
        leave(pl.ds(0, tokens)).wait()
        for half in range(tokens // (HALF)):
            moved(j, half, lambda copy: copy.wait())


def chain(own, a, dy, h, wg, wu, wd):
    tokens, d = a.shape
    ff = wg.shape[2]
    steps = pl.cdiv(ff, BLOCK)
    tail = ff - (steps - 1) * BLOCK
    full = once((tokens, d), lambda j: (0, 0))
    across = pl.BlockSpec((1, d, BLOCK), lambda j: (1, 0, j))
    down = pl.BlockSpec((1, BLOCK, d), lambda j: (1, j, 0))
    kept, stage = keeping(tokens, 3, own + tail, BF16)
    return pl.pallas_call(
        lambda *refs: chain_kernel(tail, own, *refs),
        grid=(steps,),
        in_specs=[full, full, pl.BlockSpec(memory_space=pl.ANY), across, across, down],
        out_specs=[pl.BlockSpec(memory_space=pl.ANY)] * 3,
        out_shape=[jax.ShapeDtypeStruct((tokens, d), BF16)] + kept,
        scratch_shapes=[pltpu.VMEM((tokens, d), F32)] + stage + [pltpu.VMEM((tokens, d), BF16)] * 2 + [pltpu.SemaphoreType.DMA((2,))],
        cost_estimate=pl.CostEstimate(flops=10 * tokens * d * ff, bytes_accessed=6 * d * ff, transcendentals=tokens * ff),
        compiler_params=params(),
        name="chain",
    )(a, dy, h, wg, wu, wd)


GATE_UP, DOWN = (0, 1), (2,)


def slices_kernel(layer, own, kept, count, *refs):
    me = lax.axis_index("dp")
    chip, core = me // 2, me % 2
    partner = chip * 2 + 1 - core
    others = (partner, (1 - chip) * 2 + core, (1 - chip) * 2 + 1 - core)
    final = count is not None

    def take(n):
        nonlocal refs
        taken, refs = refs[:n], refs[n:]
        return taken

    a_own, a_across, dy_own, dy_across, wg_hbm, wu_hbm, wd_hbm = take(7)
    mine, theirs = take(2)
    before = take(2) if final else ()
    outs, (a_land, dy_land, held_land) = take(8), take(3)
    wg_ref, wu_ref, wd_ref, accg_ref, accu_ref, accd_ref, a_buf, dy_buf, sums_ref = take(9)
    sems, w_sems, send_sems, recv_sems = take(4)
    terms, (held_buf,), results = take(3), take(1), take(3)
    a_refs = (a_own, a_across, a_land.at[1], a_land.at[0])
    dy_refs = (dy_own, dy_across, dy_land.at[1], dy_land.at[0])
    held_refs = (mine, None, None, held_land)
    i, steps = pl.program_id(0), pl.num_programs(0)
    each = a_own.shape[0] // ROWS
    width = wg_ref.shape[1]
    main = own // BLOCK * BLOCK

    def fetch(step, do):
        slot, who = lax.rem(step, 2), step // each
        rows = pl.ds(pl.multiple_of(lax.rem(step, each) * ROWS, ROWS), ROWS)
        for k, (a, dy, held) in enumerate(zip(a_refs, dy_refs, held_refs, strict=True)):

            @pl.when(who == k)
            def _():
                do(pltpu.make_async_copy(a.at[rows, :], a_buf.at[slot], sems.at[0, slot]))
                do(pltpu.make_async_copy(dy.at[rows, :], dy_buf.at[slot], sems.at[1, slot]))
                if held is not None:
                    do(pltpu.make_async_copy(held.at[:, rows, :], held_buf.at[slot], sems.at[2, slot]))

    def weights(which):
        extra = own - main
        parts = (
            (pl.ds(pl.multiple_of(me * main, LANES), main), pl.ds(0, main)),
            (pl.ds(pl.multiple_of(4 * main + me * extra, LANES), extra), pl.ds(main, extra)),
            (pl.ds(4 * own, width - own), pl.ds(own, width - own)),
        )
        return [
            pltpu.make_async_copy(*((hbm.at[layer, there, :], ref.at[here, :]) if n == 2 else (hbm.at[layer, :, there], ref.at[:, here])), w_sems.at[n, m])
            for n, (hbm, ref) in enumerate(((wg_hbm, wg_ref), (wu_hbm, wu_ref), (wd_hbm, wd_ref)))
            if n in which
            for m, (there, here) in enumerate(parts)
        ]

    def onward(which):
        pairs = [(a_refs[which], a_land.at[which]), (dy_refs[which], dy_land.at[which])]
        if which == 0:
            pairs.append((theirs, held_land))
        return [
            pltpu.make_async_remote_copy(
                src_ref=src,
                dst_ref=dst,
                send_sem=send_sems.at[3 * which + n],
                recv_sem=recv_sems.at[3 * which + n],
                device_id={"dp": partner},
                device_id_type=pl.DeviceIdType.MESH,
            )
            for n, (src, dst) in enumerate(pairs)
        ]

    def told(n):
        return pltpu.make_async_remote_copy(
            src_ref=sums_ref.at[0],
            dst_ref=sums_ref.at[1 + n],
            send_sem=send_sems.at[6 + n],
            recv_sem=recv_sems.at[6 + n],
            device_id={"dp": others[n]},
            device_id_type=pl.DeviceIdType.MESH,
        )

    barrier = pltpu.get_barrier_semaphore()
    spoken = others if final else others[:1]

    @pl.when(i == 0)
    def _():
        for other in spoken:
            pl.semaphore_signal(barrier, inc=1, device_id={"dp": other}, device_id_type=pl.DeviceIdType.MESH)
        for copy in weights(DOWN) if kept == 2 else ():
            copy.start()
        fetch(i, lambda copy: copy.start())
        for copy in weights(GATE_UP if kept == 2 else GATE_UP + DOWN):
            copy.start()
        for copy in weights(DOWN) if kept == 2 else ():
            copy.wait()

    @pl.when(i == 1)
    def _():
        for copy in weights(GATE_UP if kept == 2 else GATE_UP + DOWN):
            copy.wait()
        pl.semaphore_wait(barrier, len(spoken))
        for which in (1, 0):
            for copy in onward(which):
                copy.start()

    for which in range(2):

        @pl.when(i == (3 - which) * each - 1)
        def _():
            for copy in onward(which):
                copy.wait()

    @pl.when(i + 1 < steps)
    def _():
        fetch(i + 1, lambda copy: copy.start())

    slot = lax.rem(i, 2)
    pltpu.make_async_copy(a_own.at[pl.ds(0, ROWS), :], a_buf.at[slot], sems.at[0, slot]).wait()
    pltpu.make_async_copy(dy_own.at[pl.ds(0, ROWS), :], dy_buf.at[slot], sems.at[1, slot]).wait()
    blocks = [pl.ds(c, min(BLOCK, width - c)) for c in range(0, width, BLOCK)]

    def through(there, first):
        a_t, dy_t = a_buf[slot].T, dy_buf[slot].T

        def back(s, held):
            dg, du, hid = held
            for acc, left, right in ((accg_ref, a_t, dg), (accu_ref, a_t, du), (accd_ref, dy_t, hid)):
                acc[:, s] = (jnp.where(i == 0, 0.0, acc[:, s]) if first else acc[:, s]) + dot(left, right, NN)

        held = there(blocks[0])
        for s, following in zip(blocks, blocks[1:] + [None], strict=True):
            ahead = None if following is None else there(following)
            back(s, held)
            held = ahead

    known = (i // each == 0) | (i // each == 3)

    @pl.when(known)
    def _():
        pltpu.make_async_copy(mine.at[:, pl.ds(0, ROWS), :], held_buf.at[slot], sems.at[2, slot]).wait()

    if kept == 2:

        @pl.when(jnp.logical_not(known))
        def _():
            for s in blocks:
                held_buf[slot, 0, :, s] = dot(a_buf[slot], wg_ref[:, s], NN)
                held_buf[slot, 1, :, s] = dot(a_buf[slot], wu_ref[:, s], NN)

        through(lambda s: hidden_back(held_buf[slot, 0, :, s], held_buf[slot, 1, :, s], dot(dy_buf[slot], wd_ref[s, :], NT)), True)
    else:

        @pl.when(known)
        def _():
            through(lambda s: [held_buf[slot, n, :, s] for n in range(3)], True)

        @pl.when(jnp.logical_not(known))
        def _():
            a, dy = a_buf[slot], dy_buf[slot]
            through(lambda s: hidden_back(dot(a, wg_ref[:, s], NN), dot(a, wu_ref[:, s], NN), dot(dy, wd_ref[s, :], NT)), False)

    rest = pl.ds(own, width - own)

    @pl.when(lax.rem(i, each) == each - 1)
    def _():
        for acc, term in zip((accg_ref, accu_ref, accd_ref), terms, strict=True):
            term[i // each] = acc[:, rest]
            acc[:, rest] = jnp.zeros_like(acc[:, rest])

    @pl.when(i == steps - 1)
    def _():
        def rounded(part, total):
            part = part.astype(BF16)
            wide = part.astype(F32)
            return part, total + jnp.sum((wide * wide).reshape(-1, 8, LANES), 0)

        accs = (accg_ref, accu_ref, accd_ref)

        def leave(n, at):
            return pltpu.make_async_copy(results[n].at[at, :], outs[n].at[at, :], w_sems.at[n, 0])

        def rows(r, total):
            at = pl.ds(pl.multiple_of(r * LANES, LANES), LANES)
            for n, acc in enumerate(accs):
                for c in range(0, own, LANES):
                    part, total = rounded(acc[at, c : c + LANES], total)
                    if n < 2:
                        results[n][at, c : c + LANES] = part
            for n in range(2):
                leave(n, at).start()
            return total

        def turn(c, carry):
            at = pl.ds(pl.multiple_of(c * LANES, LANES), LANES)
            for r in range(0, a_buf.shape[2], LANES):
                results[2][at, r : r + LANES] = accd_ref[r : r + LANES, at].astype(BF16).T
            leave(2, at).start()
            return carry

        at = [3 * ((core + s) % 2) + (chip + s // 2) % 2 * (1 - 2 * ((core + s) % 2)) for s in range(4)]
        place = [(core + s) % 2 + 2 * ((chip + s // 2) % 2) for s in range(4)]
        sums = [lax.fori_loop(0, a_buf.shape[2] // LANES, rows, jnp.zeros((8, LANES), F32)), jnp.zeros((8, LANES), F32)]
        sums_ref[0] = sums[0] + before[0][...] if final else sums[0]
        lax.fori_loop(0, own // LANES, turn, 0)
        for n in range(len(others)) if final else ():
            told(n).start()
        for n, term in enumerate(terms):
            part, sums[1] = rounded(term[at[0]] + term[at[1]] + term[at[2]] + term[at[3]], sums[1])
            outs[3 + n][...] = part if n < 2 else part.T
        for n, result in enumerate(results):
            leave(n, pl.ds(0, result.shape[0])).wait()
        if not final:
            outs[6][...], outs[7][...] = sums
        else:
            shared = jnp.sum(sums[1] + before[1][...])
            for n in range(len(others)):
                told(n).wait()
            total = sums_ref[place[0]] + sums_ref[place[1]] + sums_ref[place[2]] + sums_ref[place[3]]
            total = jnp.full((8, LANES), jnp.sum(total) + shared, F32)
            outs[6][...] = jnp.minimum(1.0, 0.5 * lax.rsqrt(total / count + 1e-30))
            outs[7][...] = jnp.zeros((8, LANES), F32)


def slices(layer, own, a_all, dy_all, wg, wu, wd, kept, before=(), count=None):
    tokens, d = a_all[0].shape
    ff = wg.shape[2]
    rest = ff - 4 * own
    width = own + rest
    any_ = pl.BlockSpec(memory_space=pl.ANY)
    at = lambda s: once(s, lambda i: (0, 0))
    sizes = [(d, own), (d, own), (own, d), (d, rest), (d, rest), (rest, d)]
    landed = [jax.ShapeDtypeStruct((2, tokens, d), BF16)] * 2 + [kept[0]]
    return pl.pallas_call(
        lambda *refs: slices_kernel(layer, own, kept[0].shape[0], count, *refs),
        grid=(4 * tokens // ROWS,),
        in_specs=[any_] * (7 + len(kept)) + [at((8, LANES))] * len(before),
        out_specs=[any_] * 3 + [at(s) for s in sizes[3:]] + [at((8, LANES))] * 2 + [any_] * len(landed),
        scratch_shapes=[pltpu.VMEM((d, width), BF16)] * 2
        + [pltpu.VMEM((width, d), BF16)]
        + [pltpu.VMEM((d, width), F32)] * 3
        + [pltpu.VMEM((2, ROWS, d), BF16)] * 2
        + [pltpu.VMEM((4, 8, LANES), F32)]
        + [pltpu.SemaphoreType.DMA(n) for n in ((3, 2), (3, 3), (9,), (9,))]
        + [pltpu.VMEM((4, d, rest), F32)] * 3
        + [pltpu.VMEM((2, kept[0].shape[0], ROWS, width), kept[0].dtype)]
        + [pltpu.VMEM(s, BF16) for s in sizes[:3]],
        out_shape=[jax.ShapeDtypeStruct(s, BF16) for s in sizes]
        + [jax.ShapeDtypeStruct((8, LANES), F32)] * 2
        + [jax.ShapeDtypeStruct(s.shape, s.dtype) for s in landed],
        cost_estimate=pl.CostEstimate(
            flops=12 * 4 * tokens * d * width, bytes_accessed=16 * tokens * d, transcendentals=4 * tokens * width
        ),
        compiler_params=pltpu.CompilerParams(vmem_limit_bytes=62 << 20, collective_id=layer, has_side_effects=True),
        name="slices",
    )(*a_all, *dy_all, wg, wu, wd, *kept, *before)


def adam_math(f, w, m, v, g):
    g = g.astype(F32) * f
    m = 0.9 * m + 0.1 * g
    v = 0.95 * v + 0.05 * g * g
    return (0.998 * w.astype(F32) - 0.02 * (m * lax.rsqrt(v + 1e-8))).astype(BF16), m, v


SLOTS, AHEAD = 8, 4


def adam(own, factor, arrays, pieces, outs):
    d, _ = arrays[0][0].shape[1:]
    main, extra = own // BLOCK * BLOCK, own % BLOCK
    shapes = ((LANES, own), (LANES, d), (d // 2, LANES))
    rows = []
    for n, (which, layer, slot, g) in enumerate(pieces):
        kind = 1 if which == 2 else 2 if slot == 4 else 0
        for r in range(0, g.shape[0], shapes[kind][0]):
            if kind != 1:
                first = (r, 0)
            elif slot == 4:
                first = (4 * own + r, 0)
            else:
                first = (r, main) if r < main else (4 * main + r - main, extra)
            rows.append((kind, which, layer, n, slot, r, *first))
    table = np.array(rows, np.int32).T
    total = len(rows)
    kinds = sorted({row[0] for row in rows})
    n_in = 9 + len(pieces)

    def kernel(table_ref, f_ref, *refs):
        weights, grads = refs[:9], refs[9:n_in]
        refs = refs[n_in + (9 if outs is not None else 0) :]
        results, scratch = refs[:9], refs[9:]
        buffers = {kind: scratch[4 * n : 4 * n + 4] for n, kind in enumerate(kinds)}
        sem_in, sem_out = scratch[-2:]
        f = f_ref[:1, :1]
        me = lax.axis_index("dp")

        def moved(step, do):
            kind, which, layer = (table_ref[n, step] for n in range(3))
            slot = table_ref[4, step]
            unit = (me + slot) % 2 + 2 * ((me // 2 + slot // 2) % 2)
            row = table_ref[6, step] + table_ref[7, step] * unit
            for k in range(3):
                for q in [q for q in kinds if (q == 1) == (k == 2)]:
                    if q == 0:
                        columns = ((unit * main, 0, main), (4 * main + unit * extra, main, extra))
                    else:
                        columns = ((0 if q == 1 else 4 * own, 0, shapes[q][1]),)

                    @pl.when((which == k) & (kind == q))
                    def _():
                        for first, here, size in columns:
                            first = first if isinstance(first, int) else pl.multiple_of(first, LANES)
                            there = (layer, pl.ds(pl.multiple_of(row, LANES), shapes[q][0]), pl.ds(first, size))
                            do(3 * k, there, buffers[q], (lax.rem(step, SLOTS), slice(None), pl.ds(here, size)))

        def fetch(step):
            slot = lax.rem(step, SLOTS)

            def get(k, there, buffer, here):
                for n in range(3):
                    pltpu.make_async_copy(weights[k + n].at[there], buffer[n].at[here], sem_in.at[n, slot]).start()

            moved(step, get)
            piece, row = table_ref[3, step], table_ref[5, step]
            for n, (which_, _, slot_, _) in enumerate(pieces):
                q = 1 if which_ == 2 else 2 if slot_ == 4 else 0

                @pl.when(piece == n)
                def _():
                    rows_ = pl.ds(pl.multiple_of(row, 16), shapes[q][0])
                    pltpu.make_async_copy(grads[n].at[rows_, :], buffers[q][3].at[slot], sem_in.at[3, slot]).start()

        def stored(step, do):
            slot = lax.rem(step, SLOTS)

            def put(k, there, buffer, here):
                for n in range(3):
                    do(pltpu.make_async_copy(buffer[n].at[here], results[k + n].at[there], sem_out.at[n, slot]))

            moved(step, put)

        def early(step, carry):
            fetch(step)
            return carry

        lax.fori_loop(0, min(AHEAD, total), early, 0)

        def body(step, carry):
            @pl.when(step + AHEAD < total)
            def _():
                @pl.when(step + AHEAD >= SLOTS)
                def _():
                    stored(step + AHEAD - SLOTS, lambda copy: copy.wait())

                fetch(step + AHEAD)

            slot = lax.rem(step, SLOTS)
            for q in kinds:

                @pl.when(table_ref[0, step] == q)
                def _():
                    w, m, v, g = buffers[q]
                    for n in range(4):
                        pltpu.make_async_copy(buffers[q][n].at[slot], buffers[q][n].at[slot], sem_in.at[n, slot]).wait()
                    some = 32 if shapes[q][1] > LANES else 224

                    def part(r, carry):
                        at = pl.ds(pl.multiple_of(r * some, some), some)
                        new = adam_math(f, w[slot, at, :], m[slot, at, :], v[slot, at, :], g[slot, at, :])
                        w[slot, at, :], m[slot, at, :], v[slot, at, :] = new
                        return carry

                    lax.fori_loop(0, shapes[q][0] // some, part, 0)

            stored(step, lambda copy: copy.start())
            return carry

        lax.fori_loop(0, total, body, 0)

        def late(step, carry):
            stored(step, lambda copy: copy.wait())
            return carry

        lax.fori_loop(max(0, total - SLOTS), total, late, 0)

    any_ = pl.BlockSpec(memory_space=pl.ANY)
    given = [a for three in arrays for a in three]
    given = [pltpu.with_memory_space_constraint(a, pltpu.HBM) for a in given]
    if outs is None:
        pieces = [(*piece[:3], pltpu.with_memory_space_constraint(piece[3], pltpu.HBM)) for piece in pieces]
    before = [a for three in outs for a in three] if outs is not None else []
    elements = sum(piece[3].size for piece in pieces)
    new = pl.pallas_call(
        kernel,
        in_specs=[pl.BlockSpec(memory_space=pltpu.SMEM), pl.BlockSpec(memory_space=pltpu.VMEM)] + [any_] * (n_in + len(before)),
        out_specs=[any_] * 9,
        out_shape=[jax.ShapeDtypeStruct(a.shape, a.dtype) for a in given],
        scratch_shapes=[pltpu.VMEM((SLOTS, *shapes[q]), t) for q in kinds for t in (BF16, F32, F32, BF16)]
        + [pltpu.SemaphoreType.DMA((4, SLOTS)), pltpu.SemaphoreType.DMA((3, SLOTS))],
        input_output_aliases={2 + n_in + n: n for n in range(len(before))},
        cost_estimate=pl.CostEstimate(flops=2000 * elements, bytes_accessed=22 * elements, transcendentals=elements),
        compiler_params=params(30),
    )(table, factor, *given, *(piece[3] for piece in pieces), *before)
    return tuple(tuple(new[3 * n : 3 * n + 3]) for n in range(3))


def solution(mesh):
    def step(x, dy, wg, wu, wd, mg, mu, md, vg, vu, vd):
        x, dy = x[0], dy[0]
        ff = wg.shape[2]
        own = ff // LANES // 4 * LANES

        def send(a, perm):
            return perm(a)

        dy_x = send(dy, px)
        h1, a1, a0, *made = forward(own, x, wg, wu, wd)
        a1_x = send(a1, px)
        a0_x = send(a0, px)
        dh1, *kept = chain(own, a1, dy, h1, wg, wu, wd)
        dh1_x = send(dh1, px)
        top = slices(1, own, [a1, a1_x], [dy, dy_x], wg, wu, wd, kept)
        top_x = [send(top[n], px) for n in range(3)]
        top_d = [send(top[n], pd) for n in range(3)]
        low = slices(0, own, [a0, a0_x], [dh1, dh1_x], wg, wu, wd, made, top[6:8], wg.size + wu.size + wd.size)
        low_x = [send(low[n], px) for n in range(3)]
        low_d = [send(low[n], pd) for n in range(3)]

        top_xd = [send(top_x[n], pd) for n in range(3)]
        low_xd = [send(low_x[n], pd) for n in range(2)]
        arrays = ((wg, mg, vg), (wu, mu, vu), (wd, md, vd))

        def pieces(layer, slot, gs, names=(0, 1, 2)):
            return [(n, layer, slot, gs[n]) for n in names]

        first = pieces(1, 0, top) + pieces(1, 1, top_d) + pieces(1, 2, top_x) + pieces(0, 0, low)
        shared = pieces(1, 4, top[3:6]) + pieces(0, 4, low[3:6])
        outs = adam(own, low[6], arrays, first + shared, None)
        outs = adam(own, low[6], arrays, pieces(1, 3, top_xd) + pieces(0, 1, low_d), outs)
        outs, low_x[2] = lax.optimization_barrier((outs, low_x[2]))
        low_xd.append(send(low_x[2], pd))
        outs = adam(own, low[6], arrays, pieces(0, 2, low_x) + pieces(0, 3, low_xd, (0, 1)), outs)
        outs = adam(own, low[6], arrays, pieces(0, 3, low_xd, (2,)), outs)
        return tuple(outs[name][which] for which in range(3) for name in range(3))

    return jax.shard_map(
        step,
        mesh=mesh,
        in_specs=(P(("rep", "dp"), None, None),) * 2 + (P(None, None, None),) * 9,
        out_specs=(P("rep", None, None),) * 9,
        check_vma=False,
    )
```

```python
import jax
import jax.numpy as jnp
import numpy as np
from jax import lax
from jax.experimental import pallas as pl
from jax.experimental.pallas import tpu as pltpu
from jax.sharding import PartitionSpec as P


F32, BF16 = jnp.float32, jnp.bfloat16
PX, PD = (tuple((device, device ^ bit) for device in range(4)) for bit in (2, 1))
NN, NT = ((1,), (0,)), ((1,), (1,))

LANES = 128
BLOCK = 512
ROWS, FEW, TOGETHER = 512, 64, 4
HALF = 2 * ROWS


def dot(a, b, dims):
    return lax.dot_general(a, b, (dims, ((), ())), preferred_element_type=F32)


def sigmoid(x):
    return 0.5 * jnp.tanh(0.5 * x) + 0.5


def px(a):
    return lax.ppermute(a, "dp", PX)


def pd(a):
    return lax.ppermute(a, "dp", PD)


def once(shape, index):
    return pl.BlockSpec(shape, index, pipeline_mode=pl.Buffered(1))


def params(mib=62):
    return pltpu.CompilerParams(vmem_limit_bytes=mib << 20)


def norm_scale(wide):
    return lax.rsqrt(jnp.mean(wide * wide, -1, keepdims=True) + 1e-6)


def normed(h):
    wide = h.astype(F32)
    return (wide * norm_scale(wide)).astype(BF16)


def looped(count, rows, body, together=1, after=None):
    def one(n, carry):
        for part in range(together):
            body(pl.ds(pl.multiple_of((n * together + part) * rows, rows), rows))
        if after is not None:
            after(pl.ds(pl.multiple_of(n * together * rows, together * rows), together * rows))
        return carry

    lax.fori_loop(0, count // together, one, 0)


def written(step, last, half, own, tail, stage_ref, outs, sems, do):
    me = lax.axis_index("dp")
    blocks = own // BLOCK
    extra = own - blocks * BLOCK
    rows = pl.ds(pl.multiple_of(half * HALF, HALF), HALF)
    for n, (out, holder) in enumerate(zip(outs, (me, me // 2 * 2 + 1 - me % 2), strict=True)):

        def copy(here, there):
            do(pltpu.make_async_copy(stage_ref.at[half, :, :, here], out.at[:, rows, there], sems.at[n, half]))

        @pl.when((step < 4 * blocks) & (step // blocks == holder))
        def _():
            copy(pl.ds(0, BLOCK), pl.ds(pl.multiple_of(lax.rem(step, blocks) * BLOCK, BLOCK), BLOCK))

        @pl.when(step == 4 * blocks)
        def _():
            copy(pl.ds(pl.multiple_of(holder * extra, LANES), extra), pl.ds(blocks * BLOCK, extra))

        @pl.when(step == last)
        def _():
            copy(pl.ds(0, tail), pl.ds(own, tail))


def halves(tokens, width, moved, there, back):
    j = pl.program_id(0)

    def two(half, carry):
        @pl.when(j > 0)
        def _():
            moved(j - 1, half, lambda copy: copy.wait())

        def run(n):
            return half, n, pl.ds(pl.multiple_of(half * HALF + n * ROWS, ROWS), ROWS), width

        def one(n, carry):
            back(*run(n), there(*run(n)))
            return carry

        if width < BLOCK:
            lax.fori_loop(0, HALF // ROWS, one, 0)
        else:
            held = there(*run(0))
            ahead = there(*run(1))
            back(*run(0), held)
            back(*run(1), ahead)
        moved(j, half, lambda copy: copy.start())
        return carry

    lax.fori_loop(0, tokens // HALF, two, 0)


def forward_kernel(tail, own, x_ref, wg_ref, wu_ref, wd_ref, *refs):
    h_out, a_out, a0_out, mine_ref, theirs_ref, acc_ref, stage_ref, sems, h_ref, a_ref, a0_ref, out_sems = refs
    j, last = pl.program_id(0), pl.num_programs(0) - 1
    tokens = x_ref.shape[0]

    def moved(step, half, do):
        written(step, last, half, own, tail, stage_ref, (mine_ref, theirs_ref), sems, do)

    @pl.when(j == 0)
    def _():
        def start(r):
            a0_ref[r, :] = normed(x_ref[r, :])
            acc_ref[r, :] = jnp.zeros((FEW, acc_ref.shape[1]), F32)

        looped(tokens // FEW, FEW, start, TOGETHER)

    early = pltpu.make_async_copy(a0_ref, a0_out, out_sems.at[2])

    @pl.when(j == 1)
    def _():
        early.start()

    def up(half, n, r, width):
        a = a0_ref[r, :]
        g = dot(a, wg_ref[0, :, :width], NN)
        u = dot(a, wu_ref[0, :, :width], NN)
        for k, value in enumerate((g, u)):
            stage_ref[half, k, pl.ds(pl.multiple_of(n * ROWS, ROWS), ROWS), :width] = value
        return (g * sigmoid(g) * u).astype(BF16)

    def down(half, n, r, width, hid):
        acc_ref[r, :] += dot(hid, wd_ref[0, :width, :], NN)

    @pl.when(j < last)
    def _():
        halves(tokens, wg_ref.shape[2], moved, up, down)

    @pl.when(j == last)
    def _():
        halves(tokens, tail, moved, up, down)

        def end(r):
            h = (x_ref[r, :].astype(F32) + acc_ref[r, :].astype(BF16).astype(F32)).astype(BF16)
            h_ref[r, :] = h
            a_ref[r, :] = normed(h)

        def leave(n, r):
            return pltpu.make_async_copy((a_ref, h_ref)[n].at[r, :], (a_out, h_out)[n].at[r, :], out_sems.at[n])

        looped(tokens // FEW, FEW, end, TOGETHER, lambda r: [leave(n, r).start() for n in range(2)])
        for n in range(2):
            leave(n, pl.ds(0, tokens)).wait()
        early.wait()
        for half in range(tokens // (HALF)):
            moved(j, half, lambda copy: copy.wait())


def keeping(tokens, count, columns, dtype):
    kept = [jax.ShapeDtypeStruct((count, tokens, columns), dtype)] * 2
    parts = tokens // (HALF)
    return kept, [pltpu.VMEM((parts, count, HALF, BLOCK), dtype), pltpu.SemaphoreType.DMA((2, parts))]


def forward(own, x, wg, wu, wd):
    tokens, d = x.shape
    ff = wg.shape[2]
    steps = pl.cdiv(ff, BLOCK)
    tail = ff - (steps - 1) * BLOCK
    full = once((tokens, d), lambda j: (0, 0))
    across = pl.BlockSpec((1, d, BLOCK), lambda j: (0, 0, j))
    down = pl.BlockSpec((1, BLOCK, d), lambda j: (0, j, 0))
    kept, stage = keeping(tokens, 2, own + tail, F32)
    return pl.pallas_call(
        lambda *refs: forward_kernel(tail, own, *refs),
        grid=(steps,),
        in_specs=[full, across, across, down],
        out_specs=[pl.BlockSpec(memory_space=pl.ANY)] * 5,
        out_shape=[jax.ShapeDtypeStruct((tokens, d), BF16)] * 3 + kept,
        scratch_shapes=[pltpu.VMEM((tokens, d), F32)] + stage + [pltpu.VMEM((tokens, d), BF16)] * 3 + [pltpu.SemaphoreType.DMA((3,))],
        cost_estimate=pl.CostEstimate(flops=6 * tokens * d * ff, bytes_accessed=6 * d * ff, transcendentals=tokens * ff),
        compiler_params=params(),
        name="forward",
    )(x, wg, wu, wd)


def hidden_back(g, u, dhid):
    dhid = dhid.astype(BF16).astype(F32)
    sig = sigmoid(g)
    act = g * sig
    return (dhid * u * (sig + act * (1 - sig))).astype(BF16), (dhid * act).astype(BF16), (act * u).astype(BF16)


def chain_kernel(tail, own, a_ref, dy_ref, h_in, wg_ref, wu_ref, wd_ref, dh_out, mine_ref, theirs_ref, *scratch):
    acc_ref, stage_ref, sems, h_ref, dh_ref, out_sems = scratch
    j, last = pl.program_id(0), pl.num_programs(0) - 1
    tokens = a_ref.shape[0]

    def moved(step, half, do):
        written(step, last, half, own, tail, stage_ref, (mine_ref, theirs_ref), sems, do)

    late = pltpu.make_async_copy(h_in, h_ref, out_sems.at[0])

    @pl.when(j == 0)
    def _():
        def start(r):
            acc_ref[r, :] = jnp.zeros((FEW, acc_ref.shape[1]), F32)

        looped(tokens // FEW, FEW, start, TOGETHER)
        late.start()

    def there(half, n, r, width):
        a, dy = a_ref[r, :], dy_ref[r, :]
        g = dot(a, wg_ref[0, :, :width], NN)
        u = dot(a, wu_ref[0, :, :width], NN)
        for k, value in enumerate(hidden_back(g, u, dot(dy, wd_ref[0, :width, :], NT))):
            stage_ref[half, k, pl.ds(pl.multiple_of(n * ROWS, ROWS), ROWS), :width] = value

    def back(half, n, r, width, held):
        dg, du = (stage_ref[half, k, pl.ds(pl.multiple_of(n * ROWS, ROWS), ROWS), :width] for k in range(2))
        acc_ref[r, :] += dot(dg, wg_ref[0, :, :width], NT) + dot(du, wu_ref[0, :, :width], NT)

    @pl.when(j < last)
    def _():
        halves(tokens, wg_ref.shape[2], moved, there, back)

    @pl.when(j == last)
    def _():
        halves(tokens, tail, moved, there, back)
        late.wait()

        def end(r):
            wide, da = h_ref[r, :].astype(F32), acc_ref[r, :].astype(BF16).astype(F32)
            scale = norm_scale(wide)
            through = scale * da - wide * (scale * scale * scale * jnp.mean(wide * da, -1, keepdims=True))
            dh_ref[r, :] = (dy_ref[r, :].astype(F32) + through.astype(BF16).astype(F32)).astype(BF16)

        def leave(r):
            return pltpu.make_async_copy(dh_ref.at[r, :], dh_out.at[r, :], out_sems.at[1])

        looped(tokens // FEW, FEW, end, TOGETHER, lambda r: leave(r).start())
        leave(pl.ds(0, tokens)).wait()
        for half in range(tokens // (HALF)):
            moved(j, half, lambda copy: copy.wait())


def chain(own, a, dy, h, wg, wu, wd):
    tokens, d = a.shape
    ff = wg.shape[2]
    steps = pl.cdiv(ff, BLOCK)
    tail = ff - (steps - 1) * BLOCK
    full = once((tokens, d), lambda j: (0, 0))
    across = pl.BlockSpec((1, d, BLOCK), lambda j: (1, 0, j))
    down = pl.BlockSpec((1, BLOCK, d), lambda j: (1, j, 0))
    kept, stage = keeping(tokens, 3, own + tail, BF16)
    return pl.pallas_call(
        lambda *refs: chain_kernel(tail, own, *refs),
        grid=(steps,),
        in_specs=[full, full, pl.BlockSpec(memory_space=pl.ANY), across, across, down],
        out_specs=[pl.BlockSpec(memory_space=pl.ANY)] * 3,
        out_shape=[jax.ShapeDtypeStruct((tokens, d), BF16)] + kept,
        scratch_shapes=[pltpu.VMEM((tokens, d), F32)] + stage + [pltpu.VMEM((tokens, d), BF16)] * 2 + [pltpu.SemaphoreType.DMA((2,))],
        cost_estimate=pl.CostEstimate(flops=10 * tokens * d * ff, bytes_accessed=6 * d * ff, transcendentals=tokens * ff),
        compiler_params=params(),
        name="chain",
    )(a, dy, h, wg, wu, wd)


GATE_UP, DOWN = (0, 1), (2,)


def slices_kernel(layer, own, kept, count, *refs):
    me = lax.axis_index("dp")
    chip, core = me // 2, me % 2
    partner = chip * 2 + 1 - core
    others = (partner, (1 - chip) * 2 + core, (1 - chip) * 2 + 1 - core)
    final = count is not None

    def take(n):
        nonlocal refs
        taken, refs = refs[:n], refs[n:]
        return taken

    a_own, a_across, dy_own, dy_across, wg_hbm, wu_hbm, wd_hbm = take(7)
    mine, theirs = take(2)
    before = take(2) if final else ()
    outs, (a_land, dy_land) = take(8), take(2)
    held_land = take(1)[0] if kept == 3 else theirs
    wg_ref, wu_ref, wd_ref, accg_ref, accu_ref, accd_ref, a_buf, dy_buf, sums_ref = take(9)
    sems, w_sems, send_sems, recv_sems = take(4)
    terms, (held_buf,), results = take(3), take(1), take(3)
    a_refs = (a_own, a_across, a_land.at[1], a_land.at[0])
    dy_refs = (dy_own, dy_across, dy_land.at[1], dy_land.at[0])
    held_refs = (mine, None, None, held_land)
    i, steps = pl.program_id(0), pl.num_programs(0)
    each = a_own.shape[0] // ROWS
    width = wg_ref.shape[1]
    main = own // BLOCK * BLOCK

    def fetch(step, do):
        slot, who = lax.rem(step, 2), step // each
        rows = pl.ds(pl.multiple_of(lax.rem(step, each) * ROWS, ROWS), ROWS)
        for k, (a, dy, held) in enumerate(zip(a_refs, dy_refs, held_refs, strict=True)):

            @pl.when(who == k)
            def _():
                do(pltpu.make_async_copy(a.at[rows, :], a_buf.at[slot], sems.at[0, slot]))
                do(pltpu.make_async_copy(dy.at[rows, :], dy_buf.at[slot], sems.at[1, slot]))
                if held is not None:
                    do(pltpu.make_async_copy(held.at[:, rows, :], held_buf.at[slot], sems.at[2, slot]))

    def weights(which):
        extra = own - main
        parts = (
            (pl.ds(pl.multiple_of(me * main, LANES), main), pl.ds(0, main)),
            (pl.ds(pl.multiple_of(4 * main + me * extra, LANES), extra), pl.ds(main, extra)),
            (pl.ds(4 * own, width - own), pl.ds(own, width - own)),
        )
        return [
            pltpu.make_async_copy(*((hbm.at[layer, there, :], ref.at[here, :]) if n == 2 else (hbm.at[layer, :, there], ref.at[:, here])), w_sems.at[n, m])
            for n, (hbm, ref) in enumerate(((wg_hbm, wg_ref), (wu_hbm, wu_ref), (wd_hbm, wd_ref)))
            if n in which
            for m, (there, here) in enumerate(parts)
        ]

    def onward(which):
        pairs = [(a_refs[which], a_land.at[which]), (dy_refs[which], dy_land.at[which])]
        if which == 0 and kept == 3:
            pairs.append((theirs, held_land))
        return [
            pltpu.make_async_remote_copy(
                src_ref=src,
                dst_ref=dst,
                send_sem=send_sems.at[3 * which + n],
                recv_sem=recv_sems.at[3 * which + n],
                device_id={"dp": partner},
                device_id_type=pl.DeviceIdType.MESH,
            )
            for n, (src, dst) in enumerate(pairs)
        ]

    def told(n):
        return pltpu.make_async_remote_copy(
            src_ref=sums_ref.at[0],
            dst_ref=sums_ref.at[1 + n],
            send_sem=send_sems.at[6 + n],
            recv_sem=recv_sems.at[6 + n],
            device_id={"dp": others[n]},
            device_id_type=pl.DeviceIdType.MESH,
        )

    barrier = pltpu.get_barrier_semaphore()
    spoken = others if final else others[:1]

    @pl.when(i == 0)
    def _():
        for other in spoken:
            pl.semaphore_signal(barrier, inc=1, device_id={"dp": other}, device_id_type=pl.DeviceIdType.MESH)
        for copy in weights(DOWN) if kept == 2 else ():
            copy.start()
        fetch(i, lambda copy: copy.start())
        for copy in weights(GATE_UP if kept == 2 else GATE_UP + DOWN):
            copy.start()
        for copy in weights(DOWN) if kept == 2 else ():
            copy.wait()

    @pl.when(i == 1)
    def _():
        for copy in weights(GATE_UP if kept == 2 else GATE_UP + DOWN):
            copy.wait()
        pl.semaphore_wait(barrier, len(spoken))
        for which in (1, 0):
            for copy in onward(which):
                copy.start()

    for which in range(2):

        @pl.when(i == (3 - which) * each - 1)
        def _():
            for copy in onward(which):
                copy.wait()

    @pl.when(i + 1 < steps)
    def _():
        fetch(i + 1, lambda copy: copy.start())

    slot = lax.rem(i, 2)
    pltpu.make_async_copy(a_own.at[pl.ds(0, ROWS), :], a_buf.at[slot], sems.at[0, slot]).wait()
    pltpu.make_async_copy(dy_own.at[pl.ds(0, ROWS), :], dy_buf.at[slot], sems.at[1, slot]).wait()
    blocks = [pl.ds(c, min(BLOCK, width - c)) for c in range(0, width, BLOCK)]

    def through(there, first):
        a_t, dy_t = a_buf[slot].T, dy_buf[slot].T

        def back(s, held):
            dg, du, hid = held
            for acc, left, right in ((accg_ref, a_t, dg), (accu_ref, a_t, du), (accd_ref, dy_t, hid)):
                acc[:, s] = (jnp.where(i == 0, 0.0, acc[:, s]) if first else acc[:, s]) + dot(left, right, NN)

        held = there(blocks[0])
        for s, following in zip(blocks, blocks[1:] + [None], strict=True):
            ahead = None if following is None else there(following)
            back(s, held)
            held = ahead

    known = (i // each == 0) | (i // each == 3)

    @pl.when(known)
    def _():
        pltpu.make_async_copy(mine.at[:, pl.ds(0, ROWS), :], held_buf.at[slot], sems.at[2, slot]).wait()

    if kept == 2:

        @pl.when(jnp.logical_not(known))
        def _():
            for s in blocks:
                held_buf[slot, 0, :, s] = dot(a_buf[slot], wg_ref[:, s], NN)
                held_buf[slot, 1, :, s] = dot(a_buf[slot], wu_ref[:, s], NN)

        through(lambda s: hidden_back(held_buf[slot, 0, :, s], held_buf[slot, 1, :, s], dot(dy_buf[slot], wd_ref[s, :], NT)), True)
    else:

        @pl.when(known)
        def _():
            through(lambda s: [held_buf[slot, n, :, s] for n in range(3)], True)

        @pl.when(jnp.logical_not(known))
        def _():
            a, dy = a_buf[slot], dy_buf[slot]
            through(lambda s: hidden_back(dot(a, wg_ref[:, s], NN), dot(a, wu_ref[:, s], NN), dot(dy, wd_ref[s, :], NT)), False)

    rest = pl.ds(own, width - own)

    @pl.when(lax.rem(i, each) == each - 1)
    def _():
        for acc, term in zip((accg_ref, accu_ref, accd_ref), terms, strict=True):
            term[i // each] = acc[:, rest]
            acc[:, rest] = jnp.zeros_like(acc[:, rest])

    @pl.when(i == steps - 1)
    def _():
        def rounded(part, total):
            part = part.astype(BF16)
            wide = part.astype(F32)
            return part, total + jnp.sum((wide * wide).reshape(-1, 8, LANES), 0)

        accs = (accg_ref, accu_ref, accd_ref)

        def leave(n, at):
            return pltpu.make_async_copy(results[n].at[at, :], outs[n].at[at, :], w_sems.at[n, 0])

        def rows(r, total):
            at = pl.ds(pl.multiple_of(r * LANES, LANES), LANES)
            for n, acc in enumerate(accs):
                for c in range(0, own, LANES):
                    part, total = rounded(acc[at, c : c + LANES], total)
                    if n < 2:
                        results[n][at, c : c + LANES] = part
            for n in range(2):
                leave(n, at).start()
            return total

        def turn(c, carry):
            at = pl.ds(pl.multiple_of(c * LANES, LANES), LANES)
            for r in range(0, a_buf.shape[2], LANES):
                results[2][at, r : r + LANES] = accd_ref[r : r + LANES, at].astype(BF16).T
            leave(2, at).start()
            return carry

        at = [3 * ((core + s) % 2) + (chip + s // 2) % 2 * (1 - 2 * ((core + s) % 2)) for s in range(4)]
        place = [(core + s) % 2 + 2 * ((chip + s // 2) % 2) for s in range(4)]
        sums = [lax.fori_loop(0, a_buf.shape[2] // LANES, rows, jnp.zeros((8, LANES), F32)), jnp.zeros((8, LANES), F32)]
        sums_ref[0] = sums[0] + before[0][...] if final else sums[0]
        lax.fori_loop(0, own // LANES, turn, 0)
        for n in range(len(others)) if final else ():
            told(n).start()
        for n, term in enumerate(terms):
            part, sums[1] = rounded(term[at[0]] + term[at[1]] + term[at[2]] + term[at[3]], sums[1])
            outs[3 + n][...] = part if n < 2 else part.T
        for n, result in enumerate(results):
            leave(n, pl.ds(0, result.shape[0])).wait()
        if not final:
            outs[6][...], outs[7][...] = sums
        else:
            shared = jnp.sum(sums[1] + before[1][...])
            for n in range(len(others)):
                told(n).wait()
            total = sums_ref[place[0]] + sums_ref[place[1]] + sums_ref[place[2]] + sums_ref[place[3]]
            total = jnp.full((8, LANES), jnp.sum(total) + shared, F32)
            outs[6][...] = jnp.minimum(1.0, 0.5 * lax.rsqrt(total / count + 1e-30))
            outs[7][...] = jnp.zeros((8, LANES), F32)


def slices(layer, own, a_all, dy_all, wg, wu, wd, kept, before=(), count=None):
    tokens, d = a_all[0].shape
    ff = wg.shape[2]
    rest = ff - 4 * own
    width = own + rest
    any_ = pl.BlockSpec(memory_space=pl.ANY)
    at = lambda s: once(s, lambda i: (0, 0))
    sizes = [(d, own), (d, own), (own, d), (d, rest), (d, rest), (rest, d)]
    landed = [jax.ShapeDtypeStruct((2, tokens, d), BF16)] * 2 + [kept[0]] * (kept[0].shape[0] == 3)
    return pl.pallas_call(
        lambda *refs: slices_kernel(layer, own, kept[0].shape[0], count, *refs),
        grid=(4 * tokens // ROWS,),
        in_specs=[any_] * (7 + len(kept)) + [at((8, LANES))] * len(before),
        out_specs=[any_] * 3 + [at(s) for s in sizes[3:]] + [at((8, LANES))] * 2 + [any_] * len(landed),
        scratch_shapes=[pltpu.VMEM((d, width), BF16)] * 2
        + [pltpu.VMEM((width, d), BF16)]
        + [pltpu.VMEM((d, width), F32)] * 3
        + [pltpu.VMEM((2, ROWS, d), BF16)] * 2
        + [pltpu.VMEM((4, 8, LANES), F32)]
        + [pltpu.SemaphoreType.DMA(n) for n in ((3, 2), (3, 3), (9,), (9,))]
        + [pltpu.VMEM((4, d, rest), F32)] * 3
        + [pltpu.VMEM((2, kept[0].shape[0], ROWS, width), kept[0].dtype)]
        + [pltpu.VMEM(s, BF16) for s in sizes[:3]],
        out_shape=[jax.ShapeDtypeStruct(s, BF16) for s in sizes]
        + [jax.ShapeDtypeStruct((8, LANES), F32)] * 2
        + [jax.ShapeDtypeStruct(s.shape, s.dtype) for s in landed],
        cost_estimate=pl.CostEstimate(
            flops=12 * 4 * tokens * d * width, bytes_accessed=16 * tokens * d, transcendentals=4 * tokens * width
        ),
        compiler_params=pltpu.CompilerParams(vmem_limit_bytes=62 << 20, collective_id=layer, has_side_effects=True),
        name="slices",
    )(*a_all, *dy_all, wg, wu, wd, *kept, *before)


def adam_math(f, w, m, v, g):
    g = g.astype(F32) * f
    m = 0.9 * m + 0.1 * g
    v = 0.95 * v + 0.05 * g * g
    return (0.998 * w.astype(F32) - 0.02 * (m * lax.rsqrt(v + 1e-8))).astype(BF16), m, v


SLOTS, AHEAD = 8, 4


def adam(own, factor, arrays, pieces, outs):
    d, _ = arrays[0][0].shape[1:]
    main, extra = own // BLOCK * BLOCK, own % BLOCK
    shapes = ((LANES, own), (LANES, d), (d // 2, LANES))
    rows = []
    for n, (which, layer, slot, g) in enumerate(pieces):
        kind = 1 if which == 2 else 2 if slot == 4 else 0
        for r in range(0, g.shape[0], shapes[kind][0]):
            if kind != 1:
                first = (r, 0)
            elif slot == 4:
                first = (4 * own + r, 0)
            else:
                first = (r, main) if r < main else (4 * main + r - main, extra)
            rows.append((kind, which, layer, n, slot, r, *first))
    table = np.array(rows, np.int32).T
    total = len(rows)
    kinds = sorted({row[0] for row in rows})
    n_in = 9 + len(pieces)

    def kernel(table_ref, f_ref, *refs):
        weights, grads = refs[:9], refs[9:n_in]
        refs = refs[n_in + (9 if outs is not None else 0) :]
        results, scratch = refs[:9], refs[9:]
        buffers = {kind: scratch[4 * n : 4 * n + 4] for n, kind in enumerate(kinds)}
        sem_in, sem_out = scratch[-2:]
        f = f_ref[:1, :1]
        me = lax.axis_index("dp")

        def moved(step, do):
            kind, which, layer = (table_ref[n, step] for n in range(3))
            slot = table_ref[4, step]
            unit = (me + slot) % 2 + 2 * ((me // 2 + slot // 2) % 2)
            row = table_ref[6, step] + table_ref[7, step] * unit
            for k in range(3):
                for q in [q for q in kinds if (q == 1) == (k == 2)]:
                    if q == 0:
                        columns = ((unit * main, 0, main), (4 * main + unit * extra, main, extra))
                    else:
                        columns = ((0 if q == 1 else 4 * own, 0, shapes[q][1]),)

                    @pl.when((which == k) & (kind == q))
                    def _():
                        for first, here, size in columns:
                            first = first if isinstance(first, int) else pl.multiple_of(first, LANES)
                            there = (layer, pl.ds(pl.multiple_of(row, LANES), shapes[q][0]), pl.ds(first, size))
                            do(3 * k, there, buffers[q], (lax.rem(step, SLOTS), slice(None), pl.ds(here, size)))

        def fetch(step):
            slot = lax.rem(step, SLOTS)

            def get(k, there, buffer, here):
                for n in range(3):
                    pltpu.make_async_copy(weights[k + n].at[there], buffer[n].at[here], sem_in.at[n, slot]).start()

            moved(step, get)
            piece, row = table_ref[3, step], table_ref[5, step]
            for n, (which_, _, slot_, _) in enumerate(pieces):
                q = 1 if which_ == 2 else 2 if slot_ == 4 else 0

                @pl.when(piece == n)
                def _():
                    rows_ = pl.ds(pl.multiple_of(row, 16), shapes[q][0])
                    pltpu.make_async_copy(grads[n].at[rows_, :], buffers[q][3].at[slot], sem_in.at[3, slot]).start()

        def stored(step, do):
            slot = lax.rem(step, SLOTS)

            def put(k, there, buffer, here):
                for n in range(3):
                    do(pltpu.make_async_copy(buffer[n].at[here], results[k + n].at[there], sem_out.at[n, slot]))

            moved(step, put)

        def early(step, carry):
            fetch(step)
            return carry

        lax.fori_loop(0, min(AHEAD, total), early, 0)

        def body(step, carry):
            @pl.when(step + AHEAD < total)
            def _():
                @pl.when(step + AHEAD >= SLOTS)
                def _():
                    stored(step + AHEAD - SLOTS, lambda copy: copy.wait())

                fetch(step + AHEAD)

            slot = lax.rem(step, SLOTS)
            for q in kinds:

                @pl.when(table_ref[0, step] == q)
                def _():
                    w, m, v, g = buffers[q]
                    for n in range(4):
                        pltpu.make_async_copy(buffers[q][n].at[slot], buffers[q][n].at[slot], sem_in.at[n, slot]).wait()
                    some = 32 if shapes[q][1] > LANES else 224

                    def part(r, carry):
                        at = pl.ds(pl.multiple_of(r * some, some), some)
                        new = adam_math(f, w[slot, at, :], m[slot, at, :], v[slot, at, :], g[slot, at, :])
                        w[slot, at, :], m[slot, at, :], v[slot, at, :] = new
                        return carry

                    lax.fori_loop(0, shapes[q][0] // some, part, 0)

            stored(step, lambda copy: copy.start())
            return carry

        lax.fori_loop(0, total, body, 0)

        def late(step, carry):
            stored(step, lambda copy: copy.wait())
            return carry

        lax.fori_loop(max(0, total - SLOTS), total, late, 0)

    any_ = pl.BlockSpec(memory_space=pl.ANY)
    given = [a for three in arrays for a in three]
    given = [pltpu.with_memory_space_constraint(a, pltpu.HBM) for a in given]
    if outs is None:
        pieces = [(*piece[:3], pltpu.with_memory_space_constraint(piece[3], pltpu.HBM)) for piece in pieces]
    before = [a for three in outs for a in three] if outs is not None else []
    elements = sum(piece[3].size for piece in pieces)
    new = pl.pallas_call(
        kernel,
        in_specs=[pl.BlockSpec(memory_space=pltpu.SMEM), pl.BlockSpec(memory_space=pltpu.VMEM)] + [any_] * (n_in + len(before)),
        out_specs=[any_] * 9,
        out_shape=[jax.ShapeDtypeStruct(a.shape, a.dtype) for a in given],
        scratch_shapes=[pltpu.VMEM((SLOTS, *shapes[q]), t) for q in kinds for t in (BF16, F32, F32, BF16)]
        + [pltpu.SemaphoreType.DMA((4, SLOTS)), pltpu.SemaphoreType.DMA((3, SLOTS))],
        input_output_aliases={2 + n_in + n: n for n in range(len(before))},
        cost_estimate=pl.CostEstimate(flops=2000 * elements, bytes_accessed=22 * elements, transcendentals=elements),
        compiler_params=params(30),
    )(table, factor, *given, *(piece[3] for piece in pieces), *before)
    return tuple(tuple(new[3 * n : 3 * n + 3]) for n in range(3))


def solution(mesh):
    def step(x, dy, wg, wu, wd, mg, mu, md, vg, vu, vd):
        x, dy = x[0], dy[0]
        ff = wg.shape[2]
        own = ff // LANES // 4 * LANES

        def send(a, perm):
            return perm(a)

        dy_x = send(dy, px)
        h1, a1, a0, *made = forward(own, x, wg, wu, wd)
        a1_x = send(a1, px)
        a0_x = send(a0, px)
        made[1] = send(made[1], pd)
        dh1, *kept = chain(own, a1, dy, h1, wg, wu, wd)
        dh1_x = send(dh1, px)
        top = slices(1, own, [a1, a1_x], [dy, dy_x], wg, wu, wd, kept)
        top_x = [send(top[n], px) for n in range(3)]
        top_d = [send(top[n], pd) for n in range(3)]
        low = slices(0, own, [a0, a0_x], [dh1, dh1_x], wg, wu, wd, made, top[6:8], wg.size + wu.size + wd.size)
        low_x = [send(low[n], px) for n in range(3)]
        low_d = [send(low[n], pd) for n in range(3)]

        top_xd = [send(top_x[n], pd) for n in range(3)]
        low_xd = [send(low_x[n], pd) for n in range(2)]
        arrays = ((wg, mg, vg), (wu, mu, vu), (wd, md, vd))

        def pieces(layer, slot, gs, names=(0, 1, 2)):
            return [(n, layer, slot, gs[n]) for n in names]

        first = pieces(1, 0, top) + pieces(1, 1, top_d) + pieces(1, 2, top_x) + pieces(0, 0, low)
        shared = pieces(1, 4, top[3:6]) + pieces(0, 4, low[3:6])
        outs = adam(own, low[6], arrays, first + shared, None)
        outs = adam(own, low[6], arrays, pieces(1, 3, top_xd) + pieces(0, 1, low_d), outs)
        outs, low_x[2] = lax.optimization_barrier((outs, low_x[2]))
        low_xd.append(send(low_x[2], pd))
        outs = adam(own, low[6], arrays, pieces(0, 2, low_x) + pieces(0, 3, low_xd, (0, 1)), outs)
        outs = adam(own, low[6], arrays, pieces(0, 3, low_xd, (2,)), outs)
        return tuple(outs[name][which] for which in range(3) for name in range(3))

    return jax.shard_map(
        step,
        mesh=mesh,
        in_specs=(P(("rep", "dp"), None, None),) * 2 + (P(None, None, None),) * 9,
        out_specs=(P("rep", None, None),) * 9,
        check_vma=False,
    )
```
